32 devices in a mesh: section: 4 (over y, x), dev: 8 (over z, core).
Axes of the slice: x: 2, y: 2, z: 4, core: 2. Of those that a mesh axis runs over, the one named last changes fastest.
Arguments:
- late_sent: bfloat16 [4, 784, 1024], P('section', 'dev'), may hold values from -5 to 5
- entry_rows: bfloat16 [784, 1024], P('dev'), may hold values from -5 to 5
- gain_first: float32 [4, 1024], P('section'), may hold values from 0.1 to 1.9
- shift_first: float32 [4, 1024], P('section'), may hold values from -3 to 3
- expand_late: bfloat16 [4, 1024, 4096], P('section', None, 'dev'), may hold values from -0.1875 to 0.1875
- gain_inner: float32 [4, 4096], P('section', 'dev'), may hold values from 0.1 to 1.9
- shift_inner: float32 [4, 4096], P('section', 'dev'), may hold values from -3 to 3
- reduce_late: bfloat16 [4, 4096, 1024], P('section', 'dev'), may hold values from -0.09375 to 0.09375
- early_saved: bfloat16 [4, 12544, 256], P('section', 'dev'), may hold values from -6 to 6
- upstream_grad: bfloat16 [4, 12544, 256], P('section', 'dev'), may hold values from -6 to 6
- exit_grad: bfloat16 [12544, 256], P('dev'), may hold values from -6 to 6
- expand_early: bfloat16 [4, 256, 1024], P('section'), may hold values from -0.375 to 0.375
- reduce_early: bfloat16 [4, 1024, 256], P('section'), may hold values from -0.1875 to 0.1875
Outputs:
- late_out: bfloat16 [4, 784, 1024], P('section', 'dev')
- input_grad: bfloat16 [4, 12544, 256], P('section', 'dev')
- grad_expand: float32 [4, 256, 1024], P('section')
- grad_reduce: float32 [4, 1024, 256], P('section')
The draws below stay inside these ranges and needn't reach their ends.
All inputs are finite; a program needn't handle non-finite values.
Results may differ from the reference program's by a relative error of at most 0.02.
Values may be sent and summed in bfloat16 or wider, within the bound.
A program may use at most 128 MiB of HBM per device.

```python
import math
import jax
import jax.numpy as jnp
from jax import lax

CE = 256
FE = 1024
CL = 1024
FL = 4096
SECTIONS = 4
HID_DEV = 512
E_ROWS = 12544
L_ROWS = 784
N_DEV = 8


def scaled_rows(key, leading):
    keys = jax.random.split(key, 4)
    shape = (leading, L_ROWS, CL)
    base = jnp.clip(jax.random.normal(keys[0], shape, jnp.float32), -4.0, 4.0)
    weight = 0.5
    rise = 6.0
    trend = jnp.exp(math.log(rise) * jnp.arange(L_ROWS, dtype=jnp.float32) / L_ROWS).reshape(1, L_ROWS, 1)
    row_factor = jnp.exp(jax.random.uniform(keys[1], (leading, L_ROWS, 1), jnp.float32, 0.0, math.log(2.0)))
    column_factor = jnp.exp(jax.random.uniform(keys[2], (leading, 1, CL), jnp.float32, 0.0, math.log(10.0)))
    offset = jnp.clip(jax.random.normal(keys[3], (leading, 1, CL), jnp.float32), -2.0, 2.0) * weight
    return 0.005 * (base * row_factor + offset) * trend * column_factor


def draw_late_sent(key, part):
    return scaled_rows(jax.random.fold_in(key, 101), SECTIONS).astype(jnp.bfloat16)


def draw_entry_rows(key, part):
    return scaled_rows(jax.random.fold_in(key, 202), 1)[0].astype(jnp.bfloat16)


def block_scale(own_key, shape, shards, smallest, top_value):
    loudness = 1.0
    for position, parts in shards:
        steps = jax.random.uniform(jax.random.fold_in(jax.random.fold_in(own_key, 6), position), (parts,), jnp.float32, smallest / len(shards), top_value / len(shards))
        loudness = loudness * jnp.repeat(jnp.exp(steps), shape[position] // parts).reshape((-1,) + (1,) * (len(shape) - 1 - position))
    return loudness


def scatter_about(own_key, extent, deviation, reach, cuts=(), held_as=jnp.bfloat16):
    values = jax.random.normal(own_key, extent, jnp.float32) * deviation
    if len(cuts) > 0:
        values = block_scale(own_key, extent, cuts, -0.22, 0.18) * values
    return jnp.clip(values, min=-reach, max=reach).astype(held_as)


def setup_inputs(seed: int = 0) -> dict:
    key_of = jax.random.split(jax.random.key(seed), 14)
    return {
        "late_sent": draw_late_sent(jax.random.fold_in(key_of[13], 71), 0),
        "entry_rows": draw_entry_rows(jax.random.fold_in(key_of[13], 71), 0),
        "gain_first": jnp.clip(1.0 + 0.18 * jax.random.normal(key_of[2], (SECTIONS, CL), jnp.float32), 0.1, 1.9),
        "shift_first": scatter_about(key_of[3], (SECTIONS, CL), 0.5, 3.0, ((0, 4),), jnp.float32),
        "expand_late": scatter_about(key_of[4], (SECTIONS, CL, FL), CL ** -0.5, 0.1875, ((0, 4), (2, 8))),
        "gain_inner": jnp.clip(1.0 + 0.18 * jax.random.normal(key_of[5], (SECTIONS, FL), jnp.float32), 0.1, 1.9),
        "shift_inner": scatter_about(key_of[6], (SECTIONS, FL), 0.5, 3.0, ((0, 4), (1, 8)), jnp.float32),
        "reduce_late": scatter_about(key_of[7], (SECTIONS, FL, CL), FL ** -0.5, 0.09375, ((0, 4), (1, 8))),
        "early_saved": scatter_about(key_of[8], (SECTIONS, E_ROWS, CE), 1.0, 6.0, ((0, 4), (1, 8))),
        "upstream_grad": scatter_about(key_of[9], (SECTIONS, E_ROWS, CE), 1.0, 6.0, ((0, 4), (1, 8))),
        "exit_grad": scatter_about(key_of[10], (E_ROWS, CE), 1.0, 6.0, ((0, 8),)),
        "expand_early": scatter_about(key_of[11], (SECTIONS, CE, FE), CE ** -0.5, 0.375, ((0, 4),)),
        "reduce_early": scatter_about(key_of[12], (SECTIONS, FE, CE), FE ** -0.5, 0.1875, ((0, 4),)),
    }


epsilon = 1e-05

def affine(sums, squares, count, gain, shift):
    average = sums / count
    second = squares / count
    spread = gain * lax.rsqrt(second - average * average + epsilon)
    return (spread, shift - average * spread)

def silu_slope(values):
    sigma = jax.nn.sigmoid(values)
    return sigma * (1.0 + values * (1.0 - sigma))

def late_block(inputs, gain_first, shift_first, expand, gain_inner, shift_inner, reduce_weight):
    count = inputs.shape[0]
    values = inputs.astype(jnp.float32)
    spread, offset = affine(lax.optimization_barrier(jnp.sum(values, axis=0)), lax.optimization_barrier(jnp.sum(values * values, axis=0)), count, gain_first, shift_first)
    first = jax.nn.silu(values * spread + offset).astype(jnp.bfloat16)
    inner = jnp.dot(first, expand, preferred_element_type=jnp.float32)
    spread_two, offset_two = affine(lax.optimization_barrier(jnp.sum(inner, axis=0)), lax.optimization_barrier(jnp.sum(inner * inner, axis=0)), count, gain_inner, shift_inner)
    hidden = jax.nn.silu(inner * spread_two + offset_two).astype(jnp.bfloat16)

    def add_group(total, group):
        start = (group * HID_DEV).astype(jnp.int32)
        term = jnp.dot(lax.dynamic_slice_in_dim(hidden, start, HID_DEV, 1), lax.dynamic_slice_in_dim(reduce_weight, start, HID_DEV, 0), preferred_element_type=jnp.float32)
        rounded = lax.optimization_barrier(term.astype(jnp.bfloat16))
        return (total + rounded.astype(jnp.float32), None)
    total, unused = lax.scan(add_group, jnp.zeros((count, CL), jnp.float32), jnp.arange(N_DEV, dtype=jnp.int32))
    return (values + total).astype(jnp.bfloat16)

def early_block(saved, grad, expand, reduce_weight):
    pre = jnp.dot(saved, expand, preferred_element_type=jnp.float32)
    hidden = jax.nn.silu(pre).astype(jnp.bfloat16)
    back = lax.dot_general(grad, reduce_weight, (((1,), (1,)), ((), ())), preferred_element_type=jnp.float32)
    slope = (back * silu_slope(pre)).astype(jnp.bfloat16)
    result = grad.astype(jnp.float32) + lax.dot_general(slope, expand, (((1,), (1,)), ((), ())), preferred_element_type=jnp.float32)
    grad_expand = lax.dot_general(saved, slope, (((0,), (0,)), ((), ())), preferred_element_type=jnp.float32)
    grad_reduce = lax.dot_general(hidden, grad, (((0,), (0,)), ((), ())), preferred_element_type=jnp.float32)
    return (result.astype(jnp.bfloat16), grad_expand, grad_reduce)

def reference(late_sent, entry_rows, gain_first, shift_first, expand_late, gain_inner, shift_inner, reduce_late, early_saved, upstream_grad, exit_grad, expand_early, reduce_early):
    late_in = jnp.concatenate([entry_rows[None], late_sent[:-1]], axis=0)
    grad_in = jnp.concatenate([upstream_grad[1:], exit_grad[None]], axis=0)
    late_out = lax.map(lambda items: late_block(*items), (late_in, gain_first, shift_first, expand_late, gain_inner, shift_inner, reduce_late))
    input_grad, grad_expand, grad_reduce = lax.map(lambda items: early_block(*items), (early_saved, grad_in, expand_early, reduce_early))
    factor = 1.0 / math.sqrt(E_ROWS)
    return (late_out, input_grad, grad_expand * factor, grad_reduce * factor)
```

```python
import functools
import math

import jax
import jax.numpy as jnp
from jax import lax
from jax.experimental import pallas as pl
from jax.experimental.pallas import tpu as pltpu
from jax.sharding import PartitionSpec as P

MESH = pl.DeviceIdType.MESH
epsilon = 1e-05
H = 4
SKEW = 3
F32 = jnp.float32
BF16 = jnp.bfloat16


def sigmoid(x):
    return 0.5 * jnp.tanh(0.5 * x) + 0.5


def affine(sums, squares, count, gain, shift):
    average = sums / count
    second = squares / count
    spread = gain * lax.rsqrt(second - average * average + epsilon)
    return spread, shift - average * spread


def dot(a, b, ca=1, cb=0):
    return lax.dot_general(a, b, (((ca,), (cb,)), ((), ())), preferred_element_type=F32)


def both(a, b):
    return jnp.logical_and(a, b)


def kernel(
    sections, n_dev, chunk, split,
    late_hbm, entry_hbm, gain1, shift1, wexp_hbm, gain2, shift2, wred_hbm,
    saved_hbm, up_hbm, exit_hbm, eexp_hbm, ered_hbm,
    late_out, input_grad, gout,
    stage, lbuf, first, inner, hidden, part, prx, rx,
    wexp, wred, saved, grad, eexp, ered, act, dsl, slope,
    gsum, gtx, gprx, wtx, wrx,
    loc_sem, perm_send, perm_recv, gp_send, gp_recv,
    ag_s, ag_r, agp_s, agp_r, px_s, px_r, gx_s, gx_r, st_s, st_r, wp_s, wp_r,
):
    Q = n_dev // 2
    s = lax.axis_index("section")
    d = lax.axis_index("dev")
    q = d // 2
    c = lax.rem(d, 2)
    other = 1 - c
    partner = q * 2 + other
    rows = late_hbm.shape[0]
    half = late_hbm.shape[1] // H
    padded = first.shape[0] // n_dev
    e_rows = saved_hbm.shape[0]
    steps = e_rows // chunk
    total_rows = rows * n_dev
    hid = wexp.shape[1]
    wide = eexp.shape[1]
    pieces, depth = gsum.shape[1], gsum.shape[2]
    factor = 1.0 / math.sqrt(e_rows * n_dev)

    last = Q - 1
    right, left = jnp.minimum(q + 1, last), jnp.maximum(q - 1, 0)
    nxt = (right * 2 + c, left * 2 + c)
    has_next = (q < last, q > 0)
    has_prev = (q > 0, q < last)
    hops = (q, last - q)

    barrier = pltpu.get_barrier_semaphore()
    pl.semaphore_signal(barrier, inc=1, device_id=(s, partner), device_id_type=MESH)
    for way in range(2):
        @pl.when(has_next[way])
        def _():
            pl.semaphore_signal(barrier, inc=1, device_id=(s, nxt[way]), device_id_type=MESH)

    @pl.when(s > 0)
    def _():
        pl.semaphore_signal(barrier, inc=1, device_id=(s - 1, d), device_id_type=MESH)

    @pl.when(s < sections - 1)
    def _():
        pl.semaphore_signal(barrier, inc=1, device_id=(s + 1, d), device_id_type=MESH)

    stage_copy = pltpu.make_async_copy(late_hbm, stage, loc_sem.at[5])
    stage_copy.start()
    local = [
        pltpu.make_async_copy(src, dst, loc_sem.at[i])
        for i, (src, dst) in enumerate(
            ((saved_hbm, saved), (eexp_hbm, eexp), (ered_hbm, ered), (wexp_hbm, wexp), (wred_hbm, wred))
        )
    ]
    for copy in local:
        copy.start()

    def remote(src, dst, send, recv, section, dev):
        return pltpu.make_async_remote_copy(
            src_ref=src, dst_ref=dst, send_sem=send, recv_sem=recv,
            device_id=(section, dev), device_id_type=MESH,
        )

    def cols(h):
        return pl.ds(h * half, half)

    def late_copy(h):
        return remote(
            stage.at[:, cols(h)], lbuf.at[h, d], perm_send.at[h], perm_recv.at[h],
            jnp.minimum(s + 1, sections - 1), d,
        )

    def entry_copy(h):
        return pltpu.make_async_copy(entry_hbm.at[:, cols(h)], lbuf.at[h, d], perm_recv.at[h])

    def chunk_rows(j):
        return pl.ds(j * chunk, chunk)

    def grad_copy(j):
        return remote(
            up_hbm.at[chunk_rows(j)], grad.at[chunk_rows(j)], gp_send.at[j], gp_recv.at[j],
            jnp.maximum(s - 1, 0), d,
        )

    def exit_copy(j):
        return pltpu.make_async_copy(exit_hbm.at[chunk_rows(j)], grad.at[chunk_rows(j)], gp_recv.at[j])

    stage_copy.wait()
    pl.semaphore_wait(
        barrier,
        1 + jnp.minimum(q, 1) + jnp.minimum(last - q, 1) + jnp.minimum(s, 1) + jnp.minimum(sections - 1 - s, 1),
    )

    @pl.when(s < sections - 1)
    def _():
        for h in range(H):
            late_copy(h).start()

    @pl.when(s == 0)
    def _():
        for h in range(H):
            entry_copy(h).start()

    @pl.when(s > 0)
    def _():
        for j in range(steps):
            grad_copy(j).start()

    @pl.when(s == sections - 1)
    def _():
        for j in range(steps):
            exit_copy(j).start()

    def source(way, k):
        return jnp.maximum(q - k, 0) if way == 0 else jnp.minimum(q + k, last)

    def have(way, k):
        return hops[way] >= k

    def hop(way, k, h):
        piece = lbuf.at[h, source(way, k) * 2 + c]
        return remote(piece, piece, ag_s.at[way, k, h], ag_r.at[way, k, h], s, nxt[way])

    def arrival(way, k, h):
        piece = lbuf.at[h, source(way, k) * 2 + c]
        return remote(piece, piece, ag_s.at[way, k - 1, h], ag_r.at[way, k - 1, h], s, nxt[way])

    def share(way, k, h, lane):
        piece = lbuf.at[h, source(way, k) * 2 + lane]
        return remote(piece, piece, agp_s.at[way, k, h], agp_r.at[way, k, h], s, partner)

    def own(h):
        @pl.when(s == 0)
        def _():
            entry_copy(h).wait()

        @pl.when(s > 0)
        def _():
            late_copy(h).wait_recv()

        for way in range(2):
            @pl.when(has_next[way])
            def _():
                hop(way, 0, h).start()
        share(0, 0, h, c).start()

    def relay(k, h):
        for way in range(2):
            @pl.when(have(way, k))
            def _():
                arrival(way, k, h).wait_recv()
                if k < last:
                    @pl.when(has_next[way])
                    def _():
                        hop(way, k, h).start()
                share(way, k, h, c).start()

    def gathered(h):
        share(0, 0, h, other).wait_recv()
        for k in range(1, Q):
            for way in range(2):
                @pl.when(have(way, k))
                def _():
                    share(way, k, h, other).wait_recv()

    def gather_drain():
        for h in range(H):
            share(0, 0, h, c).wait_send()
            for way in range(2):
                @pl.when(has_next[way])
                def _():
                    hop(way, 0, h).wait_send()
                for k in range(1, Q):
                    @pl.when(have(way, k))
                    def _():
                        share(way, k, h, c).wait_send()
                        if k < last:
                            @pl.when(has_next[way])
                            def _():
                                hop(way, k, h).wait_send()

    def forward(j):
        at = chunk_rows(j)
        pre = dot(saved[at], eexp[...])
        sigma = sigmoid(pre)
        value = pre * sigma
        act[at] = value.astype(BF16)
        dsl[at] = (sigma * (1.0 + pre - value)).astype(BF16)

    def backward(j):
        at = chunk_rows(j)

        @pl.when(s < sections - 1)
        def _():
            grad_copy(j).wait_recv()

        @pl.when(s == sections - 1)
        def _():
            exit_copy(j).wait()

        g = grad[at]
        back = dot(g, ered[...], 1, 1)
        sl = (back * dsl[at].astype(F32)).astype(BF16)
        slope[at] = sl
        input_grad[at] = (g.astype(F32) + dot(sl, eexp[...], 1, 1)).astype(BF16)

    def weight_sums(lo, hi):
        at = pl.ds(lo * chunk, (hi - lo) * chunk)
        for n in range(wide // 256):
            col = pl.ds(n * 256, 256)
            for which, (a, b) in enumerate(((saved, slope), (grad, act))):
                value = dot(a[at], b[at, col], 0, 0).reshape(pieces, depth, 256)
                if lo > 0:
                    value += gsum[which, :, :, col]
                gsum[which, :, :, col] = value

    local[0].wait()
    local[1].wait()
    early = max(steps // 2, 1)
    for j in range(early):
        forward(j)
    for dev in range(n_dev):
        first[pl.ds((dev + 1) * padded - 16, 16), :] = jnp.zeros((16, first.shape[1]), BF16)
    for way in range(2):
        @pl.when(hops[way] == 0)
        def _():
            wrx[way] = jnp.zeros(wrx.shape[1:], BF16)
            rx[way] = jnp.zeros(rx.shape[1:], BF16)
    for h in range(H):
        own(h)
        if early + h < steps:
            forward(early + h)
    for j in range(early + H, steps):
        forward(j)
    local[2].wait()
    local[3].wait()
    local[4].wait()

    def activate(h):
        total = jnp.zeros((1, half), F32)
        squares = jnp.zeros((1, half), F32)
        for dev in range(n_dev):
            v = lbuf[h, dev].astype(F32)
            total += jnp.sum(v, axis=0, keepdims=True)
            squares += jnp.sum(v * v, axis=0, keepdims=True)
        spread, offset = affine(total, squares, total_rows, gain1[:, cols(h)], shift1[:, cols(h)])
        for dev in range(n_dev):
            v = lbuf[h, dev].astype(F32) * spread + offset
            first[pl.ds(dev * padded, rows), cols(h)] = (v * sigmoid(v)).astype(BF16)

    width = min(256, hid)

    def expand(h):
        for n in range(hid // width):
            at = pl.ds(n * width, width)
            if split:
                value = dot(first[:, cols(h)], wexp[cols(h), at])
                if h > 0:
                    value += inner[:, at]
                if h < H - 1:
                    inner[:, at] = value
            elif h == H - 1:
                value = dot(first[...], wexp[:, at])
            if h == H - 1:
                spread, offset = affine(
                    jnp.sum(value, axis=0, keepdims=True),
                    jnp.sum(value * value, axis=0, keepdims=True),
                    total_rows, gain2[:, at], shift2[:, at],
                )
                v = value * spread + offset
                hidden[:, at] = (v * sigmoid(v)).astype(BF16)

    early_back = min(2, steps)
    for k in range(1, Q):
        if k == last:
            for j in range(early_back):
                backward(j)
        for h in range(H):
            relay(k, h)
            if k == last:
                gathered(h)
                activate(h)
                expand(h)

    def pair_copy(h):
        return remote(part.at[other, h], prx.at[h], px_s.at[h], px_r.at[h], s, partner)

    tile = min(256, half)
    for h in range(H):
        for n in range(half // tile):
            value = dot(hidden[...], wred[:, pl.ds(h * half + n * tile, tile)]).astype(BF16)
            for dev in range(n_dev):
                part[dev % 2, h, dev // 2, :, pl.ds(n * tile, tile)] = value[dev * padded:dev * padded + rows]
        pair_copy(h).start()

    far = last * H

    def mine(h, chip):
        return part[c, h, chip].astype(F32) + prx[h, chip].astype(F32)

    def goal(way, m):
        return last - m if way == 0 else m

    def row_hop(way, r):
        m, h = r // H, lax.rem(r, H)
        to = goal(way, m)
        i = r + pieces * jnp.minimum(m, 1)
        return remote(part.at[c, h, to], rx.at[way, h, to], st_s.at[way, i], st_r.at[way, i], s, nxt[way])

    def row_start(way, r):
        m, h = r // H, lax.rem(r, H)
        to = goal(way, m)
        part[c, h, to] = mine(h, to).astype(BF16)
        row_hop(way, r).start()

    def row_relay(way, r):
        m, h = r // H, lax.rem(r, H)
        to = goal(way, m)

        @pl.when(last - m >= hops[way])
        def _():
            row_hop(way, r).wait_recv()

        @pl.when(last - m > hops[way])
        def _():
            part[c, h, to] = (mine(h, to) + rx[way, h, to].astype(F32)).astype(BF16)
            row_hop(way, r).start()

    def each(lo, hi, body):
        def step(i, carry):
            body(i)
            return carry
        lax.fori_loop(lo, hi, step, 0)

    for h in range(H):
        pair_copy(h).wait_recv()
        for way in range(2):
            @pl.when(hops[way] == 0)
            def _():
                row_start(way, h)

    for j in range(early_back, steps - 1):
        backward(j)
    weight_sums(0, steps - 1)
    backward(steps - 1)
    weight_sums(steps - 1, steps)

    def gx(i):
        return remote(gtx.at[i], gprx.at[i], gx_s.at[i], gx_r.at[i], s, partner)

    for i in range(pieces):
        gtx[i] = gsum[other, i].astype(BF16)
        gx(i).start()

    def term(i):
        return gsum[c, i] + gprx[i].astype(F32)

    def sum_hop(way, i):
        return remote(wtx.at[way, i], wrx.at[way, i], st_s.at[way, H + i], st_r.at[way, H + i], s, nxt[way])

    def sum_first(i):
        gx(i).wait_recv()
        for way in range(2):
            @pl.when(hops[way] == 0)
            def _():
                wtx[way, i] = term(i).astype(BF16)
                sum_hop(way, i).start()

    def sum_relay(way, i):
        sum_hop(way, i).wait_recv()

        @pl.when(has_next[way])
        def _():
            wtx[way, i] = (term(i) + wrx[way, i].astype(F32)).astype(BF16)
            sum_hop(way, i).start()

    def give(i, lane):
        return remote(gout.at[lane, i], gout.at[lane, i], wp_s.at[i], wp_r.at[i], s, partner)

    def sum_finish(i):
        value = term(i) + (wrx[0, i].astype(F32) + wrx[1, i].astype(F32))
        gout[c, i] = (value * factor).astype(BF16)
        give(i, c).start()

    each(0, pieces, sum_first)

    def rest(r):
        for way in range(2):
            @pl.when(hops[way] == 0)
            def _():
                row_start(way, r)

    each(H, far, rest)

    count = far + pieces
    farther = jnp.maximum(hops[0], hops[1])

    def slot(t):
        for way in range(2):
            i = t - SKEW * hops[way]
            live = hops[way] > 0

            @pl.when(both(live, both(i >= 0, i < H)))
            def _():
                row_relay(way, i)

            @pl.when(both(live, both(i >= H, i < H + pieces)))
            def _():
                sum_relay(way, i - H)

            @pl.when(both(live, both(i >= H + pieces, i < count)))
            def _():
                row_relay(way, i - pieces)

        i = t - SKEW * farther - H

        @pl.when(both(i >= 0, i < pieces))
        def _():
            sum_finish(i)

    each(SKEW, count + SKEW * last, slot)

    for h in range(H):
        value = mine(h, q) + rx[0, h, q].astype(F32) + rx[1, h, q].astype(F32)
        late_out[:, cols(h)] = (lbuf[h, d].astype(F32) + value).astype(BF16)

    @pl.when(s < sections - 1)
    def _():
        for h in range(H):
            late_copy(h).wait_send()

    @pl.when(s > 0)
    def _():
        for j in range(steps):
            grad_copy(j).wait_send()

    gather_drain()
    for h in range(H):
        pair_copy(h).wait_send()

    def drain_rows(r):
        for way in range(2):
            @pl.when(last - r // H > hops[way])
            def _():
                row_hop(way, r).wait_send()

    each(0, far, drain_rows)

    def drain_sums(i):
        gx(i).wait_send()
        give(i, c).wait_send()
        for way in range(2):
            @pl.when(has_next[way])
            def _():
                sum_hop(way, i).wait_send()

    each(0, pieces, drain_sums)
    for i in range(pieces):
        give(i, other).wait_recv()


def finish(late_in, grad_in, sums, late_out, input_grad, gexp, gred, wide_e, wide_r, sem):
    ce, fe = wide_e.shape
    a = pltpu.make_async_copy(grad_in, input_grad.at[0], sem.at[0])
    b = pltpu.make_async_copy(late_in, late_out.at[0], sem.at[1])
    a.start()
    b.start()
    wide_e[...] = sums[0].reshape(ce, fe).astype(F32)
    x = pltpu.make_async_copy(wide_e, gexp.at[0], sem.at[2])
    x.start()
    for n in range(fe // 256):
        at = pl.ds(n * 256, 256)
        wide_r[at, :] = sums[1, :, :, at].reshape(ce, 256).astype(F32).T
    y = pltpu.make_async_copy(wide_r, gred.at[0], sem.at[3])
    y.start()
    for copy in (a, b, x, y):
        copy.wait()


def shards(
    sections, n_dev,
    late_sent, entry_rows, gain_first, shift_first, expand_late, gain_inner, shift_inner,
    reduce_late, early_saved, upstream_grad, exit_grad, expand_early, reduce_early,
):
    rows, cl = entry_rows.shape
    e_rows, ce = exit_grad.shape
    fe = expand_early.shape[2]
    hid = expand_late.shape[2]
    Q = n_dev // 2
    half = cl // H
    padded = -(-rows // 16) * 16
    chunk = max(k for k in range(16, 257, 16) if e_rows % k == 0)
    steps = e_rows // chunk
    pieces = ce // 32
    depth = ce // pieces
    count = (Q - 1) * H + pieces
    split = n_dev * padded * hid * 4 <= 4 * 1024 * 1024
    hbm = pl.BlockSpec(memory_space=pltpu.HBM)
    any_spec = pl.BlockSpec(memory_space=pl.ANY)
    vm = pl.BlockSpec(memory_space=pltpu.VMEM)
    V = pltpu.VMEM
    dma = pltpu.SemaphoreType.DMA
    late_out, input_grad, sums = pl.pallas_call(
        functools.partial(kernel, sections, n_dev, chunk, split),
        out_shape=(
            V((rows, cl), BF16),
            V((e_rows, ce), BF16),
            V((2, pieces, depth, fe), BF16),
        ),
        in_specs=[hbm, hbm, vm, vm, hbm, vm, vm] + [hbm] * 6,
        out_specs=(vm, vm, vm),
        scratch_shapes=[
            V((rows, cl), BF16),
            V((H, n_dev, rows, half), BF16),
            V((n_dev * padded, cl), BF16),
            V((n_dev * padded, hid) if split else (8, 128), F32),
            V((n_dev * padded, hid), BF16),
            V((2, H, Q, rows, half), BF16),
            V((H, Q, rows, half), BF16),
            V((2, H, Q, rows, half), BF16),
            V((cl, hid), BF16),
            V((hid, cl), BF16),
            V((e_rows, ce), BF16),
            V((e_rows, ce), BF16),
            V((ce, fe), BF16),
            V((fe, ce), BF16),
            V((e_rows, fe), BF16),
            V((e_rows, fe), BF16),
            V((e_rows, fe), BF16),
            V((2, pieces, depth, fe), F32),
            V((pieces, depth, fe), BF16),
            V((pieces, depth, fe), BF16),
            V((2, pieces, depth, fe), BF16),
            V((2, pieces, depth, fe), BF16),
            dma((6,)), dma((H,)), dma((H,)), dma((steps,)), dma((steps,)),
            dma((2, Q - 1, H)), dma((2, Q - 1, H)), dma((2, Q, H)), dma((2, Q, H)),
            dma((H,)), dma((H,)), dma((pieces,)), dma((pieces,)),
            dma((2, count)), dma((2, count)), dma((pieces,)), dma((pieces,)),
        ],
        compiler_params=pltpu.CompilerParams(
            collective_id=0, has_side_effects=True, vmem_limit_bytes=60 * 1024 * 1024
        ),
        name="relay",
    )(
        late_sent[0], entry_rows, gain_first, shift_first, expand_late[0], gain_inner, shift_inner,
        reduce_late[0], early_saved[0], upstream_grad[0], exit_grad, expand_early[0], reduce_early[0],
    )
    return pl.pallas_call(
        finish,
        out_shape=(
            jax.ShapeDtypeStruct((1, rows, cl), BF16),
            jax.ShapeDtypeStruct((1, e_rows, ce), BF16),
            jax.ShapeDtypeStruct((1, ce, fe), F32),
            jax.ShapeDtypeStruct((1, fe, ce), F32),
        ),
        in_specs=[vm, vm, vm],
        out_specs=(any_spec,) * 4,
        scratch_shapes=[V((ce, fe), F32), V((fe, ce), F32), dma((4,))],
        compiler_params=pltpu.CompilerParams(vmem_limit_bytes=16 * 1024 * 1024),
        name="finish",
    )(late_out, input_grad, sums)


def solution(mesh):
    sections, n_dev = mesh.shape["section"], mesh.shape["dev"]
    sd, dd = P("section", "dev", None), P("dev", None)
    rep, one = P("section", None, None), P("section", None)
    in_specs = (
        sd, dd, one, one, P("section", None, "dev"), P("section", "dev"), P("section", "dev"),
        sd, sd, sd, dd, rep, rep,
    )
    return jax.shard_map(
        functools.partial(shards, sections, n_dev), mesh=mesh, in_specs=in_specs,
        out_specs=(sd, sd, rep, rep), check_vma=False,
    )
```

```python
import functools
import math

import jax
import jax.numpy as jnp
from jax import lax
from jax.experimental import pallas as pl
from jax.experimental.pallas import tpu as pltpu
from jax.sharding import PartitionSpec as P

MESH = pl.DeviceIdType.MESH
epsilon = 1e-05
H = 4
SKEW = 3
F32 = jnp.float32
BF16 = jnp.bfloat16


def scaled_silu(x, spread, offset):
    u = x * (0.5 * spread) + 0.5 * offset
    return u * jnp.tanh(u) + u


def affine(sums, squares, count, gain, shift):
    average = sums / count
    second = squares / count
    spread = gain * lax.rsqrt(second - average * average + epsilon)
    return spread, shift - average * spread


def dot(a, b, ca=1, cb=0):
    return lax.dot_general(a, b, (((ca,), (cb,)), ((), ())), preferred_element_type=F32)


def both(a, b):
    return jnp.logical_and(a, b)


def kernel(
    sections, n_dev, chunk, split,
    late_hbm, entry_hbm, gain1, shift1, wexp_hbm, gain2, shift2, wred_hbm,
    saved_hbm, up_hbm, exit_hbm, eexp_hbm, ered_hbm,
    late_out, input_grad, gout,
    stage, lbuf, first, inner, hidden, part, prx, rx,
    wexp, wred, saved, grad, eexp, ered, act, dsl, slope,
    gsum, gtx, gprx, wtx, wrx,
    loc_sem, perm_send, perm_recv, gp_send, gp_recv,
    ag_s, ag_r, agp_s, agp_r, px_s, px_r, gx_s, gx_r, st_s, st_r, wp_s, wp_r,
):
    Q = n_dev // 2
    s = lax.axis_index("section")
    d = lax.axis_index("dev")
    q = d // 2
    c = lax.rem(d, 2)
    other = 1 - c
    partner = q * 2 + other
    rows = late_hbm.shape[0]
    half = late_hbm.shape[1] // H
    padded = first.shape[0] // n_dev
    e_rows = saved_hbm.shape[0]
    steps = e_rows // chunk
    total_rows = rows * n_dev
    hid = wexp.shape[1]
    wide = eexp.shape[1]
    pieces, depth = gsum.shape[1], gsum.shape[2]
    factor = 1.0 / math.sqrt(e_rows * n_dev)

    last = Q - 1
    right, left = jnp.minimum(q + 1, last), jnp.maximum(q - 1, 0)
    nxt = (right * 2 + c, left * 2 + c)
    has_next = (q < last, q > 0)
    has_prev = (q > 0, q < last)
    hops = (q, last - q)

    barrier = pltpu.get_barrier_semaphore()
    pl.semaphore_signal(barrier, inc=1, device_id=(s, partner), device_id_type=MESH)
    for way in range(2):
        @pl.when(has_next[way])
        def _():
            pl.semaphore_signal(barrier, inc=1, device_id=(s, nxt[way]), device_id_type=MESH)

    @pl.when(s > 0)
    def _():
        pl.semaphore_signal(barrier, inc=1, device_id=(s - 1, d), device_id_type=MESH)

    @pl.when(s < sections - 1)
    def _():
        pl.semaphore_signal(barrier, inc=1, device_id=(s + 1, d), device_id_type=MESH)

    stage_copy = pltpu.make_async_copy(late_hbm, stage, loc_sem.at[5])
    stage_copy.start()
    local = [
        pltpu.make_async_copy(src, dst, loc_sem.at[i])
        for i, (src, dst) in enumerate(
            ((saved_hbm, saved), (eexp_hbm, eexp), (ered_hbm, ered), (wexp_hbm, wexp), (wred_hbm, wred))
        )
    ]
    for copy in local:
        copy.start()

    def remote(src, dst, send, recv, section, dev):
        return pltpu.make_async_remote_copy(
            src_ref=src, dst_ref=dst, send_sem=send, recv_sem=recv,
            device_id=(section, dev), device_id_type=MESH,
        )

    def cols(h):
        return pl.ds(h * half, half)

    def late_copy(h):
        return remote(
            stage.at[:, cols(h)], lbuf.at[h, d], perm_send.at[h], perm_recv.at[h],
            jnp.minimum(s + 1, sections - 1), d,
        )

    def entry_copy(h):
        return pltpu.make_async_copy(entry_hbm.at[:, cols(h)], lbuf.at[h, d], perm_recv.at[h])

    def chunk_rows(j):
        return pl.ds(j * chunk, chunk)

    def grad_copy(j):
        return remote(
            up_hbm.at[chunk_rows(j)], grad.at[chunk_rows(j)], gp_send.at[j], gp_recv.at[j],
            jnp.maximum(s - 1, 0), d,
        )

    def exit_copy(j):
        return pltpu.make_async_copy(exit_hbm.at[chunk_rows(j)], grad.at[chunk_rows(j)], gp_recv.at[j])

    stage_copy.wait()
    pl.semaphore_wait(
        barrier,
        1 + jnp.minimum(q, 1) + jnp.minimum(last - q, 1) + jnp.minimum(s, 1) + jnp.minimum(sections - 1 - s, 1),
    )

    @pl.when(s < sections - 1)
    def _():
        for h in range(H):
            late_copy(h).start()

    @pl.when(s == 0)
    def _():
        for h in range(H):
            entry_copy(h).start()

    @pl.when(s > 0)
    def _():
        for j in range(steps):
            grad_copy(j).start()

    @pl.when(s == sections - 1)
    def _():
        for j in range(steps):
            exit_copy(j).start()

    def source(way, k):
        return jnp.maximum(q - k, 0) if way == 0 else jnp.minimum(q + k, last)

    def have(way, k):
        return hops[way] >= k

    def hop(way, k, h):
        piece = lbuf.at[h, source(way, k) * 2 + c]
        return remote(piece, piece, ag_s.at[way, k, h], ag_r.at[way, k, h], s, nxt[way])

    def arrival(way, k, h):
        piece = lbuf.at[h, source(way, k) * 2 + c]
        return remote(piece, piece, ag_s.at[way, k - 1, h], ag_r.at[way, k - 1, h], s, nxt[way])

    def share(way, k, h, lane):
        piece = lbuf.at[h, source(way, k) * 2 + lane]
        return remote(piece, piece, agp_s.at[way, k, h], agp_r.at[way, k, h], s, partner)

    def own(h):
        @pl.when(s == 0)
        def _():
            entry_copy(h).wait()

        @pl.when(s > 0)
        def _():
            late_copy(h).wait_recv()

        for way in range(2):
            @pl.when(has_next[way])
            def _():
                hop(way, 0, h).start()
        share(0, 0, h, c).start()

    def relay(k, h):
        for way in range(2):
            @pl.when(have(way, k))
            def _():
                arrival(way, k, h).wait_recv()
                if k < last:
                    @pl.when(has_next[way])
                    def _():
                        hop(way, k, h).start()
                share(way, k, h, c).start()

    def gathered(h):
        share(0, 0, h, other).wait_recv()
        for k in range(1, Q):
            for way in range(2):
                @pl.when(have(way, k))
                def _():
                    share(way, k, h, other).wait_recv()

    def gather_drain():
        for h in range(H):
            share(0, 0, h, c).wait_send()
            for way in range(2):
                @pl.when(has_next[way])
                def _():
                    hop(way, 0, h).wait_send()
                for k in range(1, Q):
                    @pl.when(have(way, k))
                    def _():
                        share(way, k, h, c).wait_send()
                        if k < last:
                            @pl.when(has_next[way])
                            def _():
                                hop(way, k, h).wait_send()

    def forward(j):
        at = chunk_rows(j)
        pre = dot(saved[at], eexp[...])
        u = 0.5 * pre
        bent = jnp.tanh(u)
        sigma = 0.5 * bent + 0.5
        value = u * bent + u
        act[at] = value.astype(BF16)
        dsl[at] = (sigma * (1.0 + pre - value)).astype(BF16)

    def backward(j):
        at = chunk_rows(j)

        @pl.when(s < sections - 1)
        def _():
            grad_copy(j).wait_recv()

        @pl.when(s == sections - 1)
        def _():
            exit_copy(j).wait()

        back = dot(grad[at], ered[...], 1, 1)
        slope[at] = (back * dsl[at].astype(F32)).astype(BF16)

    def downward(j):
        at = chunk_rows(j)
        input_grad[at] = (grad[at].astype(F32) + dot(slope[at], eexp[...], 1, 1)).astype(BF16)

    def weight_sums(which, lo, hi):
        at = pl.ds(lo * chunk, (hi - lo) * chunk)
        a, b = ((saved, slope), (grad, act))[which]
        for n in range(wide // 256):
            col = pl.ds(n * 256, 256)
            value = dot(a[at], b[at, col], 0, 0).reshape(pieces, depth, 256)
            if lo > 0:
                value += gsum[which, :, :, col]
            gsum[which, :, :, col] = value

    local[0].wait()
    local[1].wait()
    early = max(steps // 2, 1)
    for j in range(early):
        forward(j)
    for dev in range(n_dev):
        first[pl.ds((dev + 1) * padded - 16, 16), :] = jnp.zeros((16, first.shape[1]), BF16)
    for way in range(2):
        @pl.when(hops[way] == 0)
        def _():
            wrx[way] = jnp.zeros(wrx.shape[1:], BF16)
            rx[way] = jnp.zeros(rx.shape[1:], BF16)
    for h in range(H):
        own(h)
        if early + h < steps:
            forward(early + h)
    for j in range(early + H, steps):
        forward(j)
    local[2].wait()
    local[3].wait()
    local[4].wait()

    def activate(h):
        total = jnp.zeros((1, half), F32)
        squares = jnp.zeros((1, half), F32)
        for dev in range(n_dev):
            v = lbuf[h, dev].astype(F32)
            total += jnp.sum(v, axis=0, keepdims=True)
            squares += jnp.sum(v * v, axis=0, keepdims=True)
        spread, offset = affine(total, squares, total_rows, gain1[:, cols(h)], shift1[:, cols(h)])
        for dev in range(n_dev):
            v = scaled_silu(lbuf[h, dev].astype(F32), spread, offset)
            first[pl.ds(dev * padded, rows), cols(h)] = v.astype(BF16)

    width = min(256, hid)

    def expand(h):
        for n in range(hid // width):
            at = pl.ds(n * width, width)
            if split:
                value = dot(first[:, cols(h)], wexp[cols(h), at])
                if h > 0:
                    value += inner[:, at]
                if h < H - 1:
                    inner[:, at] = value
            elif h == H - 1:
                value = dot(first[...], wexp[:, at])
            if h == H - 1:
                spread, offset = affine(
                    jnp.sum(value, axis=0, keepdims=True),
                    jnp.sum(value * value, axis=0, keepdims=True),
                    total_rows, gain2[:, at], shift2[:, at],
                )
                hidden[:, at] = scaled_silu(value, spread, offset).astype(BF16)

    done = 0
    ready = min(2, steps - 1)
    for k in range(1, last):
        for h in range(H):
            relay(k, h)
            if k == last - 1 and h in (1, 2) and done < ready:
                backward(done)
                downward(done)
                done += 1
    weight_sums(0, 0, done)
    for h in range(H):
        relay(last, h)
        if h == 0 and done < steps - 1:
            backward(done)
            done += 1
        if h > 0:
            gathered(h - 1)
            activate(h - 1)
            expand(h - 1)
    gathered(H - 1)
    activate(H - 1)
    expand(H - 1)

    def pair_copy(h):
        return remote(part.at[other, h], prx.at[h], px_s.at[h], px_r.at[h], s, partner)

    far = last * H

    def mine(h, chip):
        return part[c, h, chip].astype(F32) + prx[h, chip].astype(F32)

    def goal(way, m):
        return last - m if way == 0 else m

    def row_hop(way, r):
        m, h = r // H, lax.rem(r, H)
        to = goal(way, m)
        i = r + pieces * jnp.minimum(m, 1)
        return remote(part.at[c, h, to], rx.at[way, h, to], st_s.at[way, i], st_r.at[way, i], s, nxt[way])

    def row_start(way, r):
        m, h = r // H, lax.rem(r, H)
        to = goal(way, m)
        part[c, h, to] = mine(h, to).astype(BF16)
        row_hop(way, r).start()

    def row_relay(way, r):
        m, h = r // H, lax.rem(r, H)
        to = goal(way, m)

        @pl.when(last - m >= hops[way])
        def _():
            row_hop(way, r).wait_recv()

        @pl.when(last - m > hops[way])
        def _():
            part[c, h, to] = (mine(h, to) + rx[way, h, to].astype(F32)).astype(BF16)
            row_hop(way, r).start()

    def each(lo, hi, body):
        def step(i, carry):
            body(i)
            return carry
        lax.fori_loop(lo, hi, step, 0)

    def scatter(h):
        pair_copy(h).wait_recv()
        for way in range(2):
            @pl.when(hops[way] == 0)
            def _():
                row_start(way, h)

    tile = min(256, half)
    for h in range(H):
        for n in range(half // tile):
            value = dot(hidden[...], wred[:, pl.ds(h * half + n * tile, tile)]).astype(BF16)
            for dev in range(n_dev):
                part[dev % 2, h, dev // 2, :, pl.ds(n * tile, tile)] = value[dev * padded:dev * padded + rows]
        pair_copy(h).start()
        if h > 0:
            scatter(h - 1)

    def gx(i):
        return remote(gtx.at[i], gprx.at[i], gx_s.at[i], gx_r.at[i], s, partner)

    def exchange(which):
        @pl.when(other == which)
        def _():
            for i in range(pieces):
                gtx[i] = gsum[which, i].astype(BF16)
                gx(i).start()

    counted = ready
    backward(done)
    scatter(H - 1)
    for j in range(done + 1, steps):
        backward(j)
    weight_sums(1, 0, steps)
    exchange(1)
    weight_sums(0, counted, steps)
    exchange(0)
    for h in range(H):
        for way in range(2):
            @pl.when(hops[way] == 1)
            def _():
                row_relay(way, h)

    def term(i):
        return gsum[c, i] + gprx[i].astype(F32)

    def sum_hop(way, i):
        return remote(wtx.at[way, i], wrx.at[way, i], st_s.at[way, H + i], st_r.at[way, H + i], s, nxt[way])

    def sum_first(i):
        gx(i).wait_recv()
        for way in range(2):
            @pl.when(hops[way] == 0)
            def _():
                wtx[way, i] = term(i).astype(BF16)
                sum_hop(way, i).start()

    def sum_relay(way, i):
        sum_hop(way, i).wait_recv()

        @pl.when(has_next[way])
        def _():
            wtx[way, i] = (term(i) + wrx[way, i].astype(F32)).astype(BF16)
            sum_hop(way, i).start()

    def give(i, lane):
        return remote(gout.at[lane, i], gout.at[lane, i], wp_s.at[i], wp_r.at[i], s, partner)

    def sum_finish(i):
        value = term(i) + (wrx[0, i].astype(F32) + wrx[1, i].astype(F32))
        gout[c, i] = (value * factor).astype(BF16)
        give(i, c).start()

    each(0, pieces, sum_first)

    def rest(r):
        for way in range(2):
            @pl.when(hops[way] == 0)
            def _():
                row_start(way, r)

    each(H, far, rest)
    for j in range(counted, steps):
        downward(j)

    count = far + pieces
    farther = jnp.maximum(hops[0], hops[1])

    def slot(t):
        for way in range(2):
            i = t - SKEW * hops[way]
            live = hops[way] > 0

            @pl.when(both(hops[way] > 1, both(i >= 0, i < H)))
            def _():
                row_relay(way, i)

            @pl.when(both(live, both(i >= H, i < H + pieces)))
            def _():
                sum_relay(way, i - H)

            @pl.when(both(live, both(i >= H + pieces, i < count)))
            def _():
                row_relay(way, i - pieces)

        i = t - SKEW * farther - H

        @pl.when(both(i >= 0, i < pieces))
        def _():
            sum_finish(i)

    @pl.when(s < sections - 1)
    def _():
        for h in range(H):
            late_copy(h).wait_send()

    @pl.when(s > 0)
    def _():
        for j in range(steps):
            grad_copy(j).wait_send()

    gather_drain()
    for h in range(H):
        pair_copy(h).wait_send()

    each(SKEW, count + SKEW * last, slot)

    for h in range(H):
        value = mine(h, q) + rx[0, h, q].astype(F32) + rx[1, h, q].astype(F32)
        late_out[:, cols(h)] = (lbuf[h, d].astype(F32) + value).astype(BF16)

    def drain_rows(r):
        for way in range(2):
            @pl.when(last - r // H > hops[way])
            def _():
                row_hop(way, r).wait_send()

    each(0, far, drain_rows)

    def drain_sums(i):
        gx(i).wait_send()
        give(i, c).wait_send()
        for way in range(2):
            @pl.when(has_next[way])
            def _():
                sum_hop(way, i).wait_send()

    each(0, pieces, drain_sums)
    for i in range(pieces):
        give(i, other).wait_recv()


def finish(late_in, grad_in, sums, late_out, input_grad, gexp, gred, wide_e, wide_r, sem):
    ce, fe = wide_e.shape
    a = pltpu.make_async_copy(grad_in, input_grad.at[0], sem.at[0])
    b = pltpu.make_async_copy(late_in, late_out.at[0], sem.at[1])
    a.start()
    b.start()
    wide_e[...] = sums[0].reshape(ce, fe).astype(F32)
    x = pltpu.make_async_copy(wide_e, gexp.at[0], sem.at[2])
    x.start()
    for n in range(fe // 256):
        at = pl.ds(n * 256, 256)
        wide_r[at, :] = sums[1, :, :, at].reshape(ce, 256).astype(F32).T
    y = pltpu.make_async_copy(wide_r, gred.at[0], sem.at[3])
    y.start()
    for copy in (a, b, x, y):
        copy.wait()


def shards(
    sections, n_dev,
    late_sent, entry_rows, gain_first, shift_first, expand_late, gain_inner, shift_inner,
    reduce_late, early_saved, upstream_grad, exit_grad, expand_early, reduce_early,
):
    rows, cl = entry_rows.shape
    e_rows, ce = exit_grad.shape
    fe = expand_early.shape[2]
    hid = expand_late.shape[2]
    Q = n_dev // 2
    half = cl // H
    padded = -(-rows // 16) * 16
    chunk = max(k for k in range(16, 257, 16) if e_rows % k == 0)
    steps = e_rows // chunk
    pieces = ce // 32
    depth = ce // pieces
    count = (Q - 1) * H + pieces
    split = n_dev * padded * hid * 4 <= 4 * 1024 * 1024
    hbm = pl.BlockSpec(memory_space=pltpu.HBM)
    any_spec = pl.BlockSpec(memory_space=pl.ANY)
    vm = pl.BlockSpec(memory_space=pltpu.VMEM)
    V = pltpu.VMEM
    dma = pltpu.SemaphoreType.DMA
    late_out, input_grad, sums = pl.pallas_call(
        functools.partial(kernel, sections, n_dev, chunk, split),
        out_shape=(
            V((rows, cl), BF16),
            V((e_rows, ce), BF16),
            V((2, pieces, depth, fe), BF16),
        ),
        in_specs=[hbm, hbm, vm, vm, hbm, vm, vm] + [hbm] * 6,
        out_specs=(vm, vm, vm),
        scratch_shapes=[
            V((rows, cl), BF16),
            V((H, n_dev, rows, half), BF16),
            V((n_dev * padded, cl), BF16),
            V((n_dev * padded, hid) if split else (8, 128), F32),
            V((n_dev * padded, hid), BF16),
            V((2, H, Q, rows, half), BF16),
            V((H, Q, rows, half), BF16),
            V((2, H, Q, rows, half), BF16),
            V((cl, hid), BF16),
            V((hid, cl), BF16),
            V((e_rows, ce), BF16),
            V((e_rows, ce), BF16),
            V((ce, fe), BF16),
            V((fe, ce), BF16),
            V((e_rows, fe), BF16),
            V((e_rows, fe), BF16),
            V((e_rows, fe), BF16),
            V((2, pieces, depth, fe), F32),
            V((pieces, depth, fe), BF16),
            V((pieces, depth, fe), BF16),
            V((2, pieces, depth, fe), BF16),
            V((2, pieces, depth, fe), BF16),
            dma((6,)), dma((H,)), dma((H,)), dma((steps,)), dma((steps,)),
            dma((2, Q - 1, H)), dma((2, Q - 1, H)), dma((2, Q, H)), dma((2, Q, H)),
            dma((H,)), dma((H,)), dma((pieces,)), dma((pieces,)),
            dma((2, count)), dma((2, count)), dma((pieces,)), dma((pieces,)),
        ],
        compiler_params=pltpu.CompilerParams(
            collective_id=0, has_side_effects=True, vmem_limit_bytes=60 * 1024 * 1024
        ),
        name="relay",
    )(
        late_sent[0], entry_rows, gain_first, shift_first, expand_late[0], gain_inner, shift_inner,
        reduce_late[0], early_saved[0], upstream_grad[0], exit_grad, expand_early[0], reduce_early[0],
    )
    return pl.pallas_call(
        finish,
        out_shape=(
            jax.ShapeDtypeStruct((1, rows, cl), BF16),
            jax.ShapeDtypeStruct((1, e_rows, ce), BF16),
            jax.ShapeDtypeStruct((1, ce, fe), F32),
            jax.ShapeDtypeStruct((1, fe, ce), F32),
        ),
        in_specs=[vm, vm, vm],
        out_specs=(any_spec,) * 4,
        scratch_shapes=[V((ce, fe), F32), V((fe, ce), F32), dma((4,))],
        compiler_params=pltpu.CompilerParams(vmem_limit_bytes=16 * 1024 * 1024),
        name="finish",
    )(late_out, input_grad, sums)


def solution(mesh):
    sections, n_dev = mesh.shape["section"], mesh.shape["dev"]
    sd, dd = P("section", "dev", None), P("dev", None)
    rep, one = P("section", None, None), P("section", None)
    in_specs = (
        sd, dd, one, one, P("section", None, "dev"), P("section", "dev"), P("section", "dev"),
        sd, sd, sd, dd, rep, rep,
    )
    return jax.shard_map(
        functools.partial(shards, sections, n_dev), mesh=mesh, in_specs=in_specs,
        out_specs=(sd, sd, rep, rep), check_vma=False,
    )
```

```python
import functools
import math

import jax
import jax.numpy as jnp
from jax import lax
from jax.experimental import pallas as pl
from jax.experimental.pallas import tpu as pltpu
from jax.sharding import PartitionSpec as P

MESH = pl.DeviceIdType.MESH
epsilon = 1e-05
H = 4
SKEW = 3
LEAD = 2
F32 = jnp.float32
BF16 = jnp.bfloat16


def scaled_silu(x, spread, offset):
    u = x * (0.5 * spread) + 0.5 * offset
    return u * jnp.tanh(u) + u


def affine(sums, squares, count, gain, shift):
    average = sums / count
    second = squares / count
    spread = gain * lax.rsqrt(second - average * average + epsilon)
    return spread, shift - average * spread


def dot(a, b, ca=1, cb=0):
    return lax.dot_general(a, b, (((ca,), (cb,)), ((), ())), preferred_element_type=F32)


def both(a, b):
    return jnp.logical_and(a, b)


def kernel(
    sections, n_dev, chunk, split,
    late_hbm, entry_hbm, gain1, shift1, wexp_hbm, gain2, shift2, wred_hbm,
    saved_hbm, up_hbm, exit_hbm, eexp_hbm, ered_hbm,
    late_out, input_grad, gout,
    stage, lbuf, first, inner, hidden, part, prx, rx,
    wexp, wred, saved, grad, eexp, ered, act, dsl, slope,
    gsum, gtx, gprx, wtx, wrx,
    loc_sem, perm_send, perm_recv, gp_send, gp_recv,
    ag_s, ag_r, agp_s, agp_r, px_s, px_r, gx_s, gx_r, st_s, st_r, wp_s, wp_r,
):
    Q = n_dev // 2
    s = lax.axis_index("section")
    d = lax.axis_index("dev")
    q = d // 2
    c = lax.rem(d, 2)
    other = 1 - c
    partner = q * 2 + other
    rows = late_hbm.shape[0]
    half = late_hbm.shape[1] // H
    padded = first.shape[0] // n_dev
    e_rows = saved_hbm.shape[0]
    steps = e_rows // chunk
    total_rows = rows * n_dev
    hid = wexp.shape[1]
    wide = eexp.shape[1]
    pieces, depth = gsum.shape[1], gsum.shape[2]
    ce = grad.shape[1]
    front = pieces // 2
    ahead = front * depth
    factor = 1.0 / math.sqrt(e_rows * n_dev)

    last = Q - 1
    right, left = jnp.minimum(q + 1, last), jnp.maximum(q - 1, 0)
    nxt = (right * 2 + c, left * 2 + c)
    has_next = (q < last, q > 0)
    has_prev = (q > 0, q < last)
    hops = (q, last - q)

    barrier = pltpu.get_barrier_semaphore()
    pl.semaphore_signal(barrier, inc=1, device_id=(s, partner), device_id_type=MESH)
    for way in range(2):
        @pl.when(has_next[way])
        def _():
            pl.semaphore_signal(barrier, inc=1, device_id=(s, nxt[way]), device_id_type=MESH)

    @pl.when(s > 0)
    def _():
        pl.semaphore_signal(barrier, inc=1, device_id=(s - 1, d), device_id_type=MESH)

    @pl.when(s < sections - 1)
    def _():
        pl.semaphore_signal(barrier, inc=1, device_id=(s + 1, d), device_id_type=MESH)

    stage_copy = pltpu.make_async_copy(late_hbm, stage, loc_sem.at[5])
    stage_copy.start()
    local = [
        pltpu.make_async_copy(src, dst, loc_sem.at[i])
        for i, (src, dst) in enumerate(
            ((saved_hbm, saved), (eexp_hbm, eexp), (ered_hbm, ered), (wexp_hbm, wexp), (wred_hbm, wred))
        )
    ]
    for copy in local:
        copy.start()

    def remote(src, dst, send, recv, section, dev):
        return pltpu.make_async_remote_copy(
            src_ref=src, dst_ref=dst, send_sem=send, recv_sem=recv,
            device_id=(section, dev), device_id_type=MESH,
        )

    def cols(h):
        return pl.ds(h * half, half)

    def late_copy(h):
        return remote(
            stage.at[:, cols(h)], lbuf.at[h, d], perm_send.at[h], perm_recv.at[h],
            jnp.minimum(s + 1, sections - 1), d,
        )

    def entry_copy(h):
        return pltpu.make_async_copy(entry_hbm.at[:, cols(h)], lbuf.at[h, d], perm_recv.at[h])

    def chunk_rows(j):
        return pl.ds(j * chunk, chunk)

    def grad_at(j):
        if j == steps:
            return slice(None), pl.ds(0, ahead)
        return chunk_rows(j), pl.ds(ahead, ce - ahead)

    def grad_copy(j):
        return remote(
            up_hbm.at[grad_at(j)], grad.at[grad_at(j)], gp_send.at[j], gp_recv.at[j],
            jnp.maximum(s - 1, 0), d,
        )

    def exit_copy(j):
        return pltpu.make_async_copy(exit_hbm.at[grad_at(j)], grad.at[grad_at(j)], gp_recv.at[j])

    def grad_wait(j):
        @pl.when(s < sections - 1)
        def _():
            grad_copy(j).wait_recv()

        @pl.when(s == sections - 1)
        def _():
            exit_copy(j).wait()

    stage_copy.wait()
    pl.semaphore_wait(
        barrier,
        1 + jnp.minimum(q, 1) + jnp.minimum(last - q, 1) + jnp.minimum(s, 1) + jnp.minimum(sections - 1 - s, 1),
    )

    @pl.when(s < sections - 1)
    def _():
        for h in range(H):
            late_copy(h).start()

    @pl.when(s == 0)
    def _():
        for h in range(H):
            entry_copy(h).start()

    @pl.when(s > 0)
    def _():
        for j in (steps, *range(steps)):
            grad_copy(j).start()

    @pl.when(s == sections - 1)
    def _():
        for j in (steps, *range(steps)):
            exit_copy(j).start()

    def source(way, k):
        return jnp.maximum(q - k, 0) if way == 0 else jnp.minimum(q + k, last)

    def have(way, k):
        return hops[way] >= k

    def hop(way, k, h):
        piece = lbuf.at[h, source(way, k) * 2 + c]
        return remote(piece, piece, ag_s.at[way, k, h], ag_r.at[way, k, h], s, nxt[way])

    def arrival(way, k, h):
        piece = lbuf.at[h, source(way, k) * 2 + c]
        return remote(piece, piece, ag_s.at[way, k - 1, h], ag_r.at[way, k - 1, h], s, nxt[way])

    def share(way, k, h, lane):
        piece = lbuf.at[h, source(way, k) * 2 + lane]
        return remote(piece, piece, agp_s.at[way, k, h], agp_r.at[way, k, h], s, partner)

    def own(h):
        @pl.when(s == 0)
        def _():
            entry_copy(h).wait()

        @pl.when(s > 0)
        def _():
            late_copy(h).wait_recv()

        for way in range(2):
            @pl.when(has_next[way])
            def _():
                hop(way, 0, h).start()
        share(0, 0, h, c).start()

    def relay(k, h):
        for way in range(2):
            @pl.when(have(way, k))
            def _():
                arrival(way, k, h).wait_recv()
                if k < last:
                    @pl.when(has_next[way])
                    def _():
                        hop(way, k, h).start()
                share(way, k, h, c).start()

    def gathered(h):
        share(0, 0, h, other).wait_recv()
        for k in range(1, Q):
            for way in range(2):
                @pl.when(have(way, k))
                def _():
                    share(way, k, h, other).wait_recv()

    def gather_drain():
        for h in range(H):
            share(0, 0, h, c).wait_send()
            for way in range(2):
                @pl.when(has_next[way])
                def _():
                    hop(way, 0, h).wait_send()
                for k in range(1, Q):
                    @pl.when(have(way, k))
                    def _():
                        share(way, k, h, c).wait_send()
                        if k < last:
                            @pl.when(has_next[way])
                            def _():
                                hop(way, k, h).wait_send()

    def forward(j):
        at = chunk_rows(j)
        pre = dot(saved[at], eexp[...])
        u = 0.5 * pre
        bent = jnp.tanh(u)
        sigma = 0.5 * bent + 0.5
        value = u * bent + u
        act[at] = value.astype(BF16)
        dsl[at] = (sigma * (1.0 + pre - value)).astype(BF16)

    def backward(j):
        at = chunk_rows(j)
        grad_wait(j)
        back = dot(grad[at], ered[...], 1, 1)
        slope[at] = (back * dsl[at].astype(F32)).astype(BF16)

    def downward(j):
        at = chunk_rows(j)
        input_grad[at] = (grad[at].astype(F32) + dot(slope[at], eexp[...], 1, 1)).astype(BF16)

    def weight_sums(which, lo, hi):
        a, b = ((saved, slope), (grad, act))[which]
        at = pl.ds(lo * depth, (hi - lo) * depth)
        for n in range(wide // 256):
            col = pl.ds(n * 256, 256)
            gsum[which, lo:hi, :, col] = dot(a[:, at], b[:, col], 0, 0).reshape(hi - lo, depth, 256)

    local[0].wait()
    local[1].wait()
    early = max(steps // 2, 1)
    for j in range(early):
        forward(j)
    for dev in range(n_dev):
        first[pl.ds((dev + 1) * padded - 16, 16), :] = jnp.zeros((16, first.shape[1]), BF16)
    for way in range(2):
        @pl.when(hops[way] == 0)
        def _():
            wrx[way] = jnp.zeros(wrx.shape[1:], BF16)
            rx[way] = jnp.zeros(rx.shape[1:], BF16)
    for h in range(H):
        own(h)
        if early + h < steps:
            forward(early + h)
    for j in range(early + H, steps):
        forward(j)
    local[2].wait()
    local[3].wait()
    local[4].wait()

    def activate(h):
        total = jnp.zeros((1, half), F32)
        squares = jnp.zeros((1, half), F32)
        for dev in range(n_dev):
            v = lbuf[h, dev].astype(F32)
            total += jnp.sum(v, axis=0, keepdims=True)
            squares += jnp.sum(v * v, axis=0, keepdims=True)
        spread, offset = affine(total, squares, total_rows, gain1[:, cols(h)], shift1[:, cols(h)])
        for dev in range(n_dev):
            v = scaled_silu(lbuf[h, dev].astype(F32), spread, offset)
            first[pl.ds(dev * padded, rows), cols(h)] = v.astype(BF16)

    width = min(256, hid)

    def expand(h):
        for n in range(hid // width):
            at = pl.ds(n * width, width)
            if split:
                value = dot(first[:, cols(h)], wexp[cols(h), at])
                if h > 0:
                    value += inner[:, at]
                if h < H - 1:
                    inner[:, at] = value
            elif h == H - 1:
                value = dot(first[...], wexp[:, at])
            if h == H - 1:
                spread, offset = affine(
                    jnp.sum(value, axis=0, keepdims=True),
                    jnp.sum(value * value, axis=0, keepdims=True),
                    total_rows, gain2[:, at], shift2[:, at],
                )
                hidden[:, at] = scaled_silu(value, spread, offset).astype(BF16)

    def gx(i):
        return remote(gtx.at[i], gprx.at[i], gx_s.at[i], gx_r.at[i], s, partner)

    def exchange(which, lo, hi):
        @pl.when(other == which)
        def _():
            for i in range(lo, hi):
                gtx[i] = gsum[which, i].astype(BF16)
                gx(i).start()

    def term(i):
        return gsum[c, i] + gprx[i].astype(F32)

    def sum_hop(way, i):
        at = far + i
        return remote(wtx.at[way, i], wrx.at[way, i], st_s.at[way, at], st_r.at[way, at], s, nxt[way])

    def sum_first(i):
        gx(i).wait_recv()
        for way in range(2):
            @pl.when(hops[way] == 0)
            def _():
                wtx[way, i] = term(i).astype(BF16)
                sum_hop(way, i).start()

    def sum_relay(way, i):
        sum_hop(way, i).wait_recv()

        @pl.when(has_next[way])
        def _():
            wtx[way, i] = (term(i) + wrx[way, i].astype(F32)).astype(BF16)
            sum_hop(way, i).start()

    def each(lo, hi, body):
        def step(i, carry):
            body(i)
            return carry
        lax.fori_loop(lo, hi, step, 0)

    far = last * H
    lead = min(H + LEAD, far)
    for k in range(1, last):
        for h in range(H):
            relay(k, h)
    for h in range(H):
        relay(last, h)
        if h == H - 1:
            grad_wait(steps)
            weight_sums(1, 0, front)
            exchange(1, 0, front)
        if h > 0:
            gathered(h - 1)
            activate(h - 1)
            expand(h - 1)
    gathered(H - 1)
    activate(H - 1)
    expand(H - 1)

    @pl.when(c == 1)
    def _():
        each(0, front, sum_first)

    def pair_copy(h):
        return remote(part.at[other, h], prx.at[h], px_s.at[h], px_r.at[h], s, partner)

    def mine(h, chip):
        return part[c, h, chip].astype(F32) + prx[h, chip].astype(F32)

    def goal(way, m):
        return last - m if way == 0 else m

    def row_hop(way, r):
        m, h = r // H, lax.rem(r, H)
        to = goal(way, m)
        return remote(part.at[c, h, to], rx.at[way, h, to], st_s.at[way, r], st_r.at[way, r], s, nxt[way])

    def row_start(way, r):
        m, h = r // H, lax.rem(r, H)
        to = goal(way, m)
        part[c, h, to] = mine(h, to).astype(BF16)
        row_hop(way, r).start()

    def row_relay(way, r):
        m, h = r // H, lax.rem(r, H)
        to = goal(way, m)

        @pl.when(last - m >= hops[way])
        def _():
            row_hop(way, r).wait_recv()

        @pl.when(last - m > hops[way])
        def _():
            part[c, h, to] = (mine(h, to) + rx[way, h, to].astype(F32)).astype(BF16)
            row_hop(way, r).start()

    def scatter(h):
        pair_copy(h).wait_recv()
        for way in range(2):
            @pl.when(hops[way] == 0)
            def _():
                row_start(way, h)

    tile = min(256, half)
    for h in range(H):
        for n in range(half // tile):
            value = dot(hidden[...], wred[:, pl.ds(h * half + n * tile, tile)]).astype(BF16)
            for dev in range(n_dev):
                part[dev % 2, h, dev // 2, :, pl.ds(n * tile, tile)] = value[dev * padded:dev * padded + rows]
        pair_copy(h).start()
        if h < steps:
            backward(h)
        if h > 0:
            scatter(h - 1)

    def rest(r):
        for way in range(2):
            @pl.when(hops[way] == 0)
            def _():
                row_start(way, r)

    scatter(H - 1)
    each(H, lead, rest)
    for j in range(H, steps):
        backward(j)
    weight_sums(1, front, pieces)
    exchange(1, front, pieces)
    for way in range(2):
        @pl.when(both(c == 1, hops[way] == 1))
        def _():
            for i in range(front):
                sum_relay(way, i)
    weight_sums(0, 0, pieces)
    exchange(0, 0, pieces)
    for h in range(H):
        for way in range(2):
            @pl.when(hops[way] == 1)
            def _():
                row_relay(way, h)

    def give(i, lane):
        return remote(gout.at[lane, i], gout.at[lane, i], wp_s.at[i], wp_r.at[i], s, partner)

    def sum_finish(i):
        value = term(i) + (wrx[0, i].astype(F32) + wrx[1, i].astype(F32))
        gout[c, i] = (value * factor).astype(BF16)
        give(i, c).start()

    @pl.when(c == 0)
    def _():
        each(0, front, sum_first)

    each(front, pieces, sum_first)
    each(lead, far, rest)
    for j in range(steps):
        downward(j)

    count = far + pieces
    farther = jnp.maximum(hops[0], hops[1])

    def slot(t):
        for way in range(2):
            i = t - SKEW * hops[way]
            moved = c * jnp.minimum(hops[way], 1) * (2 - jnp.minimum(hops[way], 2))
            live = hops[way] > 0

            @pl.when(both(live, both(i >= H * (2 - jnp.minimum(hops[way], 2)), i < lead)))
            def _():
                row_relay(way, i)

            @pl.when(both(live, both(i >= lead + front * moved, i < lead + pieces)))
            def _():
                sum_relay(way, i - lead)

            @pl.when(both(live, both(i >= lead + pieces, i < count)))
            def _():
                row_relay(way, i - pieces)

        i = t - SKEW * farther - lead

        @pl.when(both(i >= 0, i < pieces))
        def _():
            sum_finish(i)

    @pl.when(s < sections - 1)
    def _():
        for h in range(H):
            late_copy(h).wait_send()

    @pl.when(s > 0)
    def _():
        for j in range(steps + 1):
            grad_copy(j).wait_send()

    gather_drain()
    for h in range(H):
        pair_copy(h).wait_send()

    each(SKEW, count + SKEW * last, slot)

    for h in range(H):
        value = mine(h, q) + rx[0, h, q].astype(F32) + rx[1, h, q].astype(F32)
        late_out[:, cols(h)] = (lbuf[h, d].astype(F32) + value).astype(BF16)

    def drain_rows(r):
        for way in range(2):
            @pl.when(last - r // H > hops[way])
            def _():
                row_hop(way, r).wait_send()

    each(0, far, drain_rows)

    def drain_sums(i):
        gx(i).wait_send()
        give(i, c).wait_send()
        for way in range(2):
            @pl.when(has_next[way])
            def _():
                sum_hop(way, i).wait_send()

    each(0, pieces, drain_sums)
    for i in range(pieces):
        give(i, other).wait_recv()


def finish(late_in, grad_in, sums, late_out, input_grad, gexp, gred, wide_e, wide_r, sem):
    ce, fe = wide_e.shape
    a = pltpu.make_async_copy(grad_in, input_grad.at[0], sem.at[0])
    b = pltpu.make_async_copy(late_in, late_out.at[0], sem.at[1])
    a.start()
    b.start()
    wide_e[...] = sums[0].reshape(ce, fe).astype(F32)
    x = pltpu.make_async_copy(wide_e, gexp.at[0], sem.at[2])
    x.start()
    for n in range(fe // 256):
        at = pl.ds(n * 256, 256)
        wide_r[at, :] = sums[1, :, :, at].reshape(ce, 256).astype(F32).T
    y = pltpu.make_async_copy(wide_r, gred.at[0], sem.at[3])
    y.start()
    for copy in (a, b, x, y):
        copy.wait()


def shards(
    sections, n_dev,
    late_sent, entry_rows, gain_first, shift_first, expand_late, gain_inner, shift_inner,
    reduce_late, early_saved, upstream_grad, exit_grad, expand_early, reduce_early,
):
    rows, cl = entry_rows.shape
    e_rows, ce = exit_grad.shape
    fe = expand_early.shape[2]
    hid = expand_late.shape[2]
    Q = n_dev // 2
    half = cl // H
    padded = -(-rows // 16) * 16
    chunk = max(k for k in range(16, 257, 16) if e_rows % k == 0)
    steps = e_rows // chunk
    pieces = ce // 32
    depth = ce // pieces
    count = (Q - 1) * H + pieces
    split = n_dev * padded * hid * 4 <= 4 * 1024 * 1024
    hbm = pl.BlockSpec(memory_space=pltpu.HBM)
    any_spec = pl.BlockSpec(memory_space=pl.ANY)
    vm = pl.BlockSpec(memory_space=pltpu.VMEM)
    V = pltpu.VMEM
    dma = pltpu.SemaphoreType.DMA
    late_out, input_grad, sums = pl.pallas_call(
        functools.partial(kernel, sections, n_dev, chunk, split),
        out_shape=(
            V((rows, cl), BF16),
            V((e_rows, ce), BF16),
            V((2, pieces, depth, fe), BF16),
        ),
        in_specs=[hbm, hbm, vm, vm, hbm, vm, vm] + [hbm] * 6,
        out_specs=(vm, vm, vm),
        scratch_shapes=[
            V((rows, cl), BF16),
            V((H, n_dev, rows, half), BF16),
            V((n_dev * padded, cl), BF16),
            V((n_dev * padded, hid) if split else (8, 128), F32),
            V((n_dev * padded, hid), BF16),
            V((2, H, Q, rows, half), BF16),
            V((H, Q, rows, half), BF16),
            V((2, H, Q, rows, half), BF16),
            V((cl, hid), BF16),
            V((hid, cl), BF16),
            V((e_rows, ce), BF16),
            V((e_rows, ce), BF16),
            V((ce, fe), BF16),
            V((fe, ce), BF16),
            V((e_rows, fe), BF16),
            V((e_rows, fe), BF16),
            V((e_rows, fe), BF16),
            V((2, pieces, depth, fe), F32),
            V((pieces, depth, fe), BF16),
            V((pieces, depth, fe), BF16),
            V((2, pieces, depth, fe), BF16),
            V((2, pieces, depth, fe), BF16),
            dma((6,)), dma((H,)), dma((H,)), dma((steps + 1,)), dma((steps + 1,)),
            dma((2, Q - 1, H)), dma((2, Q - 1, H)), dma((2, Q, H)), dma((2, Q, H)),
            dma((H,)), dma((H,)), dma((pieces,)), dma((pieces,)),
            dma((2, count)), dma((2, count)), dma((pieces,)), dma((pieces,)),
        ],
        compiler_params=pltpu.CompilerParams(
            collective_id=0, has_side_effects=True, vmem_limit_bytes=60 * 1024 * 1024
        ),
        name="relay",
    )(
        late_sent[0], entry_rows, gain_first, shift_first, expand_late[0], gain_inner, shift_inner,
        reduce_late[0], early_saved[0], upstream_grad[0], exit_grad, expand_early[0], reduce_early[0],
    )
    return pl.pallas_call(
        finish,
        out_shape=(
            jax.ShapeDtypeStruct((1, rows, cl), BF16),
            jax.ShapeDtypeStruct((1, e_rows, ce), BF16),
            jax.ShapeDtypeStruct((1, ce, fe), F32),
            jax.ShapeDtypeStruct((1, fe, ce), F32),
        ),
        in_specs=[vm, vm, vm],
        out_specs=(any_spec,) * 4,
        scratch_shapes=[V((ce, fe), F32), V((fe, ce), F32), dma((4,))],
        compiler_params=pltpu.CompilerParams(vmem_limit_bytes=16 * 1024 * 1024),
        name="finish",
    )(late_out, input_grad, sums)


def solution(mesh):
    sections, n_dev = mesh.shape["section"], mesh.shape["dev"]
    sd, dd = P("section", "dev", None), P("dev", None)
    rep, one = P("section", None, None), P("section", None)
    in_specs = (
        sd, dd, one, one, P("section", None, "dev"), P("section", "dev"), P("section", "dev"),
        sd, sd, sd, dd, rep, rep,
    )
    return jax.shard_map(
        functools.partial(shards, sections, n_dev), mesh=mesh, in_specs=in_specs,
        out_specs=(sd, sd, rep, rep), check_vma=False,
    )
```

```python
import functools
import math

import jax
import jax.numpy as jnp
from jax import lax
from jax.experimental import pallas as pl
from jax.experimental.pallas import tpu as pltpu
from jax.sharding import PartitionSpec as P

MESH = pl.DeviceIdType.MESH
epsilon = 1e-05
H = 4
SKEW = 5
LEAD = 1
F32 = jnp.float32
BF16 = jnp.bfloat16


def scaled_silu(x, spread, offset):
    u = x * (0.5 * spread) + 0.5 * offset
    return u * jnp.tanh(u) + u


def affine(sums, squares, count, gain, shift):
    average = sums / count
    second = squares / count
    spread = gain * lax.rsqrt(second - average * average + epsilon)
    return spread, shift - average * spread


def dot(a, b, ca=1, cb=0):
    return lax.dot_general(a, b, (((ca,), (cb,)), ((), ())), preferred_element_type=F32)


def both(a, b):
    return jnp.logical_and(a, b)


def cuts(ce):
    pieces = ce // 16
    front = pieces // 2
    return pieces, front, (pieces - front) // 2 + pieces // 2


def kernel(
    sections, n_dev, chunk, split,
    late_hbm, entry_hbm, gain1, shift1, wexp_hbm, gain2, shift2, wred_hbm,
    saved_hbm, up_hbm, exit_hbm, eexp_hbm, ered_hbm,
    late_out, input_grad, gout,
    stage, lbuf, first, inner, hidden, part, prx, rx,
    wexp, wred, saved, grad, eexp, ered, act, dsl, slope,
    gsum, gtx, gprx, wtx, wrx,
    loc_sem, perm_send, perm_recv, gp_send, gp_recv,
    ag_s, ag_r, agp_s, agp_r, px_s, px_r, gx_s, gx_r, st_s, st_r, wp_s, wp_r,
):
    Q = n_dev // 2
    s = lax.axis_index("section")
    d = lax.axis_index("dev")
    q = d // 2
    c = lax.rem(d, 2)
    other = 1 - c
    partner = q * 2 + other
    rows = late_hbm.shape[0]
    half = late_hbm.shape[1] // H
    padded = first.shape[0] // n_dev
    e_rows = saved_hbm.shape[0]
    steps = e_rows // chunk
    total_rows = rows * n_dev
    hid = wexp.shape[1]
    wide = eexp.shape[1]
    ce = grad.shape[1]
    pieces, front, share = cuts(ce)
    depth = ce // pieces
    half_r, half_e = (pieces - front) // 2, pieces // 2
    ahead = front * depth
    factor = 1.0 / math.sqrt(e_rows * n_dev)

    last = Q - 1
    right, left = jnp.minimum(q + 1, last), jnp.maximum(q - 1, 0)
    nxt = (right * 2 + c, left * 2 + c)
    has_next = (q < last, q > 0)
    has_prev = (q > 0, q < last)
    hops = (q, last - q)

    barrier = pltpu.get_barrier_semaphore()
    pl.semaphore_signal(barrier, inc=1, device_id=(s, partner), device_id_type=MESH)
    for way in range(2):
        @pl.when(has_next[way])
        def _():
            pl.semaphore_signal(barrier, inc=1, device_id=(s, nxt[way]), device_id_type=MESH)

    @pl.when(s > 0)
    def _():
        pl.semaphore_signal(barrier, inc=1, device_id=(s - 1, d), device_id_type=MESH)

    @pl.when(s < sections - 1)
    def _():
        pl.semaphore_signal(barrier, inc=1, device_id=(s + 1, d), device_id_type=MESH)

    stage_copy = pltpu.make_async_copy(late_hbm, stage, loc_sem.at[5])
    stage_copy.start()
    local = [
        pltpu.make_async_copy(src, dst, loc_sem.at[i])
        for i, (src, dst) in enumerate(
            ((saved_hbm, saved), (eexp_hbm, eexp), (ered_hbm, ered), (wexp_hbm, wexp), (wred_hbm, wred))
        )
    ]
    for copy in local:
        copy.start()

    def remote(src, dst, send, recv, section, dev):
        return pltpu.make_async_remote_copy(
            src_ref=src, dst_ref=dst, send_sem=send, recv_sem=recv,
            device_id=(section, dev), device_id_type=MESH,
        )

    def cols(h):
        return pl.ds(h * half, half)

    def late_copy(h):
        return remote(
            stage.at[:, cols(h)], lbuf.at[h, d], perm_send.at[h], perm_recv.at[h],
            jnp.minimum(s + 1, sections - 1), d,
        )

    def entry_copy(h):
        return pltpu.make_async_copy(entry_hbm.at[:, cols(h)], lbuf.at[h, d], perm_recv.at[h])

    def chunk_rows(j):
        return pl.ds(j * chunk, chunk)

    def grad_at(j):
        if j == steps:
            return slice(None), pl.ds(0, ahead)
        return chunk_rows(j), pl.ds(ahead, ce - ahead)

    def grad_copy(j):
        return remote(
            up_hbm.at[grad_at(j)], grad.at[grad_at(j)], gp_send.at[j], gp_recv.at[j],
            jnp.maximum(s - 1, 0), d,
        )

    def exit_copy(j):
        return pltpu.make_async_copy(exit_hbm.at[grad_at(j)], grad.at[grad_at(j)], gp_recv.at[j])

    def grad_wait(j):
        @pl.when(s < sections - 1)
        def _():
            grad_copy(j).wait_recv()

        @pl.when(s == sections - 1)
        def _():
            exit_copy(j).wait()

    stage_copy.wait()
    pl.semaphore_wait(
        barrier,
        1 + jnp.minimum(q, 1) + jnp.minimum(last - q, 1) + jnp.minimum(s, 1) + jnp.minimum(sections - 1 - s, 1),
    )

    @pl.when(s < sections - 1)
    def _():
        for h in range(H):
            late_copy(h).start()

    @pl.when(s == 0)
    def _():
        for h in range(H):
            entry_copy(h).start()

    @pl.when(s > 0)
    def _():
        for j in (steps, *range(steps)):
            grad_copy(j).start()

    @pl.when(s == sections - 1)
    def _():
        for j in (steps, *range(steps)):
            exit_copy(j).start()

    def source(way, k):
        return jnp.maximum(q - k, 0) if way == 0 else jnp.minimum(q + k, last)

    def have(way, k):
        return hops[way] >= k

    def hop(way, k, h):
        piece = lbuf.at[h, source(way, k) * 2 + c]
        return remote(piece, piece, ag_s.at[way, k, h], ag_r.at[way, k, h], s, nxt[way])

    def arrival(way, k, h):
        piece = lbuf.at[h, source(way, k) * 2 + c]
        return remote(piece, piece, ag_s.at[way, k - 1, h], ag_r.at[way, k - 1, h], s, nxt[way])

    def lend(way, k, h, lane):
        piece = lbuf.at[h, source(way, k) * 2 + lane]
        return remote(piece, piece, agp_s.at[way, k, h], agp_r.at[way, k, h], s, partner)

    def own(h):
        @pl.when(s == 0)
        def _():
            entry_copy(h).wait()

        @pl.when(s > 0)
        def _():
            late_copy(h).wait_recv()

        for way in range(2):
            @pl.when(has_next[way])
            def _():
                hop(way, 0, h).start()
        lend(0, 0, h, c).start()

    def relay(k, h):
        for way in range(2):
            @pl.when(have(way, k))
            def _():
                arrival(way, k, h).wait_recv()
                if k < last:
                    @pl.when(has_next[way])
                    def _():
                        hop(way, k, h).start()
                lend(way, k, h, c).start()

    def gathered(h):
        lend(0, 0, h, other).wait_recv()
        for k in range(1, Q):
            for way in range(2):
                @pl.when(have(way, k))
                def _():
                    lend(way, k, h, other).wait_recv()

    def gather_drain():
        for h in range(H):
            lend(0, 0, h, c).wait_send()
            for way in range(2):
                @pl.when(has_next[way])
                def _():
                    hop(way, 0, h).wait_send()
                for k in range(1, Q):
                    @pl.when(have(way, k))
                    def _():
                        lend(way, k, h, c).wait_send()
                        if k < last:
                            @pl.when(has_next[way])
                            def _():
                                hop(way, k, h).wait_send()

    def forward(j):
        at = chunk_rows(j)
        pre = dot(saved[at], eexp[...])
        u = 0.5 * pre
        bent = jnp.tanh(u)
        sigma = 0.5 * bent + 0.5
        value = u * bent + u
        act[at] = value.astype(BF16)
        dsl[at] = (sigma * (1.0 + pre - value)).astype(BF16)

    def backward(j):
        at = chunk_rows(j)
        back = dot(grad[at], ered[...], 1, 1)
        slope[at] = (back * dsl[at].astype(F32)).astype(BF16)

    def downward(j):
        at = pl.ds(pl.multiple_of(j * chunk, chunk), chunk)
        input_grad[at] = (grad[at].astype(F32) + dot(slope[at], eexp[...], 1, 1)).astype(BF16)

    def weight_sums(a, b, lo, hi, places):
        at = pl.ds(lo * depth, (hi - lo) * depth)
        for n in range(wide // 256):
            col = pl.ds(n * 256, 256)
            value = dot(a[:, at], b[:, col], 0, 0).reshape(hi - lo, depth, 256)
            for start, low, high in places:
                gsum[start:start + high - low, :, col] = value[low - lo:high - lo]

    local[0].wait()
    local[1].wait()
    early = max(steps // 2, 1)
    for j in range(early):
        forward(j)
    for dev in range(n_dev):
        first[pl.ds((dev + 1) * padded - 16, 16), :] = jnp.zeros((16, first.shape[1]), BF16)
    for way in range(2):
        @pl.when(hops[way] == 0)
        def _():
            wrx[way] = jnp.zeros(wrx.shape[1:], BF16)
            rx[way] = jnp.zeros(rx.shape[1:], BF16)
    for h in range(H):
        own(h)
        if early + h < steps:
            forward(early + h)
    for j in range(early + H, steps):
        forward(j)
    local[2].wait()
    local[3].wait()
    local[4].wait()

    def activate(h):
        total = jnp.zeros((1, half), F32)
        squares = jnp.zeros((1, half), F32)
        for dev in range(n_dev):
            v = lbuf[h, dev].astype(F32)
            total += jnp.sum(v, axis=0, keepdims=True)
            squares += jnp.sum(v * v, axis=0, keepdims=True)
        spread, offset = affine(total, squares, total_rows, gain1[:, cols(h)], shift1[:, cols(h)])
        for dev in range(n_dev):
            v = scaled_silu(lbuf[h, dev].astype(F32), spread, offset)
            first[pl.ds(dev * padded, rows), cols(h)] = v.astype(BF16)

    width = min(256, hid)

    def expand(h):
        for n in range(hid // width):
            at = pl.ds(n * width, width)
            if split:
                value = dot(first[:, cols(h)], wexp[cols(h), at])
                if h > 0:
                    value += inner[:, at]
                if h < H - 1:
                    inner[:, at] = value
            elif h == H - 1:
                value = dot(first[...], wexp[:, at])
            if h == H - 1:
                spread, offset = affine(
                    jnp.sum(value, axis=0, keepdims=True),
                    jnp.sum(value * value, axis=0, keepdims=True),
                    total_rows, gain2[:, at], shift2[:, at],
                )
                hidden[:, at] = scaled_silu(value, spread, offset).astype(BF16)

    def gx(i):
        return remote(gtx.at[i], gprx.at[i], gx_s.at[i], gx_r.at[i], s, partner)

    def exchange(lane, lo, hi):
        @pl.when(other == lane)
        def _():
            for i in range(lo, hi):
                gtx[i] = gsum[i + share * lane].astype(BF16)
                gx(i).start()

    def term(i):
        return gsum[i + share * c] + gprx[i].astype(F32)

    def sum_hop(way, i):
        at = far + i
        return remote(wtx.at[way, i], wrx.at[way, i], st_s.at[way, at], st_r.at[way, at], s, nxt[way])

    def sum_first(i):
        gx(i).wait_recv()
        for way in range(2):
            @pl.when(hops[way] == 0)
            def _():
                wtx[way, i] = term(i).astype(BF16)
                sum_hop(way, i).start()

    def sum_relay(way, i):
        sum_hop(way, i).wait_recv()

        @pl.when(has_next[way])
        def _():
            wtx[way, i] = (term(i) + wrx[way, i].astype(F32)).astype(BF16)
            sum_hop(way, i).start()

    def each(lo, hi, body):
        def step(i, carry):
            body(i)
            return carry
        lax.fori_loop(lo, hi, step, 0)

    far = last * H
    lead = min(H + LEAD, far)
    for k in range(1, last):
        for h in range(H):
            relay(k, h)
    for h in range(H):
        relay(last, h)
        if h == H - 1:
            grad_wait(steps)
            weight_sums(grad, act, 0, front, ((2 * share, 0, front),))
            exchange(1, share, share + front)
        if h > 0:
            gathered(h - 1)
            activate(h - 1)
            expand(h - 1)
    gathered(H - 1)
    activate(H - 1)
    expand(H - 1)

    @pl.when(c == 1)
    def _():
        each(share, share + front, sum_first)

    def pair_copy(h):
        return remote(part.at[other, h], prx.at[h], px_s.at[h], px_r.at[h], s, partner)

    def mine(h, chip):
        return part[c, h, chip].astype(F32) + prx[h, chip].astype(F32)

    def goal(way, m):
        return last - m if way == 0 else m

    def row_hop(way, r):
        m, h = r // H, lax.rem(r, H)
        to = goal(way, m)
        return remote(part.at[c, h, to], rx.at[way, h, to], st_s.at[way, r], st_r.at[way, r], s, nxt[way])

    def row_start(way, r):
        m, h = r // H, lax.rem(r, H)
        to = goal(way, m)
        part[c, h, to] = mine(h, to).astype(BF16)
        row_hop(way, r).start()

    def row_relay(way, r):
        m, h = r // H, lax.rem(r, H)
        to = goal(way, m)

        @pl.when(last - m > hops[way])
        def _():
            row_hop(way, r).wait_recv()
            part[c, h, to] = (mine(h, to) + rx[way, h, to].astype(F32)).astype(BF16)
            row_hop(way, r).start()

    def scatter(h):
        pair_copy(h).wait_recv()
        for way in range(2):
            @pl.when(hops[way] == 0)
            def _():
                row_start(way, h)

    tile = min(256, half)
    for h in range(H):
        for n in range(half // tile):
            value = dot(hidden[...], wred[:, pl.ds(h * half + n * tile, tile)]).astype(BF16)
            for dev in range(n_dev):
                part[dev % 2, h, dev // 2, :, pl.ds(n * tile, tile)] = value[dev * padded:dev * padded + rows]
        pair_copy(h).start()
        if h < steps:
            grad_wait(h)
            backward(h)
        if h > 0:
            scatter(h - 1)

    def rest(r):
        for way in range(2):
            @pl.when(hops[way] == 0)
            def _():
                row_start(way, r)

    scatter(H - 1)
    each(H, lead, rest)
    for j in range(H, steps):
        grad_wait(j)
    weight_sums(grad, act, front, pieces, ((0, front, front + half_r), (share, front + half_r, pieces)))
    for lane in range(2):
        exchange(lane, 0, half_r)
    for j in range(H, steps):
        backward(j)
    each(0, half_r, sum_first)
    for way in range(2):
        @pl.when(both(c == 1, hops[way] == 1))
        def _():
            each(share, share + front, functools.partial(sum_relay, way))
    weight_sums(saved, slope, 0, pieces, ((half_r, 0, half_e), (share + half_r, half_e, pieces)))
    for lane in range(2):
        exchange(lane, half_r, share)
    for way in range(2):
        @pl.when(hops[way] == 1)
        def _():
            each(0, H, functools.partial(row_relay, way))
    for way in range(2):
        @pl.when(both(c == 1, hops[way] == 2))
        def _():
            each(share, share + front, functools.partial(sum_relay, way))

    def give(i, lane):
        piece = gout.at[i + share * lane]
        return remote(piece, piece, wp_s.at[i], wp_r.at[i], s, partner)

    def sum_finish(i):
        value = term(i) + (wrx[0, i].astype(F32) + wrx[1, i].astype(F32))
        gout[i + share * c] = (value * factor).astype(BF16)
        give(i, c).start()

    each(half_r, share, sum_first)
    each(lead, far, rest)
    count = far + share
    farther = jnp.maximum(hops[0], hops[1])
    calm = H + 2 * SKEW

    def slot(t):
        for way in range(2):
            i = t - SKEW * hops[way]
            live = hops[way] > 0

            @pl.when(both(hops[way] > 1, both(i >= 0, i < H)))
            def _():
                row_relay(way, i)

            @pl.when(both(both(c == 1, hops[way] > 2), both(i >= H, i < H + front)))
            def _():
                sum_relay(way, i - H + share)

            @pl.when(both(live, both(i >= H, i < H + share)))
            def _():
                sum_relay(way, i - H)

            @pl.when(both(live, both(i >= H + share, i < count)))
            def _():
                row_relay(way, i - share)

        i = t - SKEW * farther - H

        @pl.when(both(c == 1, both(i >= 0, i < front)))
        def _():
            sum_finish(i + share)

        @pl.when(both(i >= 0, i < share))
        def _():
            sum_finish(i)

        @pl.when(both(t >= calm, t < calm + steps))
        def _():
            downward(t - calm)

    @pl.when(s < sections - 1)
    def _():
        for h in range(H):
            late_copy(h).wait_send()

    @pl.when(s > 0)
    def _():
        for j in range(steps + 1):
            grad_copy(j).wait_send()

    gather_drain()
    for h in range(H):
        pair_copy(h).wait_send()

    each(SKEW, max(count + SKEW * last, calm + steps), slot)

    for h in range(H):
        for way in range(2):
            @pl.when(hops[way] > 0)
            def _():
                row_hop(way, (last - hops[way]) * H + h).wait_recv()
        value = mine(h, q) + rx[0, h, q].astype(F32) + rx[1, h, q].astype(F32)
        late_out[:, cols(h)] = (lbuf[h, d].astype(F32) + value).astype(BF16)

    def drain_rows(r):
        for way in range(2):
            @pl.when(last - r // H > hops[way])
            def _():
                row_hop(way, r).wait_send()

    each(0, far, drain_rows)

    def drain_sums(i):
        give(i, c).wait_send()
        for way in range(2):
            @pl.when(has_next[way])
            def _():
                sum_hop(way, i).wait_send()

    def drain_pair(i):
        gx(i).wait_send()
        give(i, other).wait_recv()

    each(0, share, drain_sums)
    each(0, share, drain_pair)

    @pl.when(c == 1)
    def _():
        each(share, share + front, drain_sums)

    @pl.when(c == 0)
    def _():
        each(share, share + front, drain_pair)


def finish(late_in, grad_in, sums, late_out, input_grad, gexp, gred, wide_e, wide_r, sem):
    ce, fe = wide_e.shape
    a = pltpu.make_async_copy(grad_in, input_grad.at[0], sem.at[0])
    b = pltpu.make_async_copy(late_in, late_out.at[0], sem.at[1])
    a.start()
    b.start()
    pieces, front, share = cuts(ce)
    depth = ce // pieces
    half_r = (pieces - front) // 2
    for lane in range(2):
        at = pl.ds(lane * (ce // 2), ce // 2)
        wide_e[at] = sums[lane * share + half_r:lane * share + share].reshape(ce // 2, fe).astype(F32)
    x = pltpu.make_async_copy(wide_e, gexp.at[0], sem.at[2])
    x.start()
    for n in range(fe // 256):
        at = pl.ds(n * 256, 256)
        wide_r[at, 0:front * depth] = sums[2 * share:, :, at].reshape(front * depth, 256).astype(F32).T
        later = [sums[lane:lane + half_r, :, at].reshape(half_r * depth, 256) for lane in (0, share)]
        wide_r[at, front * depth:] = jnp.concatenate(later).astype(F32).T
    y = pltpu.make_async_copy(wide_r, gred.at[0], sem.at[3])
    y.start()
    for copy in (a, b, x, y):
        copy.wait()


def shards(
    sections, n_dev,
    late_sent, entry_rows, gain_first, shift_first, expand_late, gain_inner, shift_inner,
    reduce_late, early_saved, upstream_grad, exit_grad, expand_early, reduce_early,
):
    rows, cl = entry_rows.shape
    e_rows, ce = exit_grad.shape
    fe = expand_early.shape[2]
    hid = expand_late.shape[2]
    Q = n_dev // 2
    half = cl // H
    padded = -(-rows // 16) * 16
    chunk = max(k for k in range(16, 257, 16) if e_rows % k == 0)
    steps = e_rows // chunk
    pieces, front, share = cuts(ce)
    depth = ce // pieces
    own = share + front
    count = (Q - 1) * H + own
    split = n_dev * padded * hid * 4 <= 4 * 1024 * 1024
    hbm = pl.BlockSpec(memory_space=pltpu.HBM)
    any_spec = pl.BlockSpec(memory_space=pl.ANY)
    vm = pl.BlockSpec(memory_space=pltpu.VMEM)
    V = pltpu.VMEM
    dma = pltpu.SemaphoreType.DMA
    late_out, input_grad, sums = pl.pallas_call(
        functools.partial(kernel, sections, n_dev, chunk, split),
        out_shape=(
            V((rows, cl), BF16),
            V((e_rows, ce), BF16),
            V((2 * pieces, depth, fe), BF16),
        ),
        in_specs=[hbm, hbm, vm, vm, hbm, vm, vm] + [hbm] * 6,
        out_specs=(vm, vm, vm),
        scratch_shapes=[
            V((rows, cl), BF16),
            V((H, n_dev, rows, half), BF16),
            V((n_dev * padded, cl), BF16),
            V((n_dev * padded, hid) if split else (8, 128), F32),
            V((n_dev * padded, hid), BF16),
            V((2, H, Q, rows, half), BF16),
            V((H, Q, rows, half), BF16),
            V((2, H, Q, rows, half), BF16),
            V((cl, hid), BF16),
            V((hid, cl), BF16),
            V((e_rows, ce), BF16),
            V((e_rows, ce), BF16),
            V((ce, fe), BF16),
            V((fe, ce), BF16),
            V((e_rows, fe), BF16),
            V((e_rows, fe), BF16),
            V((e_rows, fe), BF16),
            V((2 * pieces, depth, fe), F32),
            V((own, depth, fe), BF16),
            V((own, depth, fe), BF16),
            V((2, own, depth, fe), BF16),
            V((2, own, depth, fe), BF16),
            dma((6,)), dma((H,)), dma((H,)), dma((steps + 1,)), dma((steps + 1,)),
            dma((2, Q - 1, H)), dma((2, Q - 1, H)), dma((2, Q, H)), dma((2, Q, H)),
            dma((H,)), dma((H,)), dma((own,)), dma((own,)),
            dma((2, count)), dma((2, count)), dma((own,)), dma((own,)),
        ],
        compiler_params=pltpu.CompilerParams(
            collective_id=0, has_side_effects=True, vmem_limit_bytes=60 * 1024 * 1024
        ),
        name="relay",
    )(
        late_sent[0], entry_rows, gain_first, shift_first, expand_late[0], gain_inner, shift_inner,
        reduce_late[0], early_saved[0], upstream_grad[0], exit_grad, expand_early[0], reduce_early[0],
    )
    return pl.pallas_call(
        finish,
        out_shape=(
            jax.ShapeDtypeStruct((1, rows, cl), BF16),
            jax.ShapeDtypeStruct((1, e_rows, ce), BF16),
            jax.ShapeDtypeStruct((1, ce, fe), F32),
            jax.ShapeDtypeStruct((1, fe, ce), F32),
        ),
        in_specs=[vm, vm, vm],
        out_specs=(any_spec,) * 4,
        scratch_shapes=[V((ce, fe), F32), V((fe, ce), F32), dma((4,))],
        compiler_params=pltpu.CompilerParams(vmem_limit_bytes=16 * 1024 * 1024),
        name="finish",
    )(late_out, input_grad, sums)


def solution(mesh):
    sections, n_dev = mesh.shape["section"], mesh.shape["dev"]
    sd, dd = P("section", "dev", None), P("dev", None)
    rep, one = P("section", None, None), P("section", None)
    in_specs = (
        sd, dd, one, one, P("section", None, "dev"), P("section", "dev"), P("section", "dev"),
        sd, sd, sd, dd, rep, rep,
    )
    return jax.shard_map(
        functools.partial(shards, sections, n_dev), mesh=mesh, in_specs=in_specs,
        out_specs=(sd, sd, rep, rep), check_vma=False,
    )
```

```python
import functools
import math

import jax
import jax.numpy as jnp
from jax import lax
from jax.experimental import pallas as pl
from jax.experimental.pallas import tpu as pltpu
from jax.sharding import PartitionSpec as P

MESH = pl.DeviceIdType.MESH
epsilon = 1e-05
H = 4
U = 2
SKEW = 4
LEAD = 0
LAG = 3
F32 = jnp.float32
BF16 = jnp.bfloat16


def scaled_silu(x, spread, offset):
    u = x * (0.5 * spread) + 0.5 * offset
    return u * jnp.tanh(u) + u


def affine(sums, squares, count, gain, shift):
    average = sums / count
    second = squares / count
    spread = gain * lax.rsqrt(second - average * average + epsilon)
    return spread, shift - average * spread


def dot(a, b, ca=1, cb=0):
    return lax.dot_general(a, b, (((ca,), (cb,)), ((), ())), preferred_element_type=F32)


def both(a, b):
    return jnp.logical_and(a, b)


def cuts(ce):
    pieces = ce // 16
    front = pieces // 2
    return pieces, front, (pieces - front) // 2 + pieces // 2


def kernel(
    sections, n_dev, chunk, split,
    late_hbm, entry_hbm, gain1, shift1, wexp_hbm, gain2, shift2, wred_hbm,
    saved_hbm, up_hbm, exit_hbm, eexp_hbm, ered_hbm,
    late_out, input_grad, gout,
    stage, lbuf, first, inner, hidden, part, prx, rx,
    wexp, wred, saved, grad, eexp, ered, act, dsl, slope,
    gsum, gtx, gprx, wtx, wrx,
    loc_sem, perm_send, perm_recv, gp_send, gp_recv,
    ag_s, ag_r, agp_s, agp_r, px_s, px_r, gx_s, gx_r, st_s, st_r, wp_s, wp_r,
):
    Q = n_dev // 2
    s = lax.axis_index("section")
    d = lax.axis_index("dev")
    q = d // 2
    c = lax.rem(d, 2)
    other = 1 - c
    partner = q * 2 + other
    rows = late_hbm.shape[0]
    half = late_hbm.shape[1] // H
    padded = first.shape[0] // n_dev
    e_rows = saved_hbm.shape[0]
    steps = e_rows // chunk
    total_rows = rows * n_dev
    hid = wexp.shape[1]
    wide = eexp.shape[1]
    ce = grad.shape[1]
    pieces, front, share = cuts(ce)
    depth = ce // pieces
    half_r, half_e = (pieces - front) // 2, pieces // 2
    ahead = front * depth
    factor = 1.0 / math.sqrt(e_rows * n_dev)

    last = Q - 1
    right, left = jnp.minimum(q + 1, last), jnp.maximum(q - 1, 0)
    nxt = (right * 2 + c, left * 2 + c)
    has_next = (q < last, q > 0)
    has_prev = (q > 0, q < last)
    hops = (q, last - q)

    barrier = pltpu.get_barrier_semaphore()
    pl.semaphore_signal(barrier, inc=1, device_id=(s, partner), device_id_type=MESH)
    for way in range(2):
        @pl.when(has_next[way])
        def _():
            pl.semaphore_signal(barrier, inc=1, device_id=(s, nxt[way]), device_id_type=MESH)

    @pl.when(s > 0)
    def _():
        pl.semaphore_signal(barrier, inc=1, device_id=(s - 1, d), device_id_type=MESH)

    @pl.when(s < sections - 1)
    def _():
        pl.semaphore_signal(barrier, inc=1, device_id=(s + 1, d), device_id_type=MESH)

    stage_copy = pltpu.make_async_copy(late_hbm, stage, loc_sem.at[5])
    stage_copy.start()
    local = [
        pltpu.make_async_copy(src, dst, loc_sem.at[i])
        for i, (src, dst) in enumerate(
            ((saved_hbm, saved), (eexp_hbm, eexp), (ered_hbm, ered), (wexp_hbm, wexp), (wred_hbm, wred))
        )
    ]
    for copy in local:
        copy.start()

    def remote(src, dst, send, recv, section, dev):
        return pltpu.make_async_remote_copy(
            src_ref=src, dst_ref=dst, send_sem=send, recv_sem=recv,
            device_id=(section, dev), device_id_type=MESH,
        )

    def cols(h):
        return pl.ds(h * half, half)

    fine = half // U
    G = H * U

    def fine_cols(g):
        return pl.ds(g * fine, fine)

    def rows_of(g, dev):
        return lbuf.at[g // U, dev, :, pl.ds(g % U * fine, fine)]

    def late_copy(g):
        return remote(
            stage.at[:, fine_cols(g)], rows_of(g, d), perm_send.at[g], perm_recv.at[g],
            jnp.minimum(s + 1, sections - 1), d,
        )

    def entry_copy(g):
        return pltpu.make_async_copy(entry_hbm.at[:, fine_cols(g)], rows_of(g, d), perm_recv.at[g])

    def chunk_rows(j):
        return pl.ds(j * chunk, chunk)

    def grad_at(j):
        if j == steps:
            return slice(None), pl.ds(0, ahead)
        return chunk_rows(j), pl.ds(ahead, ce - ahead)

    def grad_copy(j):
        return remote(
            up_hbm.at[grad_at(j)], grad.at[grad_at(j)], gp_send.at[j], gp_recv.at[j],
            jnp.maximum(s - 1, 0), d,
        )

    def exit_copy(j):
        return pltpu.make_async_copy(exit_hbm.at[grad_at(j)], grad.at[grad_at(j)], gp_recv.at[j])

    def grad_wait(j):
        @pl.when(s < sections - 1)
        def _():
            grad_copy(j).wait_recv()

        @pl.when(s == sections - 1)
        def _():
            exit_copy(j).wait()

    stage_copy.wait()
    pl.semaphore_wait(
        barrier,
        1 + jnp.minimum(q, 1) + jnp.minimum(last - q, 1) + jnp.minimum(s, 1) + jnp.minimum(sections - 1 - s, 1),
    )

    @pl.when(s < sections - 1)
    def _():
        for g in range(G):
            late_copy(g).start()

    @pl.when(s == 0)
    def _():
        for g in range(G):
            entry_copy(g).start()

    @pl.when(s > 0)
    def _():
        for j in (steps, *range(steps)):
            grad_copy(j).start()

    @pl.when(s == sections - 1)
    def _():
        for j in (steps, *range(steps)):
            exit_copy(j).start()

    def source(way, k):
        return jnp.maximum(q - k, 0) if way == 0 else jnp.minimum(q + k, last)

    def have(way, k):
        return hops[way] >= k

    def hop(way, k, h):
        piece = rows_of(h, source(way, k) * 2 + c)
        return remote(piece, piece, ag_s.at[way, k, h], ag_r.at[way, k, h], s, nxt[way])

    def arrival(way, k, h):
        piece = rows_of(h, source(way, k) * 2 + c)
        return remote(piece, piece, ag_s.at[way, k - 1, h], ag_r.at[way, k - 1, h], s, nxt[way])

    def lend(way, k, h, lane):
        piece = rows_of(h, source(way, k) * 2 + lane)
        return remote(piece, piece, agp_s.at[way, k, h], agp_r.at[way, k, h], s, partner)

    def own(h):
        @pl.when(s == 0)
        def _():
            entry_copy(h).wait()

        @pl.when(s > 0)
        def _():
            late_copy(h).wait_recv()

        for way in range(2):
            @pl.when(has_next[way])
            def _():
                hop(way, 0, h).start()
        lend(0, 0, h, c).start()

    def relay(k, h):
        for way in range(2):
            @pl.when(have(way, k))
            def _():
                arrival(way, k, h).wait_recv()
                if k < last:
                    @pl.when(has_next[way])
                    def _():
                        hop(way, k, h).start()
                lend(way, k, h, c).start()

    def gathered(h):
        for g in range(h * U, h * U + U):
            lend(0, 0, g, other).wait_recv()
            for k in range(1, Q):
                for way in range(2):
                    @pl.when(have(way, k))
                    def _():
                        lend(way, k, g, other).wait_recv()

    def gather_drain():
        for h in range(G):
            lend(0, 0, h, c).wait_send()
            for way in range(2):
                @pl.when(has_next[way])
                def _():
                    hop(way, 0, h).wait_send()
                for k in range(1, Q):
                    @pl.when(have(way, k))
                    def _():
                        lend(way, k, h, c).wait_send()
                        if k < last:
                            @pl.when(has_next[way])
                            def _():
                                hop(way, k, h).wait_send()

    def forward(j):
        at = chunk_rows(j)
        pre = dot(saved[at], eexp[...])
        u = 0.5 * pre
        bent = jnp.tanh(u)
        sigma = 0.5 * bent + 0.5
        value = u * bent + u
        act[at] = value.astype(BF16)
        dsl[at] = (sigma * (1.0 + pre - value)).astype(BF16)

    def backward(j):
        at = chunk_rows(j)
        back = dot(grad[at], ered[...], 1, 1)
        slope[at] = (back * dsl[at].astype(F32)).astype(BF16)

    def downward(j):
        at = pl.ds(pl.multiple_of(j * chunk, chunk), chunk)
        input_grad[at] = (grad[at].astype(F32) + dot(slope[at], eexp[...], 1, 1)).astype(BF16)

    def weight_sums(a, b, lo, hi, places):
        at = pl.ds(lo * depth, (hi - lo) * depth)
        for n in range(wide // 256):
            col = pl.ds(n * 256, 256)
            value = dot(a[:, at], b[:, col], 0, 0).reshape(hi - lo, depth, 256)
            for start, low, high in places:
                gsum[start:start + high - low, :, col] = value[low - lo:high - lo]

    local[0].wait()
    local[1].wait()
    early = max(steps // 2, 1)
    for j in range(early):
        forward(j)
    for dev in range(n_dev):
        first[pl.ds((dev + 1) * padded - 16, 16), :] = jnp.zeros((16, first.shape[1]), BF16)
    for way in range(2):
        @pl.when(hops[way] == 0)
        def _():
            wrx[way] = jnp.zeros(wrx.shape[1:], BF16)
            rx[way] = jnp.zeros(rx.shape[1:], BF16)
    for g in range(G):
        own(g)
        if early + g < steps:
            forward(early + g)
    for j in range(early + G, steps):
        forward(j)
    local[2].wait()
    local[3].wait()
    local[4].wait()

    def activate(h):
        total = jnp.zeros((1, half), F32)
        squares = jnp.zeros((1, half), F32)
        for dev in range(n_dev):
            v = lbuf[h, dev].astype(F32)
            total += jnp.sum(v, axis=0, keepdims=True)
            squares += jnp.sum(v * v, axis=0, keepdims=True)
        spread, offset = affine(total, squares, total_rows, gain1[:, cols(h)], shift1[:, cols(h)])
        for dev in range(n_dev):
            v = scaled_silu(lbuf[h, dev].astype(F32), spread, offset)
            first[pl.ds(dev * padded, rows), cols(h)] = v.astype(BF16)

    width = min(256, hid)

    def expand(h):
        for n in range(hid // width):
            at = pl.ds(n * width, width)
            if split:
                value = dot(first[:, cols(h)], wexp[cols(h), at])
                if h > 0:
                    value += inner[:, at]
                if h < H - 1:
                    inner[:, at] = value
            elif h == H - 1:
                value = dot(first[...], wexp[:, at])
            if h == H - 1:
                spread, offset = affine(
                    jnp.sum(value, axis=0, keepdims=True),
                    jnp.sum(value * value, axis=0, keepdims=True),
                    total_rows, gain2[:, at], shift2[:, at],
                )
                hidden[:, at] = scaled_silu(value, spread, offset).astype(BF16)

    def gx(i):
        return remote(gtx.at[i], gprx.at[i], gx_s.at[i], gx_r.at[i], s, partner)

    def exchange(lane, lo, hi):
        @pl.when(other == lane)
        def _():
            for i in range(lo, hi):
                gtx[i] = gsum[i + share * lane].astype(BF16)
                gx(i).start()

    def term(i):
        return gsum[i + share * c] + gprx[i].astype(F32)

    def sum_hop(way, i):
        at = far + i
        return remote(wtx.at[way, i], wrx.at[way, i], st_s.at[way, at], st_r.at[way, at], s, nxt[way])

    def sum_first(i):
        gx(i).wait_recv()
        for way in range(2):
            @pl.when(hops[way] == 0)
            def _():
                wtx[way, i] = term(i).astype(BF16)
                sum_hop(way, i).start()

    def sum_relay(way, i):
        sum_hop(way, i).wait_recv()

        @pl.when(has_next[way])
        def _():
            wtx[way, i] = (term(i) + wrx[way, i].astype(F32)).astype(BF16)
            sum_hop(way, i).start()

    def each(lo, hi, body):
        def step(i, carry):
            body(i)
            return carry
        lax.fori_loop(lo, hi, step, 0)

    far = last * H
    lead = min(H + LEAD, far)
    for k in range(1, last):
        for g in range(G):
            relay(k, g)
    for h in range(H):
        for g in range(h * U, h * U + U):
            relay(last, g)
        if h == H - 1:
            grad_wait(steps)
            weight_sums(grad, act, 0, front, ((2 * share, 0, front),))
            exchange(1, share, share + front)
        if h > 0:
            gathered(h - 1)
            activate(h - 1)
            expand(h - 1)
    gathered(H - 1)
    activate(H - 1)
    expand(H - 1)

    @pl.when(c == 1)
    def _():
        each(share, share + front, sum_first)

    def pair_copy(h):
        return remote(part.at[other, h], prx.at[h], px_s.at[h], px_r.at[h], s, partner)

    def mine(h, chip):
        return part[c, h, chip].astype(F32) + prx[h, chip].astype(F32)

    def goal(way, m):
        return last - m if way == 0 else m

    def row_hop(way, r):
        m, h = r // H, lax.rem(r, H)
        to = goal(way, m)
        return remote(part.at[c, h, to], rx.at[way, h, to], st_s.at[way, r], st_r.at[way, r], s, nxt[way])

    def row_start(way, r):
        m, h = r // H, lax.rem(r, H)
        to = goal(way, m)
        part[c, h, to] = mine(h, to).astype(BF16)
        row_hop(way, r).start()

    def row_relay(way, r):
        m, h = r // H, lax.rem(r, H)
        to = goal(way, m)

        @pl.when(last - m > hops[way])
        def _():
            row_hop(way, r).wait_recv()
            part[c, h, to] = (mine(h, to) + rx[way, h, to].astype(F32)).astype(BF16)
            row_hop(way, r).start()

    def scatter(h):
        pair_copy(h).wait_recv()
        for way in range(2):
            @pl.when(hops[way] == 0)
            def _():
                row_start(way, h)

    tile = min(256, half)
    for h in range(H):
        for n in range(half // tile):
            value = dot(hidden[...], wred[:, pl.ds(h * half + n * tile, tile)]).astype(BF16)
            for dev in range(n_dev):
                part[dev % 2, h, dev // 2, :, pl.ds(n * tile, tile)] = value[dev * padded:dev * padded + rows]
        pair_copy(h).start()
        if h < steps:
            grad_wait(h)
            backward(h)
        if h > 0:
            scatter(h - 1)

    def rest(r):
        for way in range(2):
            @pl.when(hops[way] == 0)
            def _():
                row_start(way, r)

    scatter(H - 1)
    each(H, lead, rest)
    for j in range(H, steps):
        grad_wait(j)
    weight_sums(grad, act, front, pieces, ((0, front, front + half_r), (share, front + half_r, pieces)))
    for lane in range(2):
        exchange(lane, 0, half_r)
    for j in range(H, steps):
        backward(j)
    each(0, half_r, sum_first)
    for way in range(2):
        @pl.when(both(c == 1, hops[way] == 1))
        def _():
            each(share, share + front, functools.partial(sum_relay, way))
    weight_sums(saved, slope, 0, pieces, ((half_r, 0, half_e), (share + half_r, half_e, pieces)))
    for lane in range(2):
        exchange(lane, half_r, share)
    per = front // H
    for h in range(H):
        for way in range(2):
            @pl.when(both(c == 1, hops[way] == 2))
            def _():
                for i in range(per):
                    sum_relay(way, share + h * per + i)
        for way in range(2):
            @pl.when(hops[way] == 1)
            def _():
                row_relay(way, h)
    for way in range(2):
        @pl.when(hops[way] == 2)
        def _():
            for h in range(H // 2):
                row_relay(way, h)

    def give(i, lane):
        piece = gout.at[i + share * lane]
        return remote(piece, piece, wp_s.at[i], wp_r.at[i], s, partner)

    def sum_finish(i):
        value = term(i) + (wrx[0, i].astype(F32) + wrx[1, i].astype(F32))
        gout[i + share * c] = (value * factor).astype(BF16)
        give(i, c).start()

    each(half_r, share, sum_first)
    each(lead, far, rest)
    count = far + share
    farther = jnp.maximum(hops[0], hops[1])
    calm = H + 2 * SKEW

    def drain_gifts(i):
        give(i, c).wait_send()

    def drain_sums(i):
        @pl.when(i < share)
        def _():
            give(i, c).wait_send()

        for way in range(2):
            @pl.when(has_next[way])
            def _():
                sum_hop(way, i).wait_send()

    def drain_pair(i):
        gx(i).wait_send()
        give(i, other).wait_recv()

    def slot(t):
        for way in range(2):
            i = t - SKEW * hops[way]
            live = hops[way] > 0

            @pl.when(both(hops[way] > 1, both(i >= H // 2 * (3 - jnp.minimum(hops[way], 3)), i < H)))
            def _():
                row_relay(way, i)

            @pl.when(both(both(c == 1, hops[way] > 2), both(i >= H, i < H + front)))
            def _():
                sum_relay(way, i - H + share)

            @pl.when(both(live, both(i >= H, i < H + share)))
            def _():
                sum_relay(way, i - H)

            @pl.when(both(live, both(i >= H + share, i < count)))
            def _():
                row_relay(way, i - share)

        i = t - SKEW * farther - H

        @pl.when(both(c == 1, both(i >= 0, i < front)))
        def _():
            sum_finish(i + share)
            drain_sums(i + share)

        @pl.when(both(i >= 0, i < share))
        def _():
            sum_finish(i)

        @pl.when(both(i >= LAG, i < share))
        def _():
            drain_sums(i - LAG)
            drain_pair(i - LAG)

        @pl.when(both(t >= calm, t < calm + steps))
        def _():
            downward(t - calm)

    @pl.when(s < sections - 1)
    def _():
        for g in range(G):
            late_copy(g).wait_send()

    @pl.when(s > 0)
    def _():
        for j in range(steps + 1):
            grad_copy(j).wait_send()

    gather_drain()
    for h in range(H):
        pair_copy(h).wait_send()

    each(SKEW, max(H + share + SKEW * last, calm + steps), slot)

    for h in range(H):
        for way in range(2):
            @pl.when(hops[way] > 0)
            def _():
                row_hop(way, (last - hops[way]) * H + h).wait_recv()
        value = mine(h, q) + rx[0, h, q].astype(F32) + rx[1, h, q].astype(F32)
        late_out[:, cols(h)] = (lbuf[h, d].astype(F32) + value).astype(BF16)

    def drain_rows(r):
        for way in range(2):
            @pl.when(last - r // H > hops[way])
            def _():
                row_hop(way, r).wait_send()

    each(0, far, drain_rows)

    each(share - LAG, share, drain_sums)
    each(share - LAG, share, drain_pair)

    @pl.when(c == 1)
    def _():
        each(share, share + front, drain_gifts)

    @pl.when(c == 0)
    def _():
        each(share, share + front, drain_pair)


def finish(late_in, grad_in, sums, late_out, input_grad, gexp, gred, wide_e, wide_r, sem):
    ce, fe = wide_e.shape
    a = pltpu.make_async_copy(grad_in, input_grad.at[0], sem.at[0])
    b = pltpu.make_async_copy(late_in, late_out.at[0], sem.at[1])
    a.start()
    b.start()
    pieces, front, share = cuts(ce)
    depth = ce // pieces
    half_r = (pieces - front) // 2
    copies = [a, b]

    def send(src, dst):
        copies.append(pltpu.make_async_copy(src, dst, sem.at[len(copies)]))
        copies[-1].start()

    for lane in range(2):
        at = pl.ds(lane * (ce // 2), ce // 2)
        wide_e[at] = sums[lane * share + half_r:lane * share + share].reshape(ce // 2, fe).astype(F32)
        send(wide_e.at[at], gexp.at[0, at])
    for n in range(fe // 256):
        at = pl.ds(n * 256, 256)
        wide_r[at, 0:front * depth] = sums[2 * share:, :, at].reshape(front * depth, 256).astype(F32).T
        later = [sums[lane:lane + half_r, :, at].reshape(half_r * depth, 256) for lane in (0, share)]
        wide_r[at, front * depth:] = jnp.concatenate(later).astype(F32).T
        send(wide_r.at[at], gred.at[0, at])
    for copy in copies:
        copy.wait()


def shards(
    sections, n_dev,
    late_sent, entry_rows, gain_first, shift_first, expand_late, gain_inner, shift_inner,
    reduce_late, early_saved, upstream_grad, exit_grad, expand_early, reduce_early,
):
    rows, cl = entry_rows.shape
    e_rows, ce = exit_grad.shape
    fe = expand_early.shape[2]
    hid = expand_late.shape[2]
    Q = n_dev // 2
    half = cl // H
    padded = -(-rows // 16) * 16
    chunk = max(k for k in range(16, 257, 16) if e_rows % k == 0)
    steps = e_rows // chunk
    pieces, front, share = cuts(ce)
    depth = ce // pieces
    own = share + front
    count = (Q - 1) * H + own
    split = n_dev * padded * hid * 4 <= 4 * 1024 * 1024
    hbm = pl.BlockSpec(memory_space=pltpu.HBM)
    any_spec = pl.BlockSpec(memory_space=pl.ANY)
    vm = pl.BlockSpec(memory_space=pltpu.VMEM)
    V = pltpu.VMEM
    dma = pltpu.SemaphoreType.DMA
    late_out, input_grad, sums = pl.pallas_call(
        functools.partial(kernel, sections, n_dev, chunk, split),
        out_shape=(
            V((rows, cl), BF16),
            V((e_rows, ce), BF16),
            V((2 * pieces, depth, fe), BF16),
        ),
        in_specs=[hbm, hbm, vm, vm, hbm, vm, vm] + [hbm] * 6,
        out_specs=(vm, vm, vm),
        scratch_shapes=[
            V((rows, cl), BF16),
            V((H, n_dev, rows, half), BF16),
            V((n_dev * padded, cl), BF16),
            V((n_dev * padded, hid) if split else (8, 128), F32),
            V((n_dev * padded, hid), BF16),
            V((2, H, Q, rows, half), BF16),
            V((H, Q, rows, half), BF16),
            V((2, H, Q, rows, half), BF16),
            V((cl, hid), BF16),
            V((hid, cl), BF16),
            V((e_rows, ce), BF16),
            V((e_rows, ce), BF16),
            V((ce, fe), BF16),
            V((fe, ce), BF16),
            V((e_rows, fe), BF16),
            V((e_rows, fe), BF16),
            V((e_rows, fe), BF16),
            V((2 * pieces, depth, fe), F32),
            V((own, depth, fe), BF16),
            V((own, depth, fe), BF16),
            V((2, own, depth, fe), BF16),
            V((2, own, depth, fe), BF16),
            dma((6,)), dma((H * U,)), dma((H * U,)), dma((steps + 1,)), dma((steps + 1,)),
            dma((2, Q - 1, H * U)), dma((2, Q - 1, H * U)), dma((2, Q, H * U)), dma((2, Q, H * U)),
            dma((H,)), dma((H,)), dma((own,)), dma((own,)),
            dma((2, count)), dma((2, count)), dma((own,)), dma((own,)),
        ],
        compiler_params=pltpu.CompilerParams(
            collective_id=0, has_side_effects=True, vmem_limit_bytes=60 * 1024 * 1024
        ),
        name="relay",
    )(
        late_sent[0], entry_rows, gain_first, shift_first, expand_late[0], gain_inner, shift_inner,
        reduce_late[0], early_saved[0], upstream_grad[0], exit_grad, expand_early[0], reduce_early[0],
    )
    return pl.pallas_call(
        finish,
        out_shape=(
            jax.ShapeDtypeStruct((1, rows, cl), BF16),
            jax.ShapeDtypeStruct((1, e_rows, ce), BF16),
            jax.ShapeDtypeStruct((1, ce, fe), F32),
            jax.ShapeDtypeStruct((1, fe, ce), F32),
        ),
        in_specs=[vm, vm, vm],
        out_specs=(any_spec,) * 4,
        scratch_shapes=[V((ce, fe), F32), V((fe, ce), F32), dma((4 + fe // 256,))],
        compiler_params=pltpu.CompilerParams(vmem_limit_bytes=16 * 1024 * 1024),
        name="finish",
    )(late_out, input_grad, sums)


def solution(mesh):
    sections, n_dev = mesh.shape["section"], mesh.shape["dev"]
    sd, dd = P("section", "dev", None), P("dev", None)
    rep, one = P("section", None, None), P("section", None)
    in_specs = (
        sd, dd, one, one, P("section", None, "dev"), P("section", "dev"), P("section", "dev"),
        sd, sd, sd, dd, rep, rep,
    )
    return jax.shard_map(
        functools.partial(shards, sections, n_dev), mesh=mesh, in_specs=in_specs,
        out_specs=(sd, sd, rep, rep), check_vma=False,
    )
```

```python
import functools
import math

import jax
import jax.numpy as jnp
from jax import lax
from jax.experimental import pallas as pl
from jax.experimental.pallas import tpu as pltpu
from jax.sharding import PartitionSpec as P

MESH = pl.DeviceIdType.MESH
epsilon = 1e-05
H = 4
U = 2
SKEW = 4
LEAD = 0
F32 = jnp.float32
BF16 = jnp.bfloat16


def scaled_silu(x, spread, offset):
    u = x * (0.5 * spread) + 0.5 * offset
    return u * jnp.tanh(u) + u


def affine(sums, squares, count, gain, shift):
    average = sums / count
    second = squares / count
    spread = gain * lax.rsqrt(second - average * average + epsilon)
    return spread, shift - average * spread


def dot(a, b, ca=1, cb=0):
    return lax.dot_general(a, b, (((ca,), (cb,)), ((), ())), preferred_element_type=F32)


def both(a, b):
    return jnp.logical_and(a, b)


def cuts(ce):
    pieces = ce // 16
    front = pieces // 2
    return pieces, front, (pieces - front) // 2 + pieces // 2


def kernel(
    sections, n_dev, chunk, split,
    late_hbm, entry_hbm, gain1_hbm, shift1_hbm, wexp_hbm, gain2_hbm, shift2_hbm, wred_hbm,
    saved_hbm, up_hbm, exit_hbm, eexp_hbm, ered_hbm,
    late_out, input_grad, gout,
    stage, lbuf, first, inner, hidden, part, prx, rx,
    wexp, wred, saved, grad, eexp, ered, act, dsl, slope,
    gsum, gtx, gprx, wtx, wrx, gain1, shift1, gain2, shift2,
    loc_sem, perm_recv, gp_recv, ag_r, agp_r, px_r, gx_r, row_r, sum_r, wp_r,
    perm_send, gp_send, ag_s, agp_s, px_s, gx_s, row_s, sum_s, wp_s,
):
    Q = n_dev // 2
    s = lax.axis_index("section")
    d = lax.axis_index("dev")
    q = d // 2
    c = lax.rem(d, 2)
    other = 1 - c
    partner = q * 2 + other
    rows = late_hbm.shape[0]
    half = late_hbm.shape[1] // H
    padded = first.shape[0] // n_dev
    e_rows = saved_hbm.shape[0]
    steps = e_rows // chunk
    total_rows = rows * n_dev
    hid = wexp.shape[1]
    wide = eexp.shape[1]
    ce = grad.shape[1]
    pieces, front, share = cuts(ce)
    depth = ce // pieces
    half_r, half_e = (pieces - front) // 2, pieces // 2
    ahead = front * depth
    factor = 1.0 / math.sqrt(e_rows * n_dev)

    last = Q - 1
    right, left = jnp.minimum(q + 1, last), jnp.maximum(q - 1, 0)
    nxt = (right * 2 + c, left * 2 + c)
    has_next = (q < last, q > 0)
    has_prev = (q > 0, q < last)
    hops = (q, last - q)

    barrier = pltpu.get_barrier_semaphore()
    pl.semaphore_signal(barrier, inc=1, device_id=(s, partner), device_id_type=MESH)
    for way in range(2):
        @pl.when(has_next[way])
        def _():
            pl.semaphore_signal(barrier, inc=1, device_id=(s, nxt[way]), device_id_type=MESH)

    @pl.when(s > 0)
    def _():
        pl.semaphore_signal(barrier, inc=1, device_id=(s - 1, d), device_id_type=MESH)

    @pl.when(s < sections - 1)
    def _():
        pl.semaphore_signal(barrier, inc=1, device_id=(s + 1, d), device_id_type=MESH)

    stage_copy = pltpu.make_async_copy(late_hbm, stage, loc_sem.at[9])
    stage_copy.start()
    local = [
        pltpu.make_async_copy(src, dst, loc_sem.at[i])
        for i, (src, dst) in enumerate(
            (
                (saved_hbm, saved), (eexp_hbm, eexp), (ered_hbm, ered), (wexp_hbm, wexp), (wred_hbm, wred),
                (gain1_hbm, gain1), (shift1_hbm, shift1), (gain2_hbm, gain2), (shift2_hbm, shift2),
            )
        )
    ]
    for copy in local:
        copy.start()

    def remote(src, dst, send, recv, section, dev):
        return pltpu.make_async_remote_copy(
            src_ref=src, dst_ref=dst, send_sem=send, recv_sem=recv,
            device_id=(section, dev), device_id_type=MESH,
        )

    def cols(h):
        return pl.ds(h * half, half)

    fine = half // U
    G = H * U

    def fine_cols(g):
        return pl.ds(g * fine, fine)

    def rows_of(g, dev):
        return lbuf.at[g // U, dev, :, pl.ds(g % U * fine, fine)]

    def late_copy(g):
        return remote(
            stage.at[:, fine_cols(g)], rows_of(g, d), perm_send, perm_recv.at[g],
            jnp.minimum(s + 1, sections - 1), d,
        )

    def entry_copy(g):
        return pltpu.make_async_copy(entry_hbm.at[:, fine_cols(g)], rows_of(g, d), perm_recv.at[g])

    def chunk_rows(j):
        return pl.ds(j * chunk, chunk)

    def grad_at(j):
        if j == steps:
            return slice(None), pl.ds(0, ahead)
        return chunk_rows(j), pl.ds(ahead, ce - ahead)

    def grad_copy(j):
        return remote(
            up_hbm.at[grad_at(j)], grad.at[grad_at(j)], gp_send, gp_recv.at[j],
            jnp.maximum(s - 1, 0), d,
        )

    def exit_copy(j):
        return pltpu.make_async_copy(exit_hbm.at[grad_at(j)], grad.at[grad_at(j)], gp_recv.at[j])

    def grad_wait(j):
        @pl.when(s < sections - 1)
        def _():
            grad_copy(j).wait_recv()

        @pl.when(s == sections - 1)
        def _():
            exit_copy(j).wait()

    stage_copy.wait()
    pl.semaphore_wait(
        barrier,
        1 + jnp.minimum(q, 1) + jnp.minimum(last - q, 1) + jnp.minimum(s, 1) + jnp.minimum(sections - 1 - s, 1),
    )

    @pl.when(s < sections - 1)
    def _():
        for g in range(G):
            late_copy(g).start()

    @pl.when(s == 0)
    def _():
        for g in range(G):
            entry_copy(g).start()

    @pl.when(s > 0)
    def _():
        for j in (steps, *range(steps)):
            grad_copy(j).start()

    @pl.when(s == sections - 1)
    def _():
        for j in (steps, *range(steps)):
            exit_copy(j).start()

    def source(way, k):
        return jnp.maximum(q - k, 0) if way == 0 else jnp.minimum(q + k, last)

    def have(way, k):
        return hops[way] >= k

    def hop(way, k, h):
        piece = rows_of(h, source(way, k) * 2 + c)
        return remote(piece, piece, ag_s.at[way], ag_r.at[way, k, h], s, nxt[way])

    def arrival(way, k, h):
        piece = rows_of(h, source(way, k) * 2 + c)
        return remote(piece, piece, ag_s.at[way], ag_r.at[way, k - 1, h], s, nxt[way])

    def lend(way, k, h, lane):
        piece = rows_of(h, source(way, k) * 2 + lane)
        return remote(piece, piece, agp_s, agp_r.at[h // U], s, partner)

    def own(h):
        @pl.when(s == 0)
        def _():
            entry_copy(h).wait()

        @pl.when(s > 0)
        def _():
            late_copy(h).wait_recv()

        for way in range(2):
            @pl.when(has_next[way])
            def _():
                hop(way, 0, h).start()
        lend(0, 0, h, c).start()

    def relay(k, h):
        for way in range(2):
            @pl.when(have(way, k))
            def _():
                arrival(way, k, h).wait_recv()
                if k < last:
                    @pl.when(has_next[way])
                    def _():
                        hop(way, k, h).start()
                lend(way, k, h, c).start()

    def span(buf, send, recv):
        return remote(buf, buf, send, recv, s, partner)

    def gathered(h):
        span(lbuf.at[h, 0:Q], agp_s, agp_r.at[h]).wait_recv()

    def gather_drain():
        span(lbuf.at[:, 0:Q], agp_s, agp_r.at[0]).wait_send()
        for way in range(2):
            for k in range(last):
                @pl.when(hops[way] == k)
                def _():
                    span(lbuf.at[:, 0:k + 1], ag_s.at[way], agp_r.at[0]).wait_send()

    def forward(j):
        at = chunk_rows(j)
        pre = dot(saved[at], eexp[...])
        u = 0.5 * pre
        bent = jnp.tanh(u)
        sigma = 0.5 * bent + 0.5
        value = u * bent + u
        act[at] = value.astype(BF16)
        dsl[at] = (sigma * (1.0 + pre - value)).astype(BF16)

    def backward(j):
        at = chunk_rows(j)
        back = dot(grad[at], ered[...], 1, 1)
        slope[at] = (back * dsl[at].astype(F32)).astype(BF16)

    def downward(j):
        at = pl.ds(pl.multiple_of(j * chunk, chunk), chunk)
        input_grad[at] = (grad[at].astype(F32) + dot(slope[at], eexp[...], 1, 1)).astype(BF16)

    def weight_sums(a, b, lo, hi, places):
        at = pl.ds(lo * depth, (hi - lo) * depth)
        for n in range(wide // 256):
            col = pl.ds(n * 256, 256)
            value = dot(a[:, at], b[:, col], 0, 0).reshape(hi - lo, depth, 256)
            for start, low, high in places:
                gsum[start:start + high - low, :, col] = value[low - lo:high - lo]

    local[0].wait()
    local[1].wait()
    early = max(steps // 2, 1)
    for j in range(early):
        forward(j)
    for dev in range(n_dev):
        first[pl.ds((dev + 1) * padded - 16, 16), :] = jnp.zeros((16, first.shape[1]), BF16)
    for way in range(2):
        @pl.when(hops[way] == 0)
        def _():
            wrx[way] = jnp.zeros(wrx.shape[1:], BF16)
            rx[way] = jnp.zeros(rx.shape[1:], BF16)
    for g in range(G):
        own(g)
        if early + g < steps:
            forward(early + g)
    for j in range(early + G, steps):
        forward(j)
    for copy in local[2:]:
        copy.wait()

    def activate(h):
        total = jnp.zeros((1, half), F32)
        squares = jnp.zeros((1, half), F32)
        for dev in range(n_dev):
            v = lbuf[h, dev].astype(F32)
            total += jnp.sum(v, axis=0, keepdims=True)
            squares += jnp.sum(v * v, axis=0, keepdims=True)
        spread, offset = affine(total, squares, total_rows, gain1[:, cols(h)], shift1[:, cols(h)])
        for dev in range(n_dev):
            v = scaled_silu(lbuf[h, dev].astype(F32), spread, offset)
            first[pl.ds(dev * padded, rows), cols(h)] = v.astype(BF16)

    width = min(256, hid)

    def expand(h):
        for n in range(hid // width):
            at = pl.ds(n * width, width)
            if split:
                value = dot(first[:, cols(h)], wexp[cols(h), at])
                if h > 0:
                    value += inner[:, at]
                if h < H - 1:
                    inner[:, at] = value
            elif h == H - 1:
                value = dot(first[...], wexp[:, at])
            if h == H - 1:
                spread, offset = affine(
                    jnp.sum(value, axis=0, keepdims=True),
                    jnp.sum(value * value, axis=0, keepdims=True),
                    total_rows, gain2[:, at], shift2[:, at],
                )
                hidden[:, at] = scaled_silu(value, spread, offset).astype(BF16)

    groups = ((0, half_r), (half_r, half_r + half_e // 2), (half_r + half_e // 2, share), (share, share + front))

    def swap(n):
        lo, hi = groups[n]
        return remote(gtx.at[lo:hi], gprx.at[lo:hi], gx_s, gx_r.at[n], s, partner)

    def exchange(lane, n):
        @pl.when(other == lane)
        def _():
            for i in range(*groups[n]):
                gtx[i] = gsum[i + share * lane].astype(BF16)
            swap(n).start()

    def met(n):
        swap(n).wait_recv()
        each(*groups[n], sum_first)

    def term(i):
        return gsum[i + share * c] + gprx[i].astype(F32)

    def sum_hop(way, i):
        return remote(wtx.at[way, i], wrx.at[way, i], sum_s.at[way], sum_r.at[way, i], s, nxt[way])

    def sum_first(i):
        for way in range(2):
            @pl.when(hops[way] == 0)
            def _():
                wtx[way, i] = term(i).astype(BF16)
                sum_hop(way, i).start()

    def sum_relay(way, i):
        sum_hop(way, i).wait_recv()

        @pl.when(has_next[way])
        def _():
            wtx[way, i] = (term(i) + wrx[way, i].astype(F32)).astype(BF16)
            sum_hop(way, i).start()

    def each(lo, hi, body):
        def step(i, carry):
            body(i)
            return carry
        lax.fori_loop(lo, hi, step, 0)

    far = last * H
    lead = min(H + LEAD, far)
    for k in range(1, last):
        for g in range(G):
            relay(k, g)
    for h in range(H):
        for g in range(h * U, h * U + U):
            relay(last, g)
        if h == H - 1:
            grad_wait(steps)
            weight_sums(grad, act, 0, front, ((2 * share, 0, front),))
            exchange(1, 3)
        if h > 0:
            gathered(h - 1)
            activate(h - 1)
            expand(h - 1)
    gathered(H - 1)
    activate(H - 1)
    expand(H - 1)

    @pl.when(c == 1)
    def _():
        met(3)

    def pair_copy(h):
        return remote(part.at[other, h], prx.at[h], px_s, px_r.at[h], s, partner)

    def mine(h, chip):
        return part[c, h, chip].astype(F32) + prx[h, chip].astype(F32)

    def goal(way, m):
        return last - m if way == 0 else m

    def row_hop(way, r):
        m, h = r // H, lax.rem(r, H)
        to = goal(way, m)
        return remote(part.at[c, h, to], rx.at[way, h, to], row_s.at[way], row_r.at[way, r], s, nxt[way])

    def row_start(way, r):
        m, h = r // H, lax.rem(r, H)
        to = goal(way, m)
        part[c, h, to] = mine(h, to).astype(BF16)
        row_hop(way, r).start()

    def row_relay(way, r):
        m, h = r // H, lax.rem(r, H)
        to = goal(way, m)

        @pl.when(last - m > hops[way])
        def _():
            row_hop(way, r).wait_recv()
            part[c, h, to] = (mine(h, to) + rx[way, h, to].astype(F32)).astype(BF16)
            row_hop(way, r).start()

    def scatter(h):
        pair_copy(h).wait_recv()
        for way in range(2):
            @pl.when(hops[way] == 0)
            def _():
                row_start(way, h)

    tile = min(256, half)
    for h in range(H):
        for n in range(half // tile):
            value = dot(hidden[...], wred[:, pl.ds(h * half + n * tile, tile)]).astype(BF16)
            for dev in range(n_dev):
                part[dev % 2, h, dev // 2, :, pl.ds(n * tile, tile)] = value[dev * padded:dev * padded + rows]
        pair_copy(h).start()
        if h < steps:
            grad_wait(h)
            backward(h)
        if h > 0:
            scatter(h - 1)

    def rest(r):
        for way in range(2):
            @pl.when(hops[way] == 0)
            def _():
                row_start(way, r)

    scatter(H - 1)
    each(H, lead, rest)
    for j in range(H, steps):
        grad_wait(j)
    weight_sums(grad, act, front, pieces, ((0, front, front + half_r), (share, front + half_r, pieces)))
    for lane in range(2):
        exchange(lane, 0)
    for j in range(H, steps):
        backward(j)
    met(0)
    for way in range(2):
        @pl.when(both(c == 1, hops[way] == 1))
        def _():
            each(share, share + front, functools.partial(sum_relay, way))
    weight_sums(saved, slope, 0, pieces, ((half_r, 0, half_e), (share + half_r, half_e, pieces)))
    for lane in range(2):
        exchange(lane, 1)
        exchange(lane, 2)
    per = front // H
    for h in range(H):
        for way in range(2):
            @pl.when(both(c == 1, hops[way] == 2))
            def _():
                for i in range(per):
                    sum_relay(way, share + h * per + i)
        for way in range(2):
            @pl.when(hops[way] == 1)
            def _():
                row_relay(way, h)
    for way in range(2):
        @pl.when(hops[way] == 2)
        def _():
            for h in range(H // 2):
                row_relay(way, h)

    def give(i, lane):
        piece = gout.at[i + share * lane]
        return remote(piece, piece, wp_s, wp_r, s, partner)

    def sum_finish(i):
        value = term(i) + (wrx[0, i].astype(F32) + wrx[1, i].astype(F32))
        gout[i + share * c] = (value * factor).astype(BF16)
        give(i, c).start()

    met(1)
    met(2)
    each(lead, far, rest)
    count = far + share
    farther = jnp.maximum(hops[0], hops[1])
    calm = H + 2 * SKEW

    def slot(t):
        for way in range(2):
            i = t - SKEW * hops[way]
            live = hops[way] > 0

            @pl.when(both(hops[way] > 1, both(i >= H // 2 * (3 - jnp.minimum(hops[way], 3)), i < H)))
            def _():
                row_relay(way, i)

            @pl.when(both(both(c == 1, hops[way] > 2), both(i >= H, i < H + front)))
            def _():
                sum_relay(way, i - H + share)

            @pl.when(both(live, both(i >= H, i < H + share)))
            def _():
                sum_relay(way, i - H)

            @pl.when(both(live, both(i >= H + share, i < count)))
            def _():
                row_relay(way, i - share)

        i = t - SKEW * farther - H

        @pl.when(both(c == 1, both(i >= 0, i < front)))
        def _():
            sum_finish(i + share)

        @pl.when(both(i >= 0, i < share))
        def _():
            sum_finish(i)

        @pl.when(both(t >= calm, t < calm + steps))
        def _():
            downward(t - calm)

    @pl.when(s < sections - 1)
    def _():
        span(stage, perm_send, perm_recv.at[0]).wait_send()

    @pl.when(s > 0)
    def _():
        remote(up_hbm, grad, gp_send, gp_recv.at[0], s, partner).wait_send()

    gather_drain()
    span(prx, px_s, px_r.at[0]).wait_send()
    for lane in range(2):
        mass = share + front * lane

        @pl.when(other == lane)
        def _():
            span(gtx.at[0:mass], gx_s, gx_r.at[0]).wait_send()

    each(SKEW, max(H + share + SKEW * last, calm + steps), slot)

    for h in range(H):
        for way in range(2):
            @pl.when(hops[way] > 0)
            def _():
                row_hop(way, (last - hops[way]) * H + h).wait_recv()
        value = mine(h, q) + rx[0, h, q].astype(F32) + rx[1, h, q].astype(F32)
        late_out[:, cols(h)] = (lbuf[h, d].astype(F32) + value).astype(BF16)

    for way in range(2):
        for k in range(last):
            @pl.when(hops[way] == k)
            def _():
                span(prx.at[:, 0:last - k], row_s.at[way], px_r.at[0]).wait_send()
    for lane in range(2):
        mass = share + front * lane
        block = gout.at[lane * share:lane * share + mass]

        @pl.when(c == lane)
        def _():
            for way in range(2):
                @pl.when(has_next[way])
                def _():
                    span(wtx.at[way, 0:mass], sum_s.at[way], gx_r.at[0]).wait_send()
            span(block, wp_s, wp_r).wait_send()

        @pl.when(other == lane)
        def _():
            span(block, wp_s, wp_r).wait_recv()


def finish(late_in, grad_in, sums, late_out, input_grad, gexp, gred, wide_e, wide_r, sem):
    ce, fe = wide_e.shape
    a = pltpu.make_async_copy(grad_in, input_grad.at[0], sem.at[0])
    b = pltpu.make_async_copy(late_in, late_out.at[0], sem.at[1])
    a.start()
    b.start()
    pieces, front, share = cuts(ce)
    depth = ce // pieces
    half_r = (pieces - front) // 2
    copies = [a, b]

    def send(src, dst):
        copies.append(pltpu.make_async_copy(src, dst, sem.at[len(copies)]))
        copies[-1].start()

    for lane in range(2):
        at = pl.ds(lane * (ce // 2), ce // 2)
        wide_e[at] = sums[lane * share + half_r:lane * share + share].reshape(ce // 2, fe).astype(F32)
        send(wide_e.at[at], gexp.at[0, at])
    for n in range(fe // 256):
        at = pl.ds(n * 256, 256)
        wide_r[at, 0:front * depth] = sums[2 * share:, :, at].reshape(front * depth, 256).astype(F32).T
        later = [sums[lane:lane + half_r, :, at].reshape(half_r * depth, 256) for lane in (0, share)]
        wide_r[at, front * depth:] = jnp.concatenate(later).astype(F32).T
        send(wide_r.at[at], gred.at[0, at])
    for copy in copies:
        copy.wait()


def shards(
    sections, n_dev,
    late_sent, entry_rows, gain_first, shift_first, expand_late, gain_inner, shift_inner,
    reduce_late, early_saved, upstream_grad, exit_grad, expand_early, reduce_early,
):
    rows, cl = entry_rows.shape
    e_rows, ce = exit_grad.shape
    fe = expand_early.shape[2]
    hid = expand_late.shape[2]
    Q = n_dev // 2
    half = cl // H
    padded = -(-rows // 16) * 16
    chunk = max(k for k in range(16, 257, 16) if e_rows % k == 0)
    steps = e_rows // chunk
    pieces, front, share = cuts(ce)
    depth = ce // pieces
    own = share + front
    split = n_dev * padded * hid * 4 <= 4 * 1024 * 1024
    hbm = pl.BlockSpec(memory_space=pltpu.HBM)
    any_spec = pl.BlockSpec(memory_space=pl.ANY)
    vm = pl.BlockSpec(memory_space=pltpu.VMEM)
    V = pltpu.VMEM
    dma = pltpu.SemaphoreType.DMA
    late_out, input_grad, sums = pl.pallas_call(
        functools.partial(kernel, sections, n_dev, chunk, split),
        out_shape=(
            V((rows, cl), BF16),
            V((e_rows, ce), BF16),
            V((2 * pieces, depth, fe), BF16),
        ),
        in_specs=[hbm] * 13,
        out_specs=(vm, vm, vm),
        scratch_shapes=[
            V((rows, cl), BF16),
            V((H, n_dev, rows, half), BF16),
            V((n_dev * padded, cl), BF16),
            V((n_dev * padded, hid) if split else (8, 128), F32),
            V((n_dev * padded, hid), BF16),
            V((2, H, Q, rows, half), BF16),
            V((H, Q, rows, half), BF16),
            V((2, H, Q, rows, half), BF16),
            V((cl, hid), BF16),
            V((hid, cl), BF16),
            V((e_rows, ce), BF16),
            V((e_rows, ce), BF16),
            V((ce, fe), BF16),
            V((fe, ce), BF16),
            V((e_rows, fe), BF16),
            V((e_rows, fe), BF16),
            V((e_rows, fe), BF16),
            V((2 * pieces, depth, fe), F32),
            V((own, depth, fe), BF16),
            V((own, depth, fe), BF16),
            V((2, own, depth, fe), BF16),
            V((2, own, depth, fe), BF16),
            V((1, cl), F32),
            V((1, cl), F32),
            V((1, hid), F32),
            V((1, hid), F32),
            dma((10,)), dma((H * U,)), dma((steps + 1,)), dma((2, Q - 1, H * U)), dma((H,)), dma((H,)),
            dma((4,)), dma((2, (Q - 1) * H)), dma((2, own)), dma,
            dma, dma, dma((2,)), dma, dma, dma, dma((2,)), dma((2,)), dma,
        ],
        compiler_params=pltpu.CompilerParams(
            collective_id=0, has_side_effects=True, vmem_limit_bytes=60 * 1024 * 1024
        ),
        name="relay",
    )(
        late_sent[0], entry_rows, gain_first, shift_first, expand_late[0], gain_inner, shift_inner,
        reduce_late[0], early_saved[0], upstream_grad[0], exit_grad, expand_early[0], reduce_early[0],
    )
    return pl.pallas_call(
        finish,
        out_shape=(
            jax.ShapeDtypeStruct((1, rows, cl), BF16),
            jax.ShapeDtypeStruct((1, e_rows, ce), BF16),
            jax.ShapeDtypeStruct((1, ce, fe), F32),
            jax.ShapeDtypeStruct((1, fe, ce), F32),
        ),
        in_specs=[vm, vm, vm],
        out_specs=(any_spec,) * 4,
        scratch_shapes=[V((ce, fe), F32), V((fe, ce), F32), dma((4 + fe // 256,))],
        compiler_params=pltpu.CompilerParams(vmem_limit_bytes=16 * 1024 * 1024),
        name="finish",
    )(late_out, input_grad, sums)


def solution(mesh):
    sections, n_dev = mesh.shape["section"], mesh.shape["dev"]
    sd, dd = P("section", "dev", None), P("dev", None)
    rep, one = P("section", None, None), P("section", None)
    in_specs = (
        sd, dd, one, one, P("section", None, "dev"), P("section", "dev"), P("section", "dev"),
        sd, sd, sd, dd, rep, rep,
    )
    return jax.shard_map(
        functools.partial(shards, sections, n_dev), mesh=mesh, in_specs=in_specs,
        out_specs=(sd, sd, rep, rep), check_vma=False,
    )
```

```python
import functools
import math

import jax
import jax.numpy as jnp
from jax import lax
from jax.experimental import pallas as pl
from jax.experimental.pallas import tpu as pltpu
from jax.sharding import PartitionSpec as P

MESH = pl.DeviceIdType.MESH
epsilon = 1e-05
H = 4
U = 2
SKEW = 4
LEAD = 0
F32 = jnp.float32
BF16 = jnp.bfloat16


def scaled_silu(x, spread, offset):
    u = x * (0.5 * spread) + 0.5 * offset
    return u * jnp.tanh(u) + u


def affine(sums, squares, count, gain, shift):
    average = sums / count
    second = squares / count
    spread = gain * lax.rsqrt(second - average * average + epsilon)
    return spread, shift - average * spread


def dot(a, b, ca=1, cb=0):
    return lax.dot_general(a, b, (((ca,), (cb,)), ((), ())), preferred_element_type=F32)


def both(a, b):
    return jnp.logical_and(a, b)


def cuts(ce):
    pieces = ce // 16
    front = pieces // 2
    return pieces, front, (pieces - front) // 2 + pieces // 2


def kernel(
    sections, n_dev, chunk, split,
    late_hbm, entry_hbm, gain1_hbm, shift1_hbm, wexp_hbm, gain2_hbm, shift2_hbm, wred_hbm,
    saved_hbm, up_hbm, exit_hbm, eexp_hbm, ered_hbm,
    late_out, input_grad, gout,
    stage, lbuf, first, inner, hidden, part, prx, rx,
    wexp, wred, saved, grad, eexp, ered, act, dsl, slope,
    gsum, gtx, gprx, wtx, wrx, gain1, shift1, gain2, shift2,
    loc_sem, perm_recv, gp_recv, ag_r, agp_r, px_r, gx_r, row_r, sum_r, wp_r,
    perm_send, gp_send, ag_s, agp_s, px_s, gx_s, row_s, sum_s, wp_s,
):
    Q = n_dev // 2
    s = lax.axis_index("section")
    d = lax.axis_index("dev")
    q = d // 2
    c = lax.rem(d, 2)
    other = 1 - c
    partner = q * 2 + other
    rows = late_hbm.shape[0]
    half = late_hbm.shape[1] // H
    padded = first.shape[0] // n_dev
    e_rows = saved_hbm.shape[0]
    steps = e_rows // chunk
    total_rows = rows * n_dev
    hid = wexp.shape[1]
    wide = eexp.shape[1]
    ce = grad.shape[1]
    pieces, front, share = cuts(ce)
    depth = ce // pieces
    half_r, half_e = (pieces - front) // 2, pieces // 2
    ahead = front * depth
    factor = 1.0 / math.sqrt(e_rows * n_dev)

    last = Q - 1
    right, left = jnp.minimum(q + 1, last), jnp.maximum(q - 1, 0)
    nxt = (right * 2 + c, left * 2 + c)
    has_next = (q < last, q > 0)
    has_prev = (q > 0, q < last)
    hops = (q, last - q)

    barrier = pltpu.get_barrier_semaphore()
    pl.semaphore_signal(barrier, inc=1, device_id=(s, partner), device_id_type=MESH)
    for way in range(2):
        @pl.when(has_next[way])
        def _():
            pl.semaphore_signal(barrier, inc=1, device_id=(s, nxt[way]), device_id_type=MESH)

    @pl.when(s > 0)
    def _():
        pl.semaphore_signal(barrier, inc=1, device_id=(s - 1, d), device_id_type=MESH)

    @pl.when(s < sections - 1)
    def _():
        pl.semaphore_signal(barrier, inc=1, device_id=(s + 1, d), device_id_type=MESH)

    stage_copy = pltpu.make_async_copy(late_hbm, stage, loc_sem.at[9])
    stage_copy.start()
    local = [
        pltpu.make_async_copy(src, dst, loc_sem.at[i])
        for i, (src, dst) in enumerate(
            (
                (saved_hbm, saved), (eexp_hbm, eexp), (ered_hbm, ered), (wexp_hbm, wexp), (wred_hbm, wred),
                (gain1_hbm, gain1), (shift1_hbm, shift1), (gain2_hbm, gain2), (shift2_hbm, shift2),
            )
        )
    ]
    for copy in local:
        copy.start()

    def remote(src, dst, send, recv, section, dev):
        return pltpu.make_async_remote_copy(
            src_ref=src, dst_ref=dst, send_sem=send, recv_sem=recv,
            device_id=(section, dev), device_id_type=MESH,
        )

    def cols(h):
        return pl.ds(h * half, half)

    cut = [(0, u * (half // U), half // U) for u in range(U)] + [(h, 0, half) for h in range(1, H)]
    G = len(cut)

    def fine_cols(g):
        h, at, size = cut[g]
        return pl.ds(h * half + at, size)

    def rows_of(g, dev):
        h, at, size = cut[g]
        return lbuf.at[h, dev, :, pl.ds(at, size)]

    def parts_of(h):
        return [g for g in range(G) if cut[g][0] == h]

    def late_copy(g):
        return remote(
            stage.at[:, fine_cols(g)], rows_of(g, d), perm_send, perm_recv.at[g],
            jnp.minimum(s + 1, sections - 1), d,
        )

    def entry_copy(g):
        return pltpu.make_async_copy(entry_hbm.at[:, fine_cols(g)], rows_of(g, d), perm_recv.at[g])

    def chunk_rows(j):
        return pl.ds(j * chunk, chunk)

    def grad_at(j):
        if j == steps:
            return slice(None), pl.ds(0, ahead)
        return chunk_rows(j), pl.ds(ahead, ce - ahead)

    def grad_copy(j):
        return remote(
            up_hbm.at[grad_at(j)], grad.at[grad_at(j)], gp_send, gp_recv.at[j],
            jnp.maximum(s - 1, 0), d,
        )

    def exit_copy(j):
        return pltpu.make_async_copy(exit_hbm.at[grad_at(j)], grad.at[grad_at(j)], gp_recv.at[j])

    def grad_wait(j):
        @pl.when(s < sections - 1)
        def _():
            grad_copy(j).wait_recv()

        @pl.when(s == sections - 1)
        def _():
            exit_copy(j).wait()

    stage_copy.wait()
    pl.semaphore_wait(
        barrier,
        1 + jnp.minimum(q, 1) + jnp.minimum(last - q, 1) + jnp.minimum(s, 1) + jnp.minimum(sections - 1 - s, 1),
    )

    @pl.when(s < sections - 1)
    def _():
        for g in range(G):
            late_copy(g).start()

    @pl.when(s == 0)
    def _():
        for g in range(G):
            entry_copy(g).start()

    @pl.when(s > 0)
    def _():
        for j in (steps, *range(steps)):
            grad_copy(j).start()

    @pl.when(s == sections - 1)
    def _():
        for j in (steps, *range(steps)):
            exit_copy(j).start()

    def source(way, k):
        return jnp.maximum(q - k, 0) if way == 0 else jnp.minimum(q + k, last)

    def have(way, k):
        return hops[way] >= k

    def hop(way, k, h):
        piece = rows_of(h, source(way, k) * 2 + c)
        return remote(piece, piece, ag_s.at[way], ag_r.at[way, k, h], s, nxt[way])

    def arrival(way, k, h):
        piece = rows_of(h, source(way, k) * 2 + c)
        return remote(piece, piece, ag_s.at[way], ag_r.at[way, k - 1, h], s, nxt[way])

    def lend(way, k, h, lane):
        piece = rows_of(h, source(way, k) * 2 + lane)
        return remote(piece, piece, agp_s, agp_r.at[cut[h][0]], s, partner)

    def own(h):
        @pl.when(s == 0)
        def _():
            entry_copy(h).wait()

        @pl.when(s > 0)
        def _():
            late_copy(h).wait_recv()

        for way in range(2):
            @pl.when(has_next[way])
            def _():
                hop(way, 0, h).start()
        lend(0, 0, h, c).start()

    def relay(k, h):
        for way in range(2):
            @pl.when(have(way, k))
            def _():
                arrival(way, k, h).wait_recv()
                if k < last:
                    @pl.when(has_next[way])
                    def _():
                        hop(way, k, h).start()
                lend(way, k, h, c).start()

    def span(buf, send, recv):
        return remote(buf, buf, send, recv, s, partner)

    def gathered(h):
        span(lbuf.at[h, 0:Q], agp_s, agp_r.at[h]).wait_recv()

    def gather_drain():
        span(lbuf.at[:, 0:Q], agp_s, agp_r.at[0]).wait_send()
        for way in range(2):
            for k in range(last):
                @pl.when(hops[way] == k)
                def _():
                    span(lbuf.at[:, 0:k + 1], ag_s.at[way], agp_r.at[0]).wait_send()

    def forward(j):
        at = chunk_rows(j)
        pre = dot(saved[at], eexp[...])
        u = 0.5 * pre
        bent = jnp.tanh(u)
        sigma = 0.5 * bent + 0.5
        value = u * bent + u
        act[at] = value.astype(BF16)
        dsl[at] = (sigma * (1.0 + pre - value)).astype(BF16)

    def backward(j):
        at = chunk_rows(j)
        back = dot(grad[at], ered[...], 1, 1)
        slope[at] = (back * dsl[at].astype(F32)).astype(BF16)

    def downward(j):
        at = pl.ds(pl.multiple_of(j * chunk, chunk), chunk)
        input_grad[at] = (grad[at].astype(F32) + dot(slope[at], eexp[...], 1, 1)).astype(BF16)

    def weight_sums(a, b, lo, hi, places):
        at = pl.ds(lo * depth, (hi - lo) * depth)
        for n in range(wide // 256):
            col = pl.ds(n * 256, 256)
            value = dot(a[:, at], b[:, col], 0, 0).reshape(hi - lo, depth, 256)
            for start, low, high in places:
                gsum[start:start + high - low, :, col] = value[low - lo:high - lo]

    local[0].wait()
    local[1].wait()
    early = max(steps // 2, 1)
    for j in range(early):
        forward(j)
    for dev in range(n_dev):
        first[pl.ds((dev + 1) * padded - 16, 16), :] = jnp.zeros((16, first.shape[1]), BF16)
    for way in range(2):
        @pl.when(hops[way] == 0)
        def _():
            wrx[way] = jnp.zeros(wrx.shape[1:], BF16)
            rx[way] = jnp.zeros(rx.shape[1:], BF16)
    for g in range(G):
        own(g)
        if early + g < steps:
            forward(early + g)
    for j in range(early + G, steps):
        forward(j)
    for copy in local[2:]:
        copy.wait()

    def activate(h):
        total = jnp.zeros((1, half), F32)
        squares = jnp.zeros((1, half), F32)
        for dev in range(n_dev):
            v = lbuf[h, dev].astype(F32)
            total += jnp.sum(v, axis=0, keepdims=True)
            squares += jnp.sum(v * v, axis=0, keepdims=True)
        spread, offset = affine(total, squares, total_rows, gain1[:, cols(h)], shift1[:, cols(h)])
        for dev in range(n_dev):
            v = scaled_silu(lbuf[h, dev].astype(F32), spread, offset)
            first[pl.ds(dev * padded, rows), cols(h)] = v.astype(BF16)

    width = min(256, hid)

    def expand(h):
        for n in range(hid // width):
            at = pl.ds(n * width, width)
            if split:
                value = dot(first[:, cols(h)], wexp[cols(h), at])
                if h > 0:
                    value += inner[:, at]
                if h < H - 1:
                    inner[:, at] = value
            elif h == H - 1:
                value = dot(first[...], wexp[:, at])
            if h == H - 1:
                spread, offset = affine(
                    jnp.sum(value, axis=0, keepdims=True),
                    jnp.sum(value * value, axis=0, keepdims=True),
                    total_rows, gain2[:, at], shift2[:, at],
                )
                hidden[:, at] = scaled_silu(value, spread, offset).astype(BF16)

    groups = ((0, half_r), (half_r, half_r + half_e // 2), (half_r + half_e // 2, share), (share, share + front))

    def swap(n):
        lo, hi = groups[n]
        return remote(gtx.at[lo:hi], gprx.at[lo:hi], gx_s, gx_r.at[n], s, partner)

    def exchange(lane, n):
        @pl.when(other == lane)
        def _():
            for i in range(*groups[n]):
                gtx[i] = gsum[i + share * lane].astype(BF16)
            swap(n).start()

    def met(n):
        swap(n).wait_recv()
        each(*groups[n], sum_first)

    def term(i):
        return gsum[i + share * c] + gprx[i].astype(F32)

    def sum_hop(way, i):
        return remote(wtx.at[way, i], wrx.at[way, i], sum_s.at[way], sum_r.at[way, i], s, nxt[way])

    def sum_first(i):
        for way in range(2):
            @pl.when(hops[way] == 0)
            def _():
                wtx[way, i] = term(i).astype(BF16)
                sum_hop(way, i).start()

    def sum_relay(way, i):
        sum_hop(way, i).wait_recv()

        @pl.when(has_next[way])
        def _():
            wtx[way, i] = (term(i) + wrx[way, i].astype(F32)).astype(BF16)
            sum_hop(way, i).start()

    def each(lo, hi, body):
        def step(i, carry):
            body(i)
            return carry
        lax.fori_loop(lo, hi, step, 0)

    far = last * H
    lead = min(H + LEAD, far)
    for k in range(1, last):
        for g in range(G):
            relay(k, g)
    for h in range(H):
        for g in parts_of(h):
            relay(last, g)
        if h == H - 1:
            grad_wait(steps)
            weight_sums(grad, act, 0, front, ((2 * share, 0, front),))
            exchange(1, 3)
        if h > 0:
            gathered(h - 1)
            activate(h - 1)
            expand(h - 1)

    gathered(H - 1)
    activate(H - 1)
    expand(H - 1)

    @pl.when(c == 1)
    def _():
        met(3)

    def pair_copy(h):
        return remote(part.at[other, h], prx.at[h], px_s, px_r.at[h], s, partner)

    rem = rows % 8
    main = rows - rem
    tall = part.shape[3]

    height = (pl.ds(0, main), pl.ds(0, tall))

    def forms(h, body):
        @pl.when(h < H - 1)
        def _():
            body(0)

        @pl.when(h == H - 1)
        def _():
            body(1)

    def mine(h, chip):
        return part[c, h, chip].astype(F32) + prx[h, chip].astype(F32)

    def goal(way, m):
        return last - m if way == 0 else m

    def row_hop(way, r, kind):
        m, h = r // H, lax.rem(r, H)
        to, at = goal(way, m), height[kind]
        return remote(
            part.at[c, h, to, at], rx.at[way, h, to, at], row_s.at[way, kind], row_r.at[way, r], s, nxt[way],
        )

    def row_start(way, r):
        m, h = r // H, lax.rem(r, H)
        to = goal(way, m)
        part[c, h, to] = mine(h, to).astype(BF16)
        forms(h, lambda kind: row_hop(way, r, kind).start())

    def row_relay(way, r):
        m, h = r // H, lax.rem(r, H)
        to = goal(way, m)

        @pl.when(last - m > hops[way])
        def _():
            forms(h, lambda kind: row_hop(way, r, kind).wait_recv())
            part[c, h, to] = (mine(h, to) + rx[way, h, to].astype(F32)).astype(BF16)
            forms(h, lambda kind: row_hop(way, r, kind).start())

    def scatter(h):
        pair_copy(h).wait_recv()
        for way in range(2):
            @pl.when(hops[way] == 0)
            def _():
                row_start(way, h)

    tile = min(256, half)
    for h in range(H):
        for n in range(half // tile):
            value = dot(hidden[...], wred[:, pl.ds(h * half + n * tile, tile)]).astype(BF16)
            for dev in range(n_dev):
                low, col = dev * padded, pl.ds(n * tile, tile)
                part[dev % 2, h, dev // 2, 0:main, col] = value[low:low + main]
                if rem:
                    tail = main + rem * h
                    part[dev % 2, H - 1, dev // 2, tail:tail + rem, col] = value[low + main:low + rows]
        pair_copy(h).start()
        if h < steps:
            grad_wait(h)
            backward(h)
        if h > 0:
            scatter(h - 1)

    def rest(r):
        for way in range(2):
            @pl.when(hops[way] == 0)
            def _():
                row_start(way, r)

    scatter(H - 1)
    each(H, lead, rest)
    for j in range(H, steps):
        grad_wait(j)
    weight_sums(grad, act, front, pieces, ((0, front, front + half_r), (share, front + half_r, pieces)))
    for lane in range(2):
        exchange(lane, 0)
    for j in range(H, steps):
        backward(j)
    met(0)
    for way in range(2):
        @pl.when(both(c == 1, hops[way] == 1))
        def _():
            each(share, share + front, functools.partial(sum_relay, way))
    weight_sums(saved, slope, 0, pieces, ((half_r, 0, half_e), (share + half_r, half_e, pieces)))
    for lane in range(2):
        exchange(lane, 1)
        exchange(lane, 2)
    per = front // H
    for h in range(H):
        for way in range(2):
            @pl.when(both(c == 1, hops[way] == 2))
            def _():
                for i in range(per):
                    sum_relay(way, share + h * per + i)
        for way in range(2):
            @pl.when(hops[way] == 1)
            def _():
                row_relay(way, h)
    for way in range(2):
        @pl.when(hops[way] == 2)
        def _():
            for h in range(H // 2):
                row_relay(way, h)

    def give(i, lane):
        piece = gout.at[i + share * lane]
        return remote(piece, piece, wp_s, wp_r, s, partner)

    def sum_finish(i):
        value = term(i) + (wrx[0, i].astype(F32) + wrx[1, i].astype(F32))
        gout[i + share * c] = (value * factor).astype(BF16)
        give(i, c).start()

    met(1)
    met(2)
    each(lead, far, rest)
    count = far + share
    farther = jnp.maximum(hops[0], hops[1])

    def slot(t):
        for way in range(2):
            i = t - SKEW * hops[way]
            live = hops[way] > 0

            @pl.when(both(hops[way] > 1, both(i >= H // 2 * (3 - jnp.minimum(hops[way], 3)), i < H)))
            def _():
                row_relay(way, i)

            @pl.when(both(both(c == 1, hops[way] > 2), both(i >= H, i < H + front)))
            def _():
                sum_relay(way, i - H + share)

            @pl.when(both(live, both(i >= H, i < H + share)))
            def _():
                sum_relay(way, i - H)

            @pl.when(both(live, both(i >= H + share, i < count)))
            def _():
                row_relay(way, i - share)

        i = t - SKEW * farther - H

        @pl.when(both(c == 1, both(i >= 0, i < front)))
        def _():
            sum_finish(i + share)

        @pl.when(both(i >= 0, i < share))
        def _():
            sum_finish(i)

    @pl.when(s < sections - 1)
    def _():
        span(stage, perm_send, perm_recv.at[0]).wait_send()

    @pl.when(s > 0)
    def _():
        remote(up_hbm, grad, gp_send, gp_recv.at[0], s, partner).wait_send()

    gather_drain()
    span(prx, px_s, px_r.at[0]).wait_send()
    for lane in range(2):
        mass = share + front * lane

        @pl.when(other == lane)
        def _():
            span(gtx.at[0:mass], gx_s, gx_r.at[0]).wait_send()

    @pl.when(farther == last)
    def _():
        each(0, steps, downward)

    each(SKEW, H + share + SKEW * last, slot)

    @pl.when(farther < last)
    def _():
        each(0, steps, downward)


    for h in range(H):
        for way in range(2):
            @pl.when(hops[way] > 0)
            def _():
                row_hop(way, (last - hops[way]) * H + h, h // (H - 1)).wait_recv()
        value = mine(h, q) + rx[0, h, q].astype(F32) + rx[1, h, q].astype(F32)
        late_out[0:main, cols(h)] = (lbuf[h, d, 0:main].astype(F32) + value[0:main]).astype(BF16)
    if rem:
        for h in range(H):
            tail = main + rem * h
            end = lbuf[h, d, main:rows].astype(F32) + value[tail:tail + rem]
            late_out[main:rows, cols(h)] = end.astype(BF16)

    for way in range(2):
        for k in range(last):
            @pl.when(hops[way] == k)
            def _():
                for kind, planes in enumerate((pl.ds(0, H - 1), pl.ds(H - 1, 1))):
                    span(prx.at[planes, 0:last - k, height[kind]], row_s.at[way, kind], px_r.at[0]).wait_send()
    for lane in range(2):
        mass = share + front * lane
        block = gout.at[lane * share:lane * share + mass]

        @pl.when(c == lane)
        def _():
            for way in range(2):
                @pl.when(has_next[way])
                def _():
                    span(wtx.at[way, 0:mass], sum_s.at[way], gx_r.at[0]).wait_send()
            span(block, wp_s, wp_r).wait_send()

        @pl.when(other == lane)
        def _():
            span(block, wp_s, wp_r).wait_recv()


def finish(late_in, grad_in, sums, late_out, input_grad, gexp, gred, wide_e, wide_r, sem):
    ce, fe = wide_e.shape
    a = pltpu.make_async_copy(grad_in, input_grad.at[0], sem.at[0])
    b = pltpu.make_async_copy(late_in, late_out.at[0], sem.at[1])
    a.start()
    b.start()
    pieces, front, share = cuts(ce)
    depth = ce // pieces
    half_r = (pieces - front) // 2
    copies = [a, b]

    def send(src, dst):
        copies.append(pltpu.make_async_copy(src, dst, sem.at[len(copies)]))
        copies[-1].start()

    for lane in range(2):
        at = pl.ds(lane * (ce // 2), ce // 2)
        wide_e[at] = sums[lane * share + half_r:lane * share + share].reshape(ce // 2, fe).astype(F32)
        send(wide_e.at[at], gexp.at[0, at])
    for n in range(fe // 256):
        at = pl.ds(n * 256, 256)
        wide_r[at, 0:front * depth] = sums[2 * share:, :, at].reshape(front * depth, 256).T.astype(F32)
        later = [sums[lane:lane + half_r, :, at].reshape(half_r * depth, 256) for lane in (0, share)]
        wide_r[at, front * depth:] = jnp.concatenate(later).T.astype(F32)
        send(wide_r.at[at], gred.at[0, at])
    for copy in copies:
        copy.wait()


def shards(
    sections, n_dev,
    late_sent, entry_rows, gain_first, shift_first, expand_late, gain_inner, shift_inner,
    reduce_late, early_saved, upstream_grad, exit_grad, expand_early, reduce_early,
):
    rows, cl = entry_rows.shape
    e_rows, ce = exit_grad.shape
    fe = expand_early.shape[2]
    hid = expand_late.shape[2]
    Q = n_dev // 2
    half = cl // H
    padded = -(-rows // 16) * 16
    tall = rows + (H - 1) * (rows % 8)
    chunk = max(k for k in range(16, 257, 16) if e_rows % k == 0)
    steps = e_rows // chunk
    pieces, front, share = cuts(ce)
    depth = ce // pieces
    own = share + front
    split = n_dev * padded * hid * 4 <= 4 * 1024 * 1024
    hbm = pl.BlockSpec(memory_space=pltpu.HBM)
    any_spec = pl.BlockSpec(memory_space=pl.ANY)
    vm = pl.BlockSpec(memory_space=pltpu.VMEM)
    V = pltpu.VMEM
    dma = pltpu.SemaphoreType.DMA
    late_out, input_grad, sums = pl.pallas_call(
        functools.partial(kernel, sections, n_dev, chunk, split),
        out_shape=(
            V((rows, cl), BF16),
            V((e_rows, ce), BF16),
            V((2 * pieces, depth, fe), BF16),
        ),
        in_specs=[hbm] * 13,
        out_specs=(vm, vm, vm),
        scratch_shapes=[
            V((rows, cl), BF16),
            V((H, n_dev, rows, half), BF16),
            V((n_dev * padded, cl), BF16),
            V((n_dev * padded, hid) if split else (8, 128), F32),
            V((n_dev * padded, hid), BF16),
            V((2, H, Q, tall, half), BF16),
            V((H, Q, tall, half), BF16),
            V((2, H, Q, tall, half), BF16),
            V((cl, hid), BF16),
            V((hid, cl), BF16),
            V((e_rows, ce), BF16),
            V((e_rows, ce), BF16),
            V((ce, fe), BF16),
            V((fe, ce), BF16),
            V((e_rows, fe), BF16),
            V((e_rows, fe), BF16),
            V((e_rows, fe), BF16),
            V((2 * pieces, depth, fe), F32),
            V((own, depth, fe), BF16),
            V((own, depth, fe), BF16),
            V((2, own, depth, fe), BF16),
            V((2, own, depth, fe), BF16),
            V((1, cl), F32),
            V((1, cl), F32),
            V((1, hid), F32),
            V((1, hid), F32),
            dma((10,)), dma((H + U - 1,)), dma((steps + 1,)), dma((2, Q - 1, H + U - 1)), dma((H,)), dma((H,)),
            dma((4,)), dma((2, (Q - 1) * H)), dma((2, own)), dma,
            dma, dma, dma((2,)), dma, dma, dma, dma((2, 2)), dma((2,)), dma,
        ],
        compiler_params=pltpu.CompilerParams(
            collective_id=0, has_side_effects=True, vmem_limit_bytes=60 * 1024 * 1024
        ),
        name="relay",
    )(
        late_sent[0], entry_rows, gain_first, shift_first, expand_late[0], gain_inner, shift_inner,
        reduce_late[0], early_saved[0], upstream_grad[0], exit_grad, expand_early[0], reduce_early[0],
    )
    return pl.pallas_call(
        finish,
        out_shape=(
            jax.ShapeDtypeStruct((1, rows, cl), BF16),
            jax.ShapeDtypeStruct((1, e_rows, ce), BF16),
            jax.ShapeDtypeStruct((1, ce, fe), F32),
            jax.ShapeDtypeStruct((1, fe, ce), F32),
        ),
        in_specs=[vm, vm, vm],
        out_specs=(any_spec,) * 4,
        scratch_shapes=[V((ce, fe), F32), V((fe, ce), F32), dma((4 + fe // 256,))],
        compiler_params=pltpu.CompilerParams(vmem_limit_bytes=16 * 1024 * 1024),
        name="finish",
    )(late_out, input_grad, sums)


def solution(mesh):
    sections, n_dev = mesh.shape["section"], mesh.shape["dev"]
    sd, dd = P("section", "dev", None), P("dev", None)
    rep, one = P("section", None, None), P("section", None)
    in_specs = (
        sd, dd, one, one, P("section", None, "dev"), P("section", "dev"), P("section", "dev"),
        sd, sd, sd, dd, rep, rep,
    )
    return jax.shard_map(
        functools.partial(shards, sections, n_dev), mesh=mesh, in_specs=in_specs,
        out_specs=(sd, sd, rep, rep), check_vma=False,
    )
```

```python
import functools
import math

import jax
import jax.numpy as jnp
from jax import lax
from jax.experimental import pallas as pl
from jax.experimental.pallas import tpu as pltpu
from jax.sharding import PartitionSpec as P

MESH = pl.DeviceIdType.MESH
epsilon = 1e-05
H = 4
U = 2
SKEW = 4
LEAD = 1
F32 = jnp.float32
BF16 = jnp.bfloat16


def scaled_silu(x, spread, offset):
    u = x * (0.5 * spread) + 0.5 * offset
    return u * jnp.tanh(u) + u


def affine(sums, squares, count, gain, shift):
    average = sums / count
    second = squares / count
    spread = gain * lax.rsqrt(second - average * average + epsilon)
    return spread, shift - average * spread


def dot(a, b, ca=1, cb=0):
    return lax.dot_general(a, b, (((ca,), (cb,)), ((), ())), preferred_element_type=F32)


def both(a, b):
    return jnp.logical_and(a, b)


def cuts(ce):
    pieces = ce // 16
    front = pieces // 2
    return pieces, front, (pieces - front) // 2 + pieces // 2


def kernel(
    sections, n_dev, chunk, split,
    late_hbm, entry_hbm, gain1_hbm, shift1_hbm, wexp_hbm, gain2_hbm, shift2_hbm, wred_hbm,
    saved_hbm, up_hbm, exit_hbm, eexp_hbm, ered_hbm,
    late_out, input_grad, gout,
    stage, lbuf, first, inner, hidden, part, prx, rx,
    wexp, wred, saved, grad, eexp, ered, act, dsl, slope,
    gsum, gtx, gprx, wtx, wrx, gain1, shift1, gain2, shift2,
    loc_sem, perm_recv, gp_recv, ag_r, agp_r, px_r, gx_r, row_r, sum_r, wp_r,
    perm_send, gp_send, ag_s, agp_s, px_s, gx_s, row_s, sum_s, wp_s,
):
    Q = n_dev // 2
    s = lax.axis_index("section")
    d = lax.axis_index("dev")
    q = d // 2
    c = lax.rem(d, 2)
    other = 1 - c
    partner = q * 2 + other
    rows = late_hbm.shape[0]
    half = late_hbm.shape[1] // H
    padded = first.shape[0] // n_dev
    e_rows = saved_hbm.shape[0]
    steps = e_rows // chunk
    total_rows = rows * n_dev
    hid = wexp.shape[1]
    wide = eexp.shape[1]
    ce = grad.shape[1]
    pieces, front, share = cuts(ce)
    depth = ce // pieces
    half_r, half_e = (pieces - front) // 2, pieces // 2
    ahead = front * depth
    factor = 1.0 / math.sqrt(e_rows * n_dev)

    last = Q - 1
    right, left = jnp.minimum(q + 1, last), jnp.maximum(q - 1, 0)
    nxt = (right * 2 + c, left * 2 + c)
    has_next = (q < last, q > 0)
    has_prev = (q > 0, q < last)
    hops = (q, last - q)

    barrier = pltpu.get_barrier_semaphore()
    pl.semaphore_signal(barrier, inc=1, device_id=(s, partner), device_id_type=MESH)
    for way in range(2):
        @pl.when(has_next[way])
        def _():
            pl.semaphore_signal(barrier, inc=1, device_id=(s, nxt[way]), device_id_type=MESH)

    @pl.when(s > 0)
    def _():
        pl.semaphore_signal(barrier, inc=1, device_id=(s - 1, d), device_id_type=MESH)

    @pl.when(s < sections - 1)
    def _():
        pl.semaphore_signal(barrier, inc=1, device_id=(s + 1, d), device_id_type=MESH)

    stage_copy = pltpu.make_async_copy(late_hbm, stage, loc_sem.at[9])
    stage_copy.start()
    local = [
        pltpu.make_async_copy(src, dst, loc_sem.at[i])
        for i, (src, dst) in enumerate(
            (
                (saved_hbm, saved), (eexp_hbm, eexp), (ered_hbm, ered), (wexp_hbm, wexp), (wred_hbm, wred),
                (gain1_hbm, gain1), (shift1_hbm, shift1), (gain2_hbm, gain2), (shift2_hbm, shift2),
            )
        )
    ]
    for copy in local:
        copy.start()

    def remote(src, dst, send, recv, section, dev):
        return pltpu.make_async_remote_copy(
            src_ref=src, dst_ref=dst, send_sem=send, recv_sem=recv,
            device_id=(section, dev), device_id_type=MESH,
        )

    def cols(h):
        return pl.ds(h * half, half)

    cut = [(0, u * (half // U), half // U) for u in range(U)] + [(h, 0, half) for h in range(1, H)]
    G = len(cut)

    def fine_cols(g):
        h, at, size = cut[g]
        return pl.ds(h * half + at, size)

    def rows_of(g, dev):
        h, at, size = cut[g]
        return lbuf.at[h, dev, :, pl.ds(at, size)]

    def parts_of(h):
        return [g for g in range(G) if cut[g][0] == h]

    def late_copy(g):
        return remote(
            stage.at[:, fine_cols(g)], rows_of(g, d), perm_send, perm_recv.at[g],
            jnp.minimum(s + 1, sections - 1), d,
        )

    def entry_copy(g):
        return pltpu.make_async_copy(entry_hbm.at[:, fine_cols(g)], rows_of(g, d), perm_recv.at[g])

    def chunk_rows(j):
        return pl.ds(j * chunk, chunk)

    def grad_at(j):
        if j == steps:
            return slice(None), pl.ds(0, ahead)
        return chunk_rows(j), pl.ds(ahead, ce - ahead)

    def grad_copy(j):
        return remote(
            up_hbm.at[grad_at(j)], grad.at[grad_at(j)], gp_send, gp_recv.at[j],
            jnp.maximum(s - 1, 0), d,
        )

    def exit_copy(j):
        return pltpu.make_async_copy(exit_hbm.at[grad_at(j)], grad.at[grad_at(j)], gp_recv.at[j])

    def grad_wait(j):
        @pl.when(s < sections - 1)
        def _():
            grad_copy(j).wait_recv()

        @pl.when(s == sections - 1)
        def _():
            exit_copy(j).wait()

    stage_copy.wait()
    pl.semaphore_wait(
        barrier,
        1 + jnp.minimum(q, 1) + jnp.minimum(last - q, 1) + jnp.minimum(s, 1) + jnp.minimum(sections - 1 - s, 1),
    )

    @pl.when(s < sections - 1)
    def _():
        for g in range(G):
            late_copy(g).start()

    @pl.when(s == 0)
    def _():
        for g in range(G):
            entry_copy(g).start()

    @pl.when(s > 0)
    def _():
        for j in (steps, *range(steps)):
            grad_copy(j).start()

    @pl.when(s == sections - 1)
    def _():
        for j in (steps, *range(steps)):
            exit_copy(j).start()

    def source(way, k):
        return jnp.maximum(q - k, 0) if way == 0 else jnp.minimum(q + k, last)

    def have(way, k):
        return hops[way] >= k

    def hop(way, k, h):
        piece = rows_of(h, source(way, k) * 2 + c)
        return remote(piece, piece, ag_s.at[way], ag_r.at[way, k, h], s, nxt[way])

    def arrival(way, k, h):
        piece = rows_of(h, source(way, k) * 2 + c)
        return remote(piece, piece, ag_s.at[way], ag_r.at[way, k - 1, h], s, nxt[way])

    def lend(way, k, h, lane):
        piece = rows_of(h, source(way, k) * 2 + lane)
        return remote(piece, piece, agp_s, agp_r.at[cut[h][0]], s, partner)

    def own(h):
        @pl.when(s == 0)
        def _():
            entry_copy(h).wait()

        @pl.when(s > 0)
        def _():
            late_copy(h).wait_recv()

        for way in range(2):
            @pl.when(has_next[way])
            def _():
                hop(way, 0, h).start()
        lend(0, 0, h, c).start()

    def relay(k, h):
        for way in range(2):
            @pl.when(have(way, k))
            def _():
                arrival(way, k, h).wait_recv()
                if k < last:
                    @pl.when(has_next[way])
                    def _():
                        hop(way, k, h).start()
                lend(way, k, h, c).start()

    def span(buf, send, recv):
        return remote(buf, buf, send, recv, s, partner)

    def gathered(h):
        span(lbuf.at[h, 0:Q], agp_s, agp_r.at[h]).wait_recv()

    def gather_drain():
        span(lbuf.at[:, 0:Q], agp_s, agp_r.at[0]).wait_send()
        for way in range(2):
            for k in range(last):
                @pl.when(hops[way] == k)
                def _():
                    span(lbuf.at[:, 0:k + 1], ag_s.at[way], agp_r.at[0]).wait_send()

    def forward(j):
        at = chunk_rows(j)
        pre = dot(saved[at], eexp[...])
        u = 0.5 * pre
        bent = jnp.tanh(u)
        sigma = 0.5 * bent + 0.5
        value = u * bent + u
        act[at] = value.astype(BF16)
        dsl[at] = (sigma * (1.0 + pre - value)).astype(BF16)

    def backward(j):
        at = chunk_rows(j)
        back = dot(grad[at], ered[...], 1, 1)
        slope[at] = (back * dsl[at].astype(F32)).astype(BF16)

    def downward(j):
        at = pl.ds(pl.multiple_of(j * chunk, chunk), chunk)
        input_grad[at] = (grad[at].astype(F32) + dot(slope[at], eexp[...], 1, 1)).astype(BF16)

    def weight_sums(a, b, lo, hi, places):
        at = pl.ds(lo * depth, (hi - lo) * depth)
        for n in range(wide // 256):
            col = pl.ds(n * 256, 256)
            value = dot(a[:, at], b[:, col], 0, 0).reshape(hi - lo, depth, 256)
            for start, low, high in places:
                gsum[start:start + high - low, :, col] = value[low - lo:high - lo]

    local[0].wait()
    local[1].wait()
    early = max(steps // 2, 1)
    for j in range(early):
        forward(j)
    for dev in range(n_dev):
        first[pl.ds((dev + 1) * padded - 16, 16), :] = jnp.zeros((16, first.shape[1]), BF16)
    for way in range(2):
        @pl.when(hops[way] == 0)
        def _():
            wrx[way] = jnp.zeros(wrx.shape[1:], BF16)
            rx[way] = jnp.zeros(rx.shape[1:], BF16)
    for g in range(G):
        own(g)
        if early + g < steps:
            forward(early + g)
    for j in range(early + G, steps):
        forward(j)
    for copy in local[2:]:
        copy.wait()

    def activate(h):
        total = jnp.zeros((1, half), F32)
        squares = jnp.zeros((1, half), F32)
        for dev in range(n_dev):
            v = lbuf[h, dev].astype(F32)
            total += jnp.sum(v, axis=0, keepdims=True)
            squares += jnp.sum(v * v, axis=0, keepdims=True)
        spread, offset = affine(total, squares, total_rows, gain1[:, cols(h)], shift1[:, cols(h)])
        for dev in range(n_dev):
            v = scaled_silu(lbuf[h, dev].astype(F32), spread, offset)
            first[pl.ds(dev * padded, rows), cols(h)] = v.astype(BF16)

    width = min(256, hid)

    def expand(h):
        for n in range(hid // width):
            at = pl.ds(n * width, width)
            if split:
                value = dot(first[:, cols(h)], wexp[cols(h), at])
                if h > 0:
                    value += inner[:, at]
                if h < H - 1:
                    inner[:, at] = value
            elif h == H - 1:
                value = dot(first[...], wexp[:, at])
            if h == H - 1:
                spread, offset = affine(
                    jnp.sum(value, axis=0, keepdims=True),
                    jnp.sum(value * value, axis=0, keepdims=True),
                    total_rows, gain2[:, at], shift2[:, at],
                )
                hidden[:, at] = scaled_silu(value, spread, offset).astype(BF16)

    groups = ((0, half_r), (half_r, half_r + half_e // 2), (half_r + half_e // 2, share), (share, share + front))

    def swap(n):
        lo, hi = groups[n]
        return remote(gtx.at[lo:hi], gprx.at[lo:hi], gx_s, gx_r.at[n], s, partner)

    def exchange(lane, n):
        @pl.when(other == lane)
        def _():
            for i in range(*groups[n]):
                gtx[i] = gsum[i + share * lane].astype(BF16)
            swap(n).start()

    def met(n):
        swap(n).wait_recv()
        each(*groups[n], sum_first)

    def term(i):
        return gsum[i + share * c] + gprx[i].astype(F32)

    def sum_hop(way, i):
        return remote(wtx.at[way, i], wrx.at[way, i], sum_s.at[way], sum_r.at[way, i], s, nxt[way])

    def sum_first(i):
        for way in range(2):
            @pl.when(hops[way] == 0)
            def _():
                wtx[way, i] = term(i).astype(BF16)
                sum_hop(way, i).start()

    def sum_relay(way, i):
        sum_hop(way, i).wait_recv()

        @pl.when(has_next[way])
        def _():
            wtx[way, i] = (term(i) + wrx[way, i].astype(F32)).astype(BF16)
            sum_hop(way, i).start()

    def each(lo, hi, body):
        def step(i, carry):
            body(i)
            return carry
        lax.fori_loop(lo, hi, step, 0)

    far = last * H
    lead = min(H + LEAD, far)
    for k in range(1, last):
        for g in range(G):
            relay(k, g)
    for h in range(H):
        for g in parts_of(h):
            relay(last, g)
        if h == H - 1:
            grad_wait(steps)
            weight_sums(grad, act, 0, front, ((2 * share, 0, front),))
            exchange(1, 3)
        if h > 0:
            gathered(h - 1)
            activate(h - 1)
            expand(h - 1)

    gathered(H - 1)
    activate(H - 1)
    expand(H - 1)

    @pl.when(c == 1)
    def _():
        met(3)

    def pair_copy(h):
        return remote(part.at[other, h], prx.at[h], px_s, px_r.at[h], s, partner)

    rem = rows % 8
    main = rows - rem
    tall = part.shape[3]

    height = (pl.ds(0, main), pl.ds(0, tall))

    def forms(h, body):
        @pl.when(h < H - 1)
        def _():
            body(0)

        @pl.when(h == H - 1)
        def _():
            body(1)

    def mine(h, chip):
        return part[c, h, chip].astype(F32) + prx[h, chip].astype(F32)

    def goal(way, m):
        return last - m if way == 0 else m

    def row_hop(way, r, kind):
        m, h = r // H, lax.rem(r, H)
        to, at = goal(way, m), height[kind]
        return remote(
            part.at[c, h, to, at], rx.at[way, h, to, at], row_s.at[way, kind], row_r.at[way, r], s, nxt[way],
        )

    def row_start(way, r):
        m, h = r // H, lax.rem(r, H)
        to = goal(way, m)
        part[c, h, to] = mine(h, to).astype(BF16)
        forms(h, lambda kind: row_hop(way, r, kind).start())

    def row_relay(way, r):
        m, h = r // H, lax.rem(r, H)
        to = goal(way, m)

        @pl.when(last - m > hops[way])
        def _():
            forms(h, lambda kind: row_hop(way, r, kind).wait_recv())
            part[c, h, to] = (mine(h, to) + rx[way, h, to].astype(F32)).astype(BF16)
            forms(h, lambda kind: row_hop(way, r, kind).start())

    def scatter(h):
        pair_copy(h).wait_recv()
        for way in range(2):
            @pl.when(hops[way] == 0)
            def _():
                row_start(way, h)

    tile = min(256, half)
    for h in range(H):
        for n in range(half // tile):
            value = dot(hidden[...], wred[:, pl.ds(h * half + n * tile, tile)]).astype(BF16)
            for dev in range(n_dev):
                low, col = dev * padded, pl.ds(n * tile, tile)
                part[dev % 2, h, dev // 2, 0:main, col] = value[low:low + main]
                if rem:
                    tail = main + rem * h
                    part[dev % 2, H - 1, dev // 2, tail:tail + rem, col] = value[low + main:low + rows]
        pair_copy(h).start()
        if h < steps:
            grad_wait(h)
            backward(h)
        if h > 0:
            scatter(h - 1)

    def rest(r):
        for way in range(2):
            @pl.when(hops[way] == 0)
            def _():
                row_start(way, r)

    scatter(H - 1)
    each(H, lead, rest)
    for j in range(H, steps):
        grad_wait(j)
    weight_sums(grad, act, front, pieces, ((0, front, front + half_r), (share, front + half_r, pieces)))
    for lane in range(2):
        exchange(lane, 0)
    for j in range(H, steps):
        backward(j)
    met(0)
    for way in range(2):
        @pl.when(both(c == 1, hops[way] == 1))
        def _():
            each(share, share + front, functools.partial(sum_relay, way))
    weight_sums(saved, slope, 0, pieces, ((half_r, 0, half_e), (share + half_r, half_e, pieces)))
    for lane in range(2):
        exchange(lane, 1)
        exchange(lane, 2)
    per = front // H
    for h in range(H):
        for way in range(2):
            @pl.when(both(c == 1, hops[way] == 2))
            def _():
                for i in range(per):
                    sum_relay(way, share + h * per + i)
        for way in range(2):
            @pl.when(hops[way] == 1)
            def _():
                row_relay(way, h)
    for way in range(2):
        @pl.when(hops[way] == 2)
        def _():
            for h in range(H // 2):
                row_relay(way, h)

    def give(i, lane):
        piece = gout.at[i + share * lane]
        return remote(piece, piece, wp_s, wp_r, s, partner)

    def sum_finish(i):
        value = term(i) + (wrx[0, i].astype(F32) + wrx[1, i].astype(F32))
        gout[i + share * c] = (value * factor).astype(BF16)
        give(i, c).start()

    met(1)
    met(2)
    each(lead, far, rest)
    count = far + share
    farther = jnp.maximum(hops[0], hops[1])

    def slot(t):
        for way in range(2):
            i = t - SKEW * hops[way]
            live = hops[way] > 0

            @pl.when(both(hops[way] > 1, both(i >= H // 2 * (3 - jnp.minimum(hops[way], 3)), i < H)))
            def _():
                row_relay(way, i)

            @pl.when(both(both(c == 1, hops[way] > 2), both(i >= H, i < H + front)))
            def _():
                sum_relay(way, i - H + share)

            @pl.when(both(live, both(i >= H, i < H + share)))
            def _():
                sum_relay(way, i - H)

            @pl.when(both(live, both(i >= H + share, i < count)))
            def _():
                row_relay(way, i - share)

        i = t - SKEW * farther - H

        @pl.when(both(c == 1, both(i >= 0, i < front)))
        def _():
            sum_finish(i + share)

        @pl.when(both(i >= 0, i < share))
        def _():
            sum_finish(i)

    @pl.when(s < sections - 1)
    def _():
        span(stage, perm_send, perm_recv.at[0]).wait_send()

    @pl.when(s > 0)
    def _():
        remote(up_hbm, grad, gp_send, gp_recv.at[0], s, partner).wait_send()

    gather_drain()
    span(prx, px_s, px_r.at[0]).wait_send()
    for lane in range(2):
        mass = share + front * lane

        @pl.when(other == lane)
        def _():
            span(gtx.at[0:mass], gx_s, gx_r.at[0]).wait_send()

    @pl.when(farther == last)
    def _():
        each(0, steps, downward)

    each(SKEW, H + share + SKEW * last, slot)

    @pl.when(farther < last)
    def _():
        each(0, steps, downward)


    for h in range(H):
        for way in range(2):
            @pl.when(hops[way] > 0)
            def _():
                row_hop(way, (last - hops[way]) * H + h, h // (H - 1)).wait_recv()
        value = mine(h, q) + rx[0, h, q].astype(F32) + rx[1, h, q].astype(F32)
        late_out[0:main, cols(h)] = (lbuf[h, d, 0:main].astype(F32) + value[0:main]).astype(BF16)
    if rem:
        for h in range(H):
            tail = main + rem * h
            end = lbuf[h, d, main:rows].astype(F32) + value[tail:tail + rem]
            late_out[main:rows, cols(h)] = end.astype(BF16)

    for way in range(2):
        for k in range(last):
            @pl.when(hops[way] == k)
            def _():
                for kind, planes in enumerate((pl.ds(0, H - 1), pl.ds(H - 1, 1))):
                    span(prx.at[planes, 0:last - k, height[kind]], row_s.at[way, kind], px_r.at[0]).wait_send()
    for lane in range(2):
        mass = share + front * lane
        block = gout.at[lane * share:lane * share + mass]

        @pl.when(c == lane)
        def _():
            for way in range(2):
                @pl.when(has_next[way])
                def _():
                    span(wtx.at[way, 0:mass], sum_s.at[way], gx_r.at[0]).wait_send()
            span(block, wp_s, wp_r).wait_send()

        @pl.when(other == lane)
        def _():
            span(block, wp_s, wp_r).wait_recv()


def finish(late_in, grad_in, sums, late_out, input_grad, gexp, gred, wide_e, wide_r, sem):
    ce, fe = wide_e.shape
    a = pltpu.make_async_copy(grad_in, input_grad.at[0], sem.at[0])
    b = pltpu.make_async_copy(late_in, late_out.at[0], sem.at[1])
    a.start()
    b.start()
    pieces, front, share = cuts(ce)
    depth = ce // pieces
    half_r = (pieces - front) // 2
    copies = [a, b]

    def send(src, dst):
        copies.append(pltpu.make_async_copy(src, dst, sem.at[len(copies)]))
        copies[-1].start()

    for lane in range(2):
        at = pl.ds(lane * (ce // 2), ce // 2)
        wide_e[at] = sums[lane * share + half_r:lane * share + share].reshape(ce // 2, fe).astype(F32)
        send(wide_e.at[at], gexp.at[0, at])
    for n in range(fe // 256):
        at = pl.ds(n * 256, 256)
        wide_r[at, 0:front * depth] = sums[2 * share:, :, at].reshape(front * depth, 256).T.astype(F32)
        later = [sums[lane:lane + half_r, :, at].reshape(half_r * depth, 256) for lane in (0, share)]
        wide_r[at, front * depth:] = jnp.concatenate(later).T.astype(F32)
        send(wide_r.at[at], gred.at[0, at])
    for copy in copies:
        copy.wait()


def shards(
    sections, n_dev,
    late_sent, entry_rows, gain_first, shift_first, expand_late, gain_inner, shift_inner,
    reduce_late, early_saved, upstream_grad, exit_grad, expand_early, reduce_early,
):
    rows, cl = entry_rows.shape
    e_rows, ce = exit_grad.shape
    fe = expand_early.shape[2]
    hid = expand_late.shape[2]
    Q = n_dev // 2
    half = cl // H
    padded = -(-rows // 16) * 16
    tall = rows + (H - 1) * (rows % 8)
    chunk = max(k for k in range(16, 257, 16) if e_rows % k == 0)
    steps = e_rows // chunk
    pieces, front, share = cuts(ce)
    depth = ce // pieces
    own = share + front
    split = n_dev * padded * hid * 4 <= 4 * 1024 * 1024
    hbm = pl.BlockSpec(memory_space=pltpu.HBM)
    any_spec = pl.BlockSpec(memory_space=pl.ANY)
    vm = pl.BlockSpec(memory_space=pltpu.VMEM)
    V = pltpu.VMEM
    dma = pltpu.SemaphoreType.DMA
    late_out, input_grad, sums = pl.pallas_call(
        functools.partial(kernel, sections, n_dev, chunk, split),
        out_shape=(
            V((rows, cl), BF16),
            V((e_rows, ce), BF16),
            V((2 * pieces, depth, fe), BF16),
        ),
        in_specs=[hbm] * 13,
        out_specs=(vm, vm, vm),
        scratch_shapes=[
            V((rows, cl), BF16),
            V((H, n_dev, rows, half), BF16),
            V((n_dev * padded, cl), BF16),
            V((n_dev * padded, hid) if split else (8, 128), F32),
            V((n_dev * padded, hid), BF16),
            V((2, H, Q, tall, half), BF16),
            V((H, Q, tall, half), BF16),
            V((2, H, Q, tall, half), BF16),
            V((cl, hid), BF16),
            V((hid, cl), BF16),
            V((e_rows, ce), BF16),
            V((e_rows, ce), BF16),
            V((ce, fe), BF16),
            V((fe, ce), BF16),
            V((e_rows, fe), BF16),
            V((e_rows, fe), BF16),
            V((e_rows, fe), BF16),
            V((2 * pieces, depth, fe), F32),
            V((own, depth, fe), BF16),
            V((own, depth, fe), BF16),
            V((2, own, depth, fe), BF16),
            V((2, own, depth, fe), BF16),
            V((1, cl), F32),
            V((1, cl), F32),
            V((1, hid), F32),
            V((1, hid), F32),
            dma((10,)), dma((H + U - 1,)), dma((steps + 1,)), dma((2, Q - 1, H + U - 1)), dma((H,)), dma((H,)),
            dma((4,)), dma((2, (Q - 1) * H)), dma((2, own)), dma,
            dma, dma, dma((2,)), dma, dma, dma, dma((2, 2)), dma((2,)), dma,
        ],
        compiler_params=pltpu.CompilerParams(
            collective_id=0, has_side_effects=True, vmem_limit_bytes=60 * 1024 * 1024
        ),
        name="relay",
    )(
        late_sent[0], entry_rows, gain_first, shift_first, expand_late[0], gain_inner, shift_inner,
        reduce_late[0], early_saved[0], upstream_grad[0], exit_grad, expand_early[0], reduce_early[0],
    )
    return pl.pallas_call(
        finish,
        out_shape=(
            jax.ShapeDtypeStruct((1, rows, cl), BF16),
            jax.ShapeDtypeStruct((1, e_rows, ce), BF16),
            jax.ShapeDtypeStruct((1, ce, fe), F32),
            jax.ShapeDtypeStruct((1, fe, ce), F32),
        ),
        in_specs=[vm, vm, vm],
        out_specs=(any_spec,) * 4,
        scratch_shapes=[V((ce, fe), F32), V((fe, ce), F32), dma((4 + fe // 256,))],
        compiler_params=pltpu.CompilerParams(vmem_limit_bytes=16 * 1024 * 1024),
        name="finish",
    )(late_out, input_grad, sums)


def solution(mesh):
    sections, n_dev = mesh.shape["section"], mesh.shape["dev"]
    sd, dd = P("section", "dev", None), P("dev", None)
    rep, one = P("section", None, None), P("section", None)
    in_specs = (
        sd, dd, one, one, P("section", None, "dev"), P("section", "dev"), P("section", "dev"),
        sd, sd, sd, dd, rep, rep,
    )
    return jax.shard_map(
        functools.partial(shards, sections, n_dev), mesh=mesh, in_specs=in_specs,
        out_specs=(sd, sd, rep, rep), check_vma=False,
    )
```
